8 devices in a mesh: dp: 2 (over z, y), cp: 4 (over x, core).
Axes of the slice: x: 2, y: 2, z: 1, core: 2. Of those that a mesh axis runs over, the one named last changes fastest.
Arguments:
- hidden: bfloat16 [32, 256, 2304], P('dp'), parts along dimension 0
- start_pos: int32 [32], P('dp'), parts along dimension 0
- cache_k: bfloat16 [32, 512, 1024], P('dp', 'cp'), parts along dimension 0
- cache_v: bfloat16 [32, 512, 1024], P('dp', 'cp'), parts along dimension 0
- w_q: bfloat16 [2304, 8, 256], replicated
- w_k: bfloat16 [2304, 4, 256], replicated
- w_v: bfloat16 [2304, 4, 256], replicated
- w_o: bfloat16 [8, 256, 2304], replicated
- w_gate: bfloat16 [2304, 9216], replicated
- w_up: bfloat16 [2304, 9216], replicated
- w_down: bfloat16 [9216, 2304], replicated
- norm_attn: bfloat16 [2304], replicated
- norm_mlp: bfloat16 [2304], replicated
Outputs:
- output 1: bfloat16 [32, 256, 2304], P('dp'), parts along dimension 0
- output 2: bfloat16 [32, 512, 1024], P('dp', 'cp'), parts along dimension 0
- output 3: bfloat16 [32, 512, 1024], P('dp', 'cp'), parts along dimension 0
There are 2 independent parts. The reference program is written for one: setup_inputs(seed, part) draws one part's arguments, and reference() takes and returns one part's arrays. A program takes and returns all parts, laid end to end along the dimension named above; an argument that names none is the same for every part.
All inputs are finite; a program needn't handle non-finite values.
Results may differ from the reference program's by a relative error of at most 0.0180753.
Values sent between devices are 32-bit elements.
A program may use at most 1 GiB of HBM per device.

```python
import jax
import jax.numpy as jnp
from jax import lax

NUM_SEQ = 16
CHUNK_LEN = 256
MODEL_DIM = 2304
NUM_HEADS = 8
KV_HEADS = 4
HEAD_DIM = 256
FF_DIM = 9216
CACHE_LEN = 512

GROUP_SIZE = NUM_HEADS // KV_HEADS
KV_WIDTH = KV_HEADS * HEAD_DIM
NORM_EPS = 1e-6
ROPE_BASE = 1.0e4


def normal_weight(rng_key, shape, fan_in, scale_gain):
    return (jax.random.normal(rng_key, shape, jnp.float32) * (scale_gain * fan_in ** -0.5)).astype(jnp.bfloat16)


def setup_inputs(seed: int = 0, part: int = 0) -> dict:
    part_keys = jax.random.split(jax.random.fold_in(jax.random.key(seed), part), 4)
    shared_keys = jax.random.split(jax.random.key(seed + 1), 9)
    hidden = jax.random.normal(part_keys[0], (NUM_SEQ, CHUNK_LEN, MODEL_DIM), jnp.float32).astype(jnp.bfloat16)
    seq_index = jnp.arange(NUM_SEQ, dtype=jnp.int32)
    drawn = jax.random.randint(part_keys[1], (NUM_SEQ,), 0, CACHE_LEN - CHUNK_LEN + 1, dtype=jnp.int32)
    start_pos = jnp.where(seq_index == 0, CACHE_LEN - CHUNK_LEN, jnp.where(seq_index == 1, 0, drawn)).astype(jnp.int32)
    cache_k = jax.random.normal(part_keys[2], (NUM_SEQ, CACHE_LEN, KV_WIDTH), jnp.float32).astype(jnp.bfloat16)
    cache_v = jax.random.normal(part_keys[3], (NUM_SEQ, CACHE_LEN, KV_WIDTH), jnp.float32).astype(jnp.bfloat16)
    return {
        'hidden': hidden,
        'start_pos': start_pos,
        'cache_k': cache_k,
        'cache_v': cache_v,
        'w_q': normal_weight(shared_keys[0], (MODEL_DIM, NUM_HEADS, HEAD_DIM), MODEL_DIM, 2.5),
        'w_k': normal_weight(shared_keys[1], (MODEL_DIM, KV_HEADS, HEAD_DIM), MODEL_DIM, 1.0),
        'w_v': normal_weight(shared_keys[2], (MODEL_DIM, KV_HEADS, HEAD_DIM), MODEL_DIM, 1.0),
        'w_o': normal_weight(shared_keys[3], (NUM_HEADS, HEAD_DIM, MODEL_DIM), NUM_HEADS * HEAD_DIM, 2.0),
        'w_gate': normal_weight(shared_keys[4], (MODEL_DIM, FF_DIM), MODEL_DIM, 1.0),
        'w_up': normal_weight(shared_keys[5], (MODEL_DIM, FF_DIM), MODEL_DIM, 1.0),
        'w_down': normal_weight(shared_keys[6], (FF_DIM, MODEL_DIM), FF_DIM, 1.0),
        'norm_attn': (0.3 * jax.random.normal(shared_keys[7], (MODEL_DIM,), jnp.float32)).astype(jnp.bfloat16),
        'norm_mlp': (0.3 * jax.random.normal(shared_keys[8], (MODEL_DIM,), jnp.float32)).astype(jnp.bfloat16),
    }


def rms_norm(hidden, gain):
    hid_f32 = hidden.astype(jnp.float32)
    inv_rms = lax.rsqrt(jnp.mean(hid_f32 * hid_f32, axis=-1, keepdims=True) + NORM_EPS)
    return (hid_f32 * inv_rms * (1.0 + gain.astype(jnp.float32))).astype(jnp.bfloat16)


def rotate(proj, positions):
    half_dim = HEAD_DIM // 2
    inv_freq = ROPE_BASE ** (-2.0 * jnp.arange(half_dim, dtype=jnp.float32) / HEAD_DIM)
    angles = positions.astype(jnp.float32)[:, :, None, None] * inv_freq
    cos_tab = jnp.cos(angles)
    sin_tab = jnp.sin(angles)
    first = proj[..., :half_dim]
    second = proj[..., half_dim:]
    return jnp.concatenate([first * cos_tab - second * sin_tab, second * cos_tab + first * sin_tab], axis=-1)


def put_one(rows_old, rows_new, offset):
    return lax.dynamic_update_slice(rows_old, rows_new, (offset, jnp.zeros((), offset.dtype)))


def reference(hidden, start_pos, cache_k, cache_v, w_q, w_k, w_v, w_o, w_gate, w_up, w_down, norm_attn, norm_mlp):
    normed = rms_norm(hidden, norm_attn)
    positions = start_pos[:, None] + jnp.arange(CHUNK_LEN, dtype=jnp.int32)[None, :]
    normed_f = normed.astype(jnp.float32)
    q_proj = jnp.einsum('bcd,dhe->bche', normed_f, w_q.astype(jnp.float32))
    queries = (rotate(q_proj, positions) * HEAD_DIM ** -0.5).astype(jnp.bfloat16)
    k_proj = jnp.einsum('bcd,dhe->bche', normed_f, w_k.astype(jnp.float32))
    k_rows = rotate(k_proj, positions).astype(jnp.bfloat16).reshape(NUM_SEQ, CHUNK_LEN, KV_WIDTH)
    v_rows = jnp.einsum('bcd,dhe->bche', normed_f, w_v.astype(jnp.float32)).astype(jnp.bfloat16).reshape(NUM_SEQ, CHUNK_LEN, KV_WIDTH)
    put_rows = jax.vmap(put_one)
    new_k = put_rows(cache_k, k_rows, start_pos)
    new_v = put_rows(cache_v, v_rows, start_pos)
    key_pos = jnp.arange(CACHE_LEN, dtype=jnp.int32)

    def one_sequence(seq_inputs):
        q_seq, k_seq, v_seq, pos_seq = seq_inputs
        q_grp = q_seq.reshape(CHUNK_LEN, KV_HEADS, GROUP_SIZE, HEAD_DIM).astype(jnp.float32)
        k_all = k_seq.reshape(CACHE_LEN, KV_HEADS, HEAD_DIM).astype(jnp.float32)
        v_all = v_seq.reshape(CACHE_LEN, KV_HEADS, HEAD_DIM).astype(jnp.float32)
        scores = jnp.einsum('ckgd,skd->kgcs', q_grp, k_all)
        allowed = key_pos[None, :] <= pos_seq[:, None]
        probs = jax.nn.softmax(jnp.where(allowed, scores, -jnp.inf), axis=-1)
        mixed = jnp.einsum('kgcs,skd->ckgd', probs, v_all)
        return mixed.reshape(CHUNK_LEN, NUM_HEADS, HEAD_DIM)

    attended = lax.map(one_sequence, (queries, new_k, new_v, positions)).astype(jnp.bfloat16)
    attn_out = jnp.einsum('bchd,hde->bce', attended.astype(jnp.float32), w_o.astype(jnp.float32))
    residual = (hidden.astype(jnp.float32) + attn_out).astype(jnp.bfloat16)
    normed_mlp = rms_norm(residual, norm_mlp).astype(jnp.float32)
    gate_proj = jnp.einsum('bcd,df->bcf', normed_mlp, w_gate.astype(jnp.float32))
    up_proj = jnp.einsum('bcd,df->bcf', normed_mlp, w_up.astype(jnp.float32))
    gated_mid = (jax.nn.gelu(gate_proj, approximate=True) * up_proj).astype(jnp.bfloat16)
    down_proj = jnp.einsum('bcf,fd->bcd', gated_mid.astype(jnp.float32), w_down.astype(jnp.float32))
    hidden_out = (residual.astype(jnp.float32) + down_proj).astype(jnp.bfloat16)
    return (hidden_out, new_k, new_v)
```

```python
import functools

import jax
import jax.numpy as jnp
from jax import lax
from jax.experimental import pallas as pl
from jax.experimental.pallas import tpu as pltpu
from jax.sharding import PartitionSpec as P

NORM_EPS = 1e-6
ROPE_BASE = 1.0e4
MASK_FLOOR = -1.0e30
GELU_C = 0.7978845608028654

UNIT = 32
N_P1, N_P2, N_P3 = 2, 6, 18
FF_BLK = 768
F32 = jnp.float32
BF16 = jnp.bfloat16


def rms_norm(x, gain):
    inv = lax.rsqrt(jnp.mean(x * x, axis=-1, keepdims=True) + NORM_EPS)
    return (x * inv * (1.0 + gain)).astype(BF16)


def rotate(x, cos, sin):
    half = x.shape[-1] // 2
    first, second = x[:, :half], x[:, half:]
    return jnp.concatenate([first * cos - second * sin, second * cos + first * sin], axis=-1)


def gelu_tanh(x):
    return 0.5 * x * (1.0 + jnp.tanh(GELU_C * (x + 0.044715 * (x * x * x))))


def dot(a, b):
    return jnp.dot(a, b, preferred_element_type=F32)


def dot_t(a, b):
    return lax.dot_general(a, b, (((1,), (1,)), ((), ())), preferred_element_type=F32)


def pack_kernel(n_out, seq_ref, row_ref, ck_ref, cv_ref, *rest):
    outs = rest[: len(n_out)]
    raw, wide, in_sem, out_sem = rest[len(n_out):]
    total = sum(n_out)

    def in_copies(u):
        src = pl.ds(pl.multiple_of(row_ref[u], UNIT), UNIT)
        return (
            pltpu.make_async_copy(ck_ref.at[seq_ref[u], src, :], raw.at[u, 0], in_sem.at[u, 0]),
            pltpu.make_async_copy(cv_ref.at[seq_ref[u], src, :], raw.at[u, 1], in_sem.at[u, 1]),
        )

    @pl.loop(0, total)
    def _(u):
        for copy in in_copies(u):
            copy.start()

    base = 0
    for out, n in zip(outs, n_out):
        @pl.loop(0, n)
        def _(k, out=out, base=base):
            u = base + k
            for copy in in_copies(u):
                copy.wait()
            wide[u, :, :1024] = raw[u, 0].astype(F32)
            wide[u, :, 1024:] = raw[u, 1].astype(F32)
            pltpu.make_async_copy(wide.at[u], out.at[k], out_sem.at[u]).start()
        base += n
    base = 0
    for out, n in zip(outs, n_out):
        @pl.loop(0, n)
        def _(k, out=out, base=base):
            pltpu.make_async_copy(wide.at[base + k], out.at[k], out_sem.at[base + k]).wait()
        base += n


def pack_units(cache_k, cache_v, seqs, rows, n_out, name):
    total = sum(n_out)
    return pl.pallas_call(
        functools.partial(pack_kernel, n_out),
        out_shape=[jax.ShapeDtypeStruct((n, UNIT, 2048), F32) for n in n_out],
        grid_spec=pltpu.PrefetchScalarGridSpec(
            num_scalar_prefetch=2,
            grid=(),
            in_specs=[pl.BlockSpec(memory_space=pl.ANY)] * 2,
            out_specs=[pl.BlockSpec(memory_space=pl.ANY)] * len(n_out),
            scratch_shapes=[
                pltpu.VMEM((total, 2, UNIT, 1024), BF16),
                pltpu.VMEM((total, UNIT, 2048), F32),
                pltpu.SemaphoreType.DMA((total, 2)),
                pltpu.SemaphoreType.DMA((total,)),
            ],
        ),
        compiler_params=pltpu.CompilerParams(vmem_limit_bytes=48 * 2**20),
        cost_estimate=pl.CostEstimate(flops=100_000_000, bytes_accessed=total * UNIT * 2048 * 6, transcendentals=0),
        name=name,
    )(seqs, rows, cache_k, cache_v)


def blank_kernel(*refs):
    pass


def blank(n, count):
    return pl.pallas_call(
        blank_kernel,
        out_shape=[jax.ShapeDtypeStruct((n, UNIT, 2048), F32)] * count,
        out_specs=[pl.BlockSpec(memory_space=pl.ANY)] * count,
        name="blank",
    )()


def layer_kernel(n_ff, n_pieces, sc_ref, h_ref, ga_ref, gm_ref, cos_ref, sin_ref, wq_ref, wk_ref, wv_ref, wo_ref,
                 wg_ref, wu_ref, wd_ref, ck_ref, cv_ref, sib_ref, full_ref, fullf_ref, *rest):
    pieces = rest[: 2 * n_pieces]
    out_ref, act, acc, stage, hist, sem, own_sem = rest[2 * n_pieces:]
    step = pl.program_id(0)
    x_pos, core = sc_ref[2], sc_ref[3]
    start = sc_ref[1]
    per_half = 128 // UNIT
    piece_base = (0, N_P1, N_P1 + N_P2, N_P1 + N_P2 + N_P3)

    def unit_copies(hh, u):
        k = hh * per_half + u
        dst = stage.at[pl.ds(pl.multiple_of(k * UNIT, UNIT), UNIT), :]
        live = u < sc_ref[9 + hh]
        far = x_pos == 1
        direct = core == hh
        ovf = sc_ref[4] == 1
        pos = sc_ref[7 + hh] + u
        out = [
            (live & (x_pos == 0) & (core != hh), sib_ref.at[sc_ref[5] * per_half + u]),
            (live & far & ovf & direct, full_ref.at[sc_ref[6] * per_half + u]),
            (live & far & ovf & jnp.logical_not(direct), fullf_ref.at[sc_ref[6] * per_half + u]),
        ]
        for p in range(n_pieces):
            here = live & far & jnp.logical_not(ovf) & (pos >= piece_base[p]) & (pos < piece_base[p + 1])
            idx = jnp.clip(pos - piece_base[p], 0, piece_base[p + 1] - piece_base[p] - 1)
            out.append((here & direct, pieces[2 * p].at[idx]))
            out.append((here & jnp.logical_not(direct), pieces[2 * p + 1].at[idx]))
        return [(c, pltpu.make_async_copy(src, dst, sem.at[k])) for c, src in out]

    def own_copies(hh):
        rows = pl.ds(hh * 128, 128)
        return (
            pltpu.make_async_copy(ck_ref.at[sc_ref[0]], hist.at[rows, pl.ds(0, 1024)], own_sem.at[0]),
            pltpu.make_async_copy(cv_ref.at[sc_ref[0]], hist.at[rows, pl.ds(1024, 1024)], own_sem.at[1]),
        )

    @pl.when(step == 0)
    def _():
        for hh in range(2):
            @pl.loop(0, per_half)
            def _(u, hh=hh):
                for cond, copy in unit_copies(hh, u):
                    @pl.when(cond)
                    def _(copy=copy):
                        copy.start()

            @pl.when((x_pos == 0) & (core == hh))
            def _(hh=hh):
                for copy in own_copies(hh):
                    copy.start()
        act[...] = rms_norm(h_ref[0].astype(F32), ga_ref[...].astype(F32))
        acc[...] = jnp.zeros_like(acc)
        for hh in range(2):
            @pl.loop(0, per_half)
            def _(u, hh=hh):
                for cond, copy in unit_copies(hh, u):
                    @pl.when(cond)
                    def _(copy=copy):
                        copy.wait()

            @pl.when((x_pos == 0) & (core == hh))
            def _(hh=hh):
                for copy in own_copies(hh):
                    copy.wait()

            @pl.when((x_pos == 1) | (core != hh))
            def _(hh=hh):
                hist[hh * 128:(hh + 1) * 128, :] = stage[hh * 128:(hh + 1) * 128, :].astype(BF16)

    @pl.when(step < 4)
    def _():
        cos, sin = cos_ref[0], sin_ref[0]
        a = act[...]
        k_new = rotate(dot(a, wk_ref[0]), cos, sin).astype(BF16)
        v_new = dot(a, wv_ref[0]).astype(BF16)
        off = pl.multiple_of(step * 256, 256)
        k_old = hist[:, pl.ds(off, 256)]
        row = lax.broadcasted_iota(jnp.int32, (256, 256), 0)
        col = lax.broadcasted_iota(jnp.int32, (256, 256), 1)
        v_old = jnp.where(row < start, hist[:, pl.ds(off + 1024, 256)], jnp.zeros((), BF16))
        old_ok = col < start
        new_ok = col <= row
        heads = []
        for j in range(2):
            q = (rotate(dot(a, wq_ref[j]), cos, sin) * 0.0625).astype(BF16)
            s_old = jnp.where(old_ok, dot_t(q, k_old), MASK_FLOOR)
            s_new = jnp.where(new_ok, dot_t(q, k_new), MASK_FLOOR)
            top = jnp.maximum(jnp.max(s_old, axis=-1, keepdims=True), jnp.max(s_new, axis=-1, keepdims=True))
            p_old = jnp.where(old_ok, jnp.exp(s_old - top), 0.0)
            p_new = jnp.where(new_ok, jnp.exp(s_new - top), 0.0)
            den = jnp.sum(p_old, axis=-1, keepdims=True) + jnp.sum(p_new, axis=-1, keepdims=True)
            num = dot(p_old.astype(BF16), v_old) + dot(p_new.astype(BF16), v_new)
            heads.append((num / den).astype(BF16))
        acc[...] += dot(jnp.concatenate(heads, axis=-1), wo_ref[...])

    @pl.when(step == 3)
    def _():
        res = (h_ref[0].astype(F32) + acc[...]).astype(BF16).astype(F32)
        act[...] = rms_norm(res, gm_ref[...].astype(F32))
        acc[...] = res

    @pl.when(step >= 4)
    def _():
        c = act[...]
        mid = (gelu_tanh(dot(c, wg_ref[...])) * dot(c, wu_ref[...])).astype(BF16)
        acc[...] += dot(mid, wd_ref[...])

    @pl.when(step == n_ff + 3)
    def _():
        out_ref[...] = acc[...].astype(BF16).astype(F32)


def run_layer(slot, scalars, hidden, ga, gm, cos, sin, wq, wk, wv, wo, wg, wu, wd, ck, cv, sib, full, fullf, pieces):
    n_ff = wg.shape[1] // FF_BLK
    n_pieces = len(pieces) // 2
    att = lambda i, *_: jnp.minimum(i, 3)
    ffn = lambda i, *_: jnp.clip(i - 4, 0, n_ff - 1)
    one = pl.Buffered(1)
    any_spec = pl.BlockSpec(memory_space=pl.ANY)
    d = hidden.shape[2]
    flops = 2 * 256 * d * (2048 * 2 + 1024 * 2 + 3 * wg.shape[1]) + 1_100_000_000
    return pl.pallas_call(
        functools.partial(layer_kernel, n_ff, n_pieces),
        out_shape=jax.ShapeDtypeStruct((256, d), F32),
        grid_spec=pltpu.PrefetchScalarGridSpec(
            num_scalar_prefetch=1,
            grid=(n_ff + 4,),
            in_specs=[
                pl.BlockSpec((1, 256, d), lambda i, sc: (sc[0], 0, 0), pipeline_mode=one),
                pl.BlockSpec((1, d), lambda i, sc: (0, 0), pipeline_mode=one),
                pl.BlockSpec((1, d), lambda i, sc: (0, 0), pipeline_mode=one),
                pl.BlockSpec((1, 256, 128), lambda i, sc: (slot, 0, 0), pipeline_mode=one),
                pl.BlockSpec((1, 256, 128), lambda i, sc: (slot, 0, 0), pipeline_mode=one),
                pl.BlockSpec((2, d, 256), lambda i, sc: (att(i), 0, 0)),
                pl.BlockSpec((1, d, 256), lambda i, sc: (att(i), 0, 0)),
                pl.BlockSpec((1, d, 256), lambda i, sc: (att(i), 0, 0)),
                pl.BlockSpec((512, d), lambda i, sc: (att(i), 0)),
                pl.BlockSpec((d, FF_BLK), lambda i, sc: (0, ffn(i))),
                pl.BlockSpec((d, FF_BLK), lambda i, sc: (0, ffn(i))),
                pl.BlockSpec((FF_BLK, d), lambda i, sc: (ffn(i), 0)),
            ] + [any_spec] * (5 + 2 * n_pieces),
            out_specs=pl.BlockSpec((256, d), lambda i, sc: (0, 0), pipeline_mode=one),
            scratch_shapes=[
                pltpu.VMEM((256, d), BF16),
                pltpu.VMEM((256, d), F32),
                pltpu.VMEM((256, 2048), F32),
                pltpu.VMEM((256, 2048), BF16),
                pltpu.SemaphoreType.DMA((8,)),
                pltpu.SemaphoreType.DMA((2,)),
            ],
        ),
        compiler_params=pltpu.CompilerParams(vmem_limit_bytes=62 * 2**20),
        cost_estimate=pl.CostEstimate(flops=flops, bytes_accessed=160_000_000, transcendentals=0),
        name=f"layer_{slot}",
    )(scalars, hidden, ga, gm, cos, sin, wq, wk, wv, wo, wg, wu, wd, ck, cv, sib, full, fullf, *pieces)


def window_kernel(sc_ref, h_ref, ga_ref, cos_ref, sin_ref, wk_ref, wv_ref, ck_ref, cv_ref, ok_ref, ov_ref):
    step = pl.program_id(0)
    lo = sc_ref[16]
    a_rows, inside = [], []
    for j in range(2):
        first = lo - sc_ref[2 * step + j]
        want = first + lax.broadcasted_iota(jnp.int32, (128, 256), 0)
        have = lax.broadcasted_iota(jnp.int32, (128, 256), 1)
        pick = jnp.where(want == have, 1.0, 0.0).astype(BF16)
        a_rows.append(dot(pick, h_ref[j]))
        idx = first + lax.broadcasted_iota(jnp.int32, (128, 256), 0)
        inside.append((idx >= 0) & (idx < 256))
    a = rms_norm(jnp.concatenate(a_rows, axis=0), ga_ref[...].astype(F32))
    cos = jnp.concatenate([cos_ref[...]] * 2, axis=0)
    sin = jnp.concatenate([sin_ref[...]] * 2, axis=0)
    for g in range(4):
        k = rotate(dot(a, wk_ref[g]), cos, sin).astype(BF16)
        v = dot(a, wv_ref[g]).astype(BF16)
        cols = slice(g * 256, (g + 1) * 256)
        for j in range(2):
            rows = slice(j * 128, (j + 1) * 128)
            ok_ref[j, :, cols] = jnp.where(inside[j], k[rows], ck_ref[j, :, cols])
            ov_ref[j, :, cols] = jnp.where(inside[j], v[rows], cv_ref[j, :, cols])


def write_windows(scalars, hidden, ga, cos, sin, wk, wv, cache_k, cache_v):
    n_seq, rows, width = cache_k.shape
    d = hidden.shape[2]
    one = pl.Buffered(1)
    cache_spec = pl.BlockSpec((2, rows, width), lambda i, sc: (i, 0, 0))
    return pl.pallas_call(
        window_kernel,
        out_shape=[jax.ShapeDtypeStruct(cache_k.shape, BF16)] * 2,
        grid_spec=pltpu.PrefetchScalarGridSpec(
            num_scalar_prefetch=1,
            grid=(n_seq // 2,),
            in_specs=[
                pl.BlockSpec((2, 256, d), lambda i, sc: (i, 0, 0)),
                pl.BlockSpec((1, d), lambda i, sc: (0, 0), pipeline_mode=one),
                pl.BlockSpec((rows, 128), lambda i, sc: (0, 0), pipeline_mode=one),
                pl.BlockSpec((rows, 128), lambda i, sc: (0, 0), pipeline_mode=one),
                pl.BlockSpec((4, d, 256), lambda i, sc: (0, 0, 0), pipeline_mode=one),
                pl.BlockSpec((4, d, 256), lambda i, sc: (0, 0, 0), pipeline_mode=one),
                cache_spec,
                cache_spec,
            ],
            out_specs=[cache_spec, cache_spec],
        ),
        compiler_params=pltpu.CompilerParams(vmem_limit_bytes=56 * 2**20),
        cost_estimate=pl.CostEstimate(flops=2 * n_seq * rows * d * 2 * width, bytes_accessed=60_000_000, transcendentals=0),
        name="cache_window",
    )(scalars, hidden, ga, cos, sin, wk, wv, cache_k, cache_v)


def place_kernel(seq_ref, own_ref, sib_ref, crs_ref, dia_ref, *rest):
    out_ref = rest[-1]
    src = pl.program_id(0)
    for k, ref in enumerate((own_ref, sib_ref, crs_ref, dia_ref)):
        @pl.when(src == k)
        def _(ref=ref):
            out_ref[0] = ref[...].astype(BF16)


def place_rows(seqs, parts, out, n_seq, slot):
    rows, d = parts[0].shape
    n_blk = 2
    blk = rows // n_blk

    def part_map(k):
        def index(src, b, sq):
            return (jnp.where(src == k, b, jnp.where(src < k, 0, n_blk - 1)), 0)
        return index

    in_specs = [pl.BlockSpec((blk, d), part_map(k)) for k in range(4)]
    args = [seqs, *parts]
    aliases = {}
    if out is not None:
        in_specs.append(pl.BlockSpec(memory_space=pl.ANY))
        aliases = {5: 0}
        args.append(out)
    return pl.pallas_call(
        place_kernel,
        out_shape=jax.ShapeDtypeStruct((n_seq, rows, d), BF16),
        grid_spec=pltpu.PrefetchScalarGridSpec(
            num_scalar_prefetch=1,
            grid=(4, n_blk),
            in_specs=in_specs,
            out_specs=pl.BlockSpec((1, blk, d), lambda src, b, sq: (sq[src], b, 0)),
        ),
        input_output_aliases=aliases,
        cost_estimate=pl.CostEstimate(flops=10_000_000, bytes_accessed=4 * rows * d * 6, transcendentals=0),
        name=f"place_{slot}",
    )(*args)


def solution(mesh):
    d2d = [(0, 1), (1, 0), (2, 3), (3, 2)]
    cross = [(0, 2), (1, 3), (2, 0), (3, 1)]

    def local_layer(hidden, start_pos, cache_k, cache_v, w_q, w_k, w_v, w_o, w_gate, w_up, w_down, norm_attn, norm_mlp):
        n_seq, chunk_len, d = hidden.shape
        shard_len = cache_k.shape[1]
        i32 = jnp.int32
        me = lax.axis_index('cp').astype(i32)
        x_pos, core = me // 2, me % 2
        per_half = shard_len // UNIT

        sid = jnp.arange(n_seq, dtype=i32)
        before = (start_pos[None, :] < start_pos[:, None]) | (
            (start_pos[None, :] == start_pos[:, None]) & (sid[None, :] < sid[:, None]))
        rank = jnp.sum(before.astype(i32), axis=1)
        onehot = (rank[None, :] == sid[:, None]).astype(i32)
        order = jnp.sum(onehot * sid[None, :], axis=1)
        length = jnp.sum(onehot * start_pos[None, :], axis=1)

        slot = jnp.arange(4, dtype=i32)
        src_x = jnp.stack([x_pos, x_pos, 1 - x_pos, 1 - x_pos])[:, None]
        src_c = jnp.stack([core, 1 - core, core, 1 - core])[:, None]
        idx8 = 2 * slot[None, :] + ((src_c + slot[None, :]) % 2)
        ranks = 8 * (1 - src_x) + idx8
        pick = (ranks[:, :, None] == sid[None, None, :]).astype(i32)
        seq_tbl = jnp.sum(pick * order[None, None, :], axis=-1)
        my_len = jnp.sum(pick[0] * length[None, :], axis=-1)

        halves = jnp.arange(2, dtype=i32)[:, None]
        cnt = jnp.clip((length[None, :8] - halves * shard_len + UNIT - 1) // UNIT, 0, per_half)
        ends = jnp.cumsum(cnt, axis=1) + halves * N_P1
        pos = ends - cnt
        over = (ends[0, 7] > N_P1 + N_P2 + N_P3) | (ends[1, 7] > N_P1 + N_P2) | (ends[0, 1] > N_P1) | (ends[1, 1] > N_P1)
        over = lax.pmax(over.astype(i32), ('dp', 'cp'))

        my_cnt8 = jnp.clip((my_len[None, :] - halves * shard_len + UNIT - 1) // UNIT, 0, per_half)
        pick8 = (idx8[0][:, None] == jnp.arange(8, dtype=i32)[None, :]).astype(i32)
        my_pos = jnp.sum(pick8[None] * pos[:, None, :], axis=-1)
        scal = jnp.stack([
            seq_tbl[0], my_len, jnp.broadcast_to(x_pos, (4,)), jnp.broadcast_to(core, (4,)),
            jnp.broadcast_to(over, (4,)), slot, idx8[0], my_pos[0], my_pos[1], my_cnt8[0], my_cnt8[1],
        ], axis=1)

        def pick_order(rk):
            return jnp.sum((rk[:, None] == sid[None, :]).astype(i32) * order[None, :], axis=-1)

        my_ends = jnp.where(core == 0, ends[0], ends[1])
        my_start = jnp.where(core == 0, pos[0], pos[1])
        p_all = jnp.arange(N_P1 + N_P2 + N_P3, dtype=i32)
        p_rank = jnp.minimum(jnp.sum((my_ends[None, :] <= p_all[:, None]).astype(i32), axis=1), 7)
        p_first = jnp.sum((p_rank[:, None] == jnp.arange(8, dtype=i32)[None, :]).astype(i32) * my_start[None, :], axis=1)
        p_unit = jnp.clip(p_all - p_first, 0, per_half - 1)
        b_all = jnp.arange(4 * per_half, dtype=i32)
        b_slot = b_all // per_half
        b_rank = 8 + 2 * b_slot + ((1 - core + b_slot) % 2)
        pack_seq = jnp.concatenate([pick_order(p_rank), pick_order(b_rank)])
        pack_row = jnp.concatenate([p_unit, b_all % per_half]) * UNIT
        p1, p2, p3, sib_src = pack_units(cache_k, cache_v, pack_seq, pack_row, (N_P1, N_P2, N_P3, 4 * per_half), "pack")
        p1d = lax.ppermute(p1, 'cp', [(0, 2)])
        sib = lax.ppermute(sib_src, 'cp', [(0, 1), (1, 0)])
        p1f = lax.ppermute(p1d, 'cp', [(2, 3)])
        p2d = lax.ppermute(p2, 'cp', [(0, 2), (1, 3)])
        p2f = lax.ppermute(p2d, 'cp', [(2, 3), (3, 2)])
        p3d = lax.ppermute(p3, 'cp', [(0, 2)])
        p3f = lax.ppermute(p3d, 'cp', [(2, 3)])

        def send_all(_):
            f_all = jnp.arange(8 * per_half, dtype=i32)
            (everything,) = pack_units(cache_k, cache_v, pick_order(f_all // per_half), (f_all % per_half) * UNIT,
                                       (8 * per_half,), "pack_full")
            got = lax.ppermute(everything, 'cp', [(0, 2), (1, 3)])
            return got, lax.ppermute(got, 'cp', [(2, 3), (3, 2)])

        full, full_f = lax.cond(over > 0, send_all, lambda _: tuple(blank(8 * per_half, 2)), 0)

        head_dim = w_q.shape[2]
        inv_freq = ROPE_BASE ** (-2.0 * jnp.arange(head_dim // 2, dtype=F32) / head_dim)
        own_pos = my_len[:, None] + jnp.arange(chunk_len, dtype=i32)[None, :]
        angles = own_pos.astype(F32)[:, :, None] * inv_freq
        cos, sin = jnp.cos(angles), jnp.sin(angles)
        win_lo = me * shard_len
        win_angles = (win_lo + jnp.arange(shard_len, dtype=i32)).astype(F32)[:, None] * inv_freq
        win_cos, win_sin = jnp.cos(win_angles), jnp.sin(win_angles)
        wq = w_q.transpose(1, 0, 2)
        wk = w_k.transpose(1, 0, 2)
        wv = w_v.transpose(1, 0, 2)
        wo = w_o.reshape(-1, d)
        ga, gm = norm_attn[None, :], norm_mlp[None, :]

        out = None
        parts = []
        for t in range(4):
            pieces = (p1d, p1f) if t == 0 else (p1d, p1f, p2d, p2f, p3d, p3f)
            own = run_layer(t, scal[t], hidden, ga, gm, cos, sin, wq, wk, wv, wo, w_gate, w_up, w_down,
                            cache_k, cache_v, sib, full, full_f, pieces)
            crs = lax.ppermute(own, 'cp', cross)
            near = lax.ppermute(own, 'cp', d2d)
            dia = lax.ppermute(crs, 'cp', d2d)
            parts.append((own, near, crs, dia))
        new_k, new_v = write_windows(jnp.concatenate([start_pos, win_lo[None]]), hidden, ga, win_cos, win_sin, wk, wv,
                                     cache_k, cache_v)
        for t in range(4):
            out = place_rows(seq_tbl[:, t], parts[t], out, n_seq, t)
        return out, new_k, new_v

    group_spec = P('dp', None, None)
    cache_spec = P('dp', 'cp', None)
    whole_spec = P()
    return jax.shard_map(
        local_layer,
        mesh=mesh,
        in_specs=(group_spec, P('dp'), cache_spec, cache_spec) + (whole_spec,) * 9,
        out_specs=(group_spec, cache_spec, cache_spec),
        check_vma=False,
    )
```

```python
import functools

import jax
import jax.numpy as jnp
from jax import lax
from jax.experimental import pallas as pl
from jax.experimental.pallas import tpu as pltpu
from jax.sharding import PartitionSpec as P


NORM_EPS = 1e-6
ROPE_BASE = 1.0e4
MASK_FLOOR = -1.0e30
GELU_C = 0.7978845608028654

UNIT = 16
PER_HALF = 128 // UNIT
PIECES = (5, 13, 10, 22)
BASE = (0, 5, 18, 28, 50)
N_PACK = BASE[-1]
N_SIB = 4 * PER_HALF
ROW = 16
BLK = 512
DEPTH = 3
F32 = jnp.float32
BF16 = jnp.bfloat16


def rms_norm(x, gain):
    inv = lax.rsqrt(jnp.mean(x * x, axis=-1, keepdims=True) + NORM_EPS)
    return (x * inv * (1.0 + gain)).astype(BF16)


def rotate(x, cos, sin):
    half = x.shape[-1] // 2
    first, second = x[:, :half], x[:, half:]
    return jnp.concatenate([first * cos - second * sin, second * cos + first * sin], axis=-1)


def gelu_tanh(x):
    return 0.5 * x * (1.0 + jnp.tanh(GELU_C * (x + 0.044715 * (x * x * x))))


def dot(a, b):
    return jnp.dot(a, b, preferred_element_type=F32)


def dot_t(a, b):
    return lax.dot_general(a, b, (((1,), (1,)), ((), ())), preferred_element_type=F32)


def make_plan(start_ref, table, order, length, pos, cnt):
    me = lax.axis_index('cp')
    x_pos, core = me // 2, me % 2
    starts = [start_ref[i] for i in range(16)]
    for i in range(16):
        rank = jnp.int32(0)
        for j in range(16):
            if j != i:
                ahead = (starts[j] <= starts[i]) if j < i else (starts[j] < starts[i])
                rank = rank + ahead.astype(jnp.int32)
        order[rank] = i
        length[rank] = starts[i]
    over = jnp.int32(0)
    for hh in range(2):
        at = jnp.int32(0 if hh == 0 else BASE[2])
        for j in range(8):
            n = jnp.clip((length[j] - 128 * hh + UNIT - 1) // UNIT, 0, PER_HALF)
            pos[hh * 8 + j] = at
            cnt[hh * 8 + j] = n
            at = at + n
            if hh == 0 and j == 1:
                over = over | (at > BASE[1]).astype(jnp.int32)
            if hh == 0 and j == 3:
                over = over | (at > BASE[2]).astype(jnp.int32)
            if hh == 1 and j == 3:
                over = over | (at > BASE[2]).astype(jnp.int32)
        over = over | (at > (BASE[4] if hh == 0 else BASE[3])).astype(jnp.int32)
    for t in range(4):
        for k in range(4):
            xx = x_pos if k < 2 else 1 - x_pos
            cc = core if k % 2 == 0 else 1 - core
            place = 2 * t + (cc + t) % 2
            rank = 8 * (1 - xx) + place
            table[ROW * t + k] = order[rank]
            if k == 0:
                table[ROW * t + 4] = length[rank]
                table[ROW * t + 5] = x_pos
                table[ROW * t + 6] = core
                table[ROW * t + 7] = place
                for hh in range(2):
                    table[ROW * t + 8 + hh] = pos[hh * 8 + place]
                    table[ROW * t + 10 + hh] = jnp.clip((length[rank] - 128 * hh + UNIT - 1) // UNIT, 0, PER_HALF)
    table[64] = over
    return x_pos, core


def pack_kernel(start_ref, ck_ref, cv_ref, table, over_ref, *rest):
    outs = rest[:5]
    order, length, pos, cnt, raw, wide, in_sem, out_sem = rest[5:]
    x_pos, core = make_plan(start_ref, table, order, length, pos, cnt)
    over_ref[0, 0] = table[64]
    d = 1024

    def copies(seq, row, where):
        rows = pl.ds(pl.multiple_of(row, UNIT), UNIT)
        return (
            pltpu.make_async_copy(ck_ref.at[seq, rows, :], raw.at[where, :, pl.ds(0, d)], in_sem.at[where, 0]),
            pltpu.make_async_copy(cv_ref.at[seq, rows, :], raw.at[where, :, pl.ds(d, d)], in_sem.at[where, 1]),
        )

    def each_unit(act):
        for j in range(8):
            @pl.loop(0, PER_HALF)
            def _(u, j=j):
                where = pos[core * 8 + j] + u

                @pl.when((u < cnt[core * 8 + j]) & (where < N_PACK))
                def _():
                    for copy in copies(order[j], u * UNIT, where):
                        act(copy)
        for t in range(4):
            seq = order[8 + 2 * t + (1 - core + t) % 2]

            @pl.loop(0, PER_HALF)
            def _(u, t=t, seq=seq):
                for copy in copies(seq, u * UNIT, N_PACK + t * PER_HALF + u):
                    act(copy)

    sizes = PIECES + (N_SIB,)
    starts = BASE[:4] + (N_PACK,)

    def out_copy(k):
        return pltpu.make_async_copy(wide.at[pl.ds(starts[k], sizes[k])], outs[k], out_sem.at[k])

    @pl.when(x_pos == 0)
    def _():
        each_unit(lambda copy: copy.start())
        each_unit(lambda copy: copy.wait())
        for k in range(5):
            @pl.loop(0, sizes[k])
            def _(u, k=k):
                wide[starts[k] + u] = raw[starts[k] + u].astype(F32)

            out_copy(k).start()
        for k in range(5):
            out_copy(k).wait()


def plan_and_pack(start_pos, cache_k, cache_v):
    any_spec = pl.BlockSpec(memory_space=pl.ANY)
    smem = pl.BlockSpec(memory_space=pltpu.SMEM)
    total = N_PACK + N_SIB
    return pl.pallas_call(
        pack_kernel,
        out_shape=[jax.ShapeDtypeStruct((80,), jnp.int32), jax.ShapeDtypeStruct((1, 1), jnp.int32)]
        + [jax.ShapeDtypeStruct((n, UNIT, 2048), F32) for n in PIECES + (N_SIB,)],
        in_specs=[smem, any_spec, any_spec],
        out_specs=[smem, smem] + [any_spec] * 5,
        scratch_shapes=[
            pltpu.SMEM((16,), jnp.int32),
            pltpu.SMEM((16,), jnp.int32),
            pltpu.SMEM((16,), jnp.int32),
            pltpu.SMEM((16,), jnp.int32),
            pltpu.VMEM((total, UNIT, 2048), BF16),
            pltpu.VMEM((total, UNIT, 2048), F32),
            pltpu.SemaphoreType.DMA((total, 2)),
            pltpu.SemaphoreType.DMA((5,)),
        ],
        compiler_params=pltpu.CompilerParams(vmem_limit_bytes=40 * 2**20),
        cost_estimate=pl.CostEstimate(flops=20_000_000, bytes_accessed=16_000_000, transcendentals=0),
        name="pack",
    )(start_pos, cache_k, cache_v)


def pack_full_kernel(order_ref, ck_ref, cv_ref, out_ref, raw, wide, sem):
    d = 1024

    @pl.loop(0, 8)
    def _(j):
        seq = order_ref[j]
        copies = (
            pltpu.make_async_copy(ck_ref.at[seq], raw.at[:, pl.ds(0, d)], sem.at[0]),
            pltpu.make_async_copy(cv_ref.at[seq], raw.at[:, pl.ds(d, d)], sem.at[1]),
        )
        for copy in copies:
            copy.start()
        for copy in copies:
            copy.wait()
        wide[...] = raw[...].astype(F32)
        out = pltpu.make_async_copy(wide, out_ref.at[j], sem.at[2])
        out.start()
        out.wait()


def pack_full(order, cache_k, cache_v):
    any_spec = pl.BlockSpec(memory_space=pl.ANY)
    return pl.pallas_call(
        pack_full_kernel,
        out_shape=jax.ShapeDtypeStruct((8, 128, 2048), F32),
        in_specs=[pl.BlockSpec(memory_space=pltpu.SMEM), any_spec, any_spec],
        out_specs=any_spec,
        scratch_shapes=[
            pltpu.VMEM((128, 2048), BF16),
            pltpu.VMEM((128, 2048), F32),
            pltpu.SemaphoreType.DMA((3,)),
        ],
        name="pack_full",
    )(order, cache_k, cache_v)


def blank_kernel(*refs):
    pass


def blank(count):
    return pl.pallas_call(
        blank_kernel,
        out_shape=[jax.ShapeDtypeStruct((8, 128, 2048), F32)] * count,
        out_specs=[pl.BlockSpec(memory_space=pl.ANY)] * count,
        name="blank",
    )()


def layer_kernel(n_att, n_ff, n_pieces, slot, tab_ref, over_ref, ga_ref, gm_ref, cos_ref, sin_ref, h_ref, wq_ref, wk_ref,
                 wv_ref, wo_ref, wg_ref, wu_ref, wd_ref, ck_ref, cv_ref, sib_ref, full_ref, fullf_ref, *rest):
    pieces = rest[: 2 * n_pieces]
    out_ref, h_rows, act, acc, stage, hist, ring_a, ring_b, sem, own_sem, ring_sem = rest[2 * n_pieces:]
    base = ROW * slot
    seq, start, x_pos, core = tab_ref[base], tab_ref[base + 4], tab_ref[base + 5], tab_ref[base + 6]
    place = tab_ref[base + 7]
    ovf = over_ref[0] > 0

    def unit_copies(hh, u):
        k = hh * PER_HALF + u
        dst = stage.at[pl.ds(pl.multiple_of(k * UNIT, UNIT), UNIT), :]
        rows = pl.ds(pl.multiple_of(u * UNIT, UNIT), UNIT)
        live = u < tab_ref[base + 10 + hh]
        far = x_pos == 1
        direct = core == hh
        pos = tab_ref[base + 8 + hh] + u
        out = [
            (live & (x_pos == 0) & (core != hh), sib_ref.at[slot * PER_HALF + u]),
            (live & far & ovf & direct, full_ref.at[place, rows, :]),
            (live & far & ovf & jnp.logical_not(direct), fullf_ref.at[place, rows, :]),
        ]
        for p in range(n_pieces):
            here = live & far & jnp.logical_not(ovf) & (pos >= BASE[p]) & (pos < BASE[p + 1])
            idx = jnp.clip(pos - BASE[p], 0, PIECES[p] - 1)
            out.append((here & direct, pieces[2 * p].at[idx]))
            out.append((here & jnp.logical_not(direct), pieces[2 * p + 1].at[idx]))
        return [(c, pltpu.make_async_copy(src, dst, sem.at[k])) for c, src in out]

    def own_copies(hh):
        rows = pl.ds(hh * 128, 128)
        return (
            pltpu.make_async_copy(ck_ref.at[seq], hist.at[rows, pl.ds(0, 1024)], own_sem.at[0]),
            pltpu.make_async_copy(cv_ref.at[seq], hist.at[rows, pl.ds(1024, 1024)], own_sem.at[1]),
        )

    n_step = n_att + n_ff

    def weight_copies(i, kind):
        at = lax.rem(i, DEPTH)
        if kind == 0:
            lo, hi = pl.ds(0, 256), pl.ds(256, 256)
            return [
                pltpu.make_async_copy(wq_ref.at[2 * i], ring_a.at[2 * at, :, lo], ring_sem.at[at, 0]),
                pltpu.make_async_copy(wq_ref.at[2 * i + 1], ring_a.at[2 * at, :, hi], ring_sem.at[at, 1]),
                pltpu.make_async_copy(wk_ref.at[i], ring_a.at[2 * at + 1, :, lo], ring_sem.at[at, 2]),
                pltpu.make_async_copy(wv_ref.at[i], ring_a.at[2 * at + 1, :, hi], ring_sem.at[at, 3]),
                pltpu.make_async_copy(wo_ref.at[pl.ds(i * BLK, BLK), :], ring_b.at[at], ring_sem.at[at, 4]),
            ]
        cols = pl.ds(pl.multiple_of((i - n_att) * BLK, BLK), BLK)
        return [
            pltpu.make_async_copy(wg_ref.at[:, cols], ring_a.at[2 * at], ring_sem.at[at, 0]),
            pltpu.make_async_copy(wu_ref.at[:, cols], ring_a.at[2 * at + 1], ring_sem.at[at, 1]),
            pltpu.make_async_copy(wd_ref.at[cols, :], ring_b.at[at], ring_sem.at[at, 4]),
        ]

    def fetch(i):
        @pl.when(i < n_att)
        def _():
            for copy in weight_copies(i, 0):
                copy.start()

        @pl.when((i >= n_att) & (i < n_step))
        def _():
            for copy in weight_copies(i, 1):
                copy.start()

    row_copy = pltpu.make_async_copy(h_ref.at[seq], h_rows, own_sem.at[2])
    row_copy.start()
    for hh in range(2):
        @pl.when((x_pos == 0) & (core == hh))
        def _(hh=hh):
            for copy in own_copies(hh):
                copy.start()
    for copy in weight_copies(0, 0):
        copy.start()
    for hh in range(2):
        @pl.loop(0, PER_HALF)
        def _(u, hh=hh):
            for cond, copy in unit_copies(hh, u):
                @pl.when(cond)
                def _(copy=copy):
                    copy.start()
    for i in range(1, DEPTH):
        for copy in weight_copies(i, 0):
            copy.start()
    row_copy.wait()
    act[...] = rms_norm(h_rows[...].astype(F32), ga_ref[...].astype(F32))
    acc[...] = h_rows[...].astype(F32)
    for hh in range(2):
        @pl.loop(0, PER_HALF)
        def _(u, hh=hh):
            for cond, copy in unit_copies(hh, u):
                @pl.when(cond)
                def _(copy=copy):
                    copy.wait()

        @pl.when((x_pos == 0) & (core == hh))
        def _(hh=hh):
            for copy in own_copies(hh):
                copy.wait()

        @pl.when((x_pos == 1) | (core != hh))
        def _(hh=hh):
            hist[hh * 128:(hh + 1) * 128, :] = stage[hh * 128:(hh + 1) * 128, :].astype(BF16)

    @pl.loop(0, n_att)
    def _(i):
        at = lax.rem(i, DEPTH)
        for copy in weight_copies(i, 0):
            copy.wait()
        cos, sin = cos_ref[0], sin_ref[0]
        a = act[...]
        off = pl.multiple_of(i * 256, 256)
        row = lax.broadcasted_iota(jnp.int32, (256, 256), 0)
        v_old = jnp.where(row < start, hist[:, pl.ds(off + 1024, 256)], jnp.zeros((), BF16))
        kv = dot(a, ring_a[2 * at + 1])
        k_all = jnp.concatenate([hist[:, pl.ds(off, 256)], rotate(kv[:, :256], cos, sin).astype(BF16)], axis=0)
        v_all = jnp.concatenate([v_old, kv[:, 256:].astype(BF16)], axis=0)
        qq = dot(a, ring_a[2 * at])
        qs = [(rotate(qq[:, j * 256:(j + 1) * 256], cos, sin) * 0.0625).astype(BF16) for j in range(2)]
        row = lax.broadcasted_iota(jnp.int32, (256, 512), 0)
        col = lax.broadcasted_iota(jnp.int32, (256, 512), 1)
        ok = (col < start) | ((col >= 256) & (col - 256 <= row))
        scores = [jnp.where(ok, dot_t(q, k_all), MASK_FLOOR) for q in qs]
        tops = [jnp.max(s, axis=-1, keepdims=True) for s in scores]
        probs = [jnp.exp(s - top) for s, top in zip(scores, tops)]
        dens = [jnp.sum(p, axis=-1, keepdims=True) for p in probs]
        nums = [dot(p.astype(BF16), v_all) for p in probs]
        heads = [(num / den).astype(BF16) for num, den in zip(nums, dens)]
        acc[...] += dot(jnp.concatenate(heads, axis=-1), ring_b[at])
        fetch(i + DEPTH)

    res = acc[...].astype(BF16).astype(F32)
    act[...] = rms_norm(res, gm_ref[...].astype(F32))
    acc[...] = res

    @pl.loop(n_att, n_step)
    def _(i):
        at = lax.rem(i, DEPTH)
        for copy in weight_copies(i, 1):
            copy.wait()
        c = act[...]
        mid = (gelu_tanh(dot(c, ring_a[2 * at])) * dot(c, ring_a[2 * at + 1])).astype(BF16)
        acc[...] += dot(mid, ring_b[at])
        fetch(i + DEPTH)

    acc[...] = acc[...].astype(BF16).astype(F32)
    done = pltpu.make_async_copy(acc, out_ref, own_sem.at[3])
    done.start()
    done.wait()


def run_layer(slot, table, over, hidden, ga, gm, cos, sin, wq, wk, wv, wo, wg, wu, wd, ck, cv, sib, full, fullf, pieces):
    n_ff = wg.shape[1] // BLK
    n_pieces = len(pieces) // 2
    any_spec = pl.BlockSpec(memory_space=pl.ANY)
    smem = pl.BlockSpec(memory_space=pltpu.SMEM)
    vmem = pl.BlockSpec(memory_space=pltpu.VMEM)
    d = hidden.shape[2]
    flops = 2 * 256 * d * (2048 * 2 + 1024 * 2 + 3 * wg.shape[1]) + 1_100_000_000
    table_spec = pl.BlockSpec((1, 256, 128), lambda i: (slot, 0, 0))
    return pl.pallas_call(
        functools.partial(layer_kernel, 4, n_ff, n_pieces, slot),
        out_shape=jax.ShapeDtypeStruct((256, d), F32),
        grid=(1,),
        in_specs=[smem, smem, vmem, vmem, table_spec, table_spec] + [any_spec] * (13 + 2 * n_pieces),
        out_specs=any_spec,
        scratch_shapes=[
            pltpu.VMEM((256, d), BF16),
            pltpu.VMEM((256, d), BF16),
            pltpu.VMEM((256, d), F32),
            pltpu.VMEM((256, 2048), F32),
            pltpu.VMEM((256, 2048), BF16),
            pltpu.VMEM((2 * DEPTH, d, BLK), BF16),
            pltpu.VMEM((DEPTH, BLK, d), BF16),
            pltpu.SemaphoreType.DMA((2 * PER_HALF,)),
            pltpu.SemaphoreType.DMA((4,)),
            pltpu.SemaphoreType.DMA((DEPTH, 5)),
        ],
        compiler_params=pltpu.CompilerParams(vmem_limit_bytes=60 * 2**20),
        cost_estimate=pl.CostEstimate(flops=flops, bytes_accessed=160_000_000, transcendentals=0),
    )(table, over, ga, gm, cos, sin, hidden, wq, wk, wv, wo, wg, wu, wd, ck, cv, sib, full, fullf, *pieces)


def window_kernel(sc_ref, h_ref, ga_ref, cos_ref, sin_ref, wk_ref, wv_ref, ck_ref, cv_ref, ok_ref, ov_ref):
    step = pl.program_id(0)
    lo = lax.axis_index('cp') * 128
    a_rows, inside = [], []
    for j in range(2):
        first = lo - sc_ref[2 * step + j]
        want = first + lax.broadcasted_iota(jnp.int32, (128, 256), 0)
        have = lax.broadcasted_iota(jnp.int32, (128, 256), 1)
        pick = jnp.where(want == have, 1.0, 0.0).astype(BF16)
        a_rows.append(dot(pick, h_ref[j]))
        idx = first + lax.broadcasted_iota(jnp.int32, (128, 256), 0)
        inside.append((idx >= 0) & (idx < 256))
    a = rms_norm(jnp.concatenate(a_rows, axis=0), ga_ref[...].astype(F32))
    cos = jnp.concatenate([cos_ref[...]] * 2, axis=0)
    sin = jnp.concatenate([sin_ref[...]] * 2, axis=0)
    for g in range(4):
        k = rotate(dot(a, wk_ref[g]), cos, sin).astype(BF16)
        v = dot(a, wv_ref[g]).astype(BF16)
        cols = slice(g * 256, (g + 1) * 256)
        for j in range(2):
            rows = slice(j * 128, (j + 1) * 128)
            ok_ref[j, :, cols] = jnp.where(inside[j], k[rows], ck_ref[j, :, cols])
            ov_ref[j, :, cols] = jnp.where(inside[j], v[rows], cv_ref[j, :, cols])


def write_windows(scalars, hidden, ga, cos, sin, wk, wv, cache_k, cache_v):
    n_seq, rows, width = cache_k.shape
    d = hidden.shape[2]
    one = pl.Buffered(1)
    cache_spec = pl.BlockSpec((2, rows, width), lambda i, sc: (i, 0, 0))
    return pl.pallas_call(
        window_kernel,
        out_shape=[jax.ShapeDtypeStruct(cache_k.shape, BF16)] * 2,
        grid_spec=pltpu.PrefetchScalarGridSpec(
            num_scalar_prefetch=1,
            grid=(n_seq // 2,),
            in_specs=[
                pl.BlockSpec((2, 256, d), lambda i, sc: (i, 0, 0)),
                pl.BlockSpec((1, d), lambda i, sc: (0, 0), pipeline_mode=one),
                pl.BlockSpec((rows, 128), lambda i, sc: (0, 0), pipeline_mode=one),
                pl.BlockSpec((rows, 128), lambda i, sc: (0, 0), pipeline_mode=one),
                pl.BlockSpec((4, d, 256), lambda i, sc: (0, 0, 0), pipeline_mode=one),
                pl.BlockSpec((4, d, 256), lambda i, sc: (0, 0, 0), pipeline_mode=one),
                cache_spec,
                cache_spec,
            ],
            out_specs=[cache_spec, cache_spec],
        ),
        compiler_params=pltpu.CompilerParams(vmem_limit_bytes=56 * 2**20),
        cost_estimate=pl.CostEstimate(flops=2 * n_seq * rows * d * 2 * width, bytes_accessed=60_000_000, transcendentals=0),
        name="cache_window",
    )(scalars, hidden, ga, cos, sin, wk, wv, cache_k, cache_v)


def place_kernel(slot, n_part, blk, tab_ref, *rest):
    parts = rest[:n_part]
    out_ref, narrow, sem = rest[-3:]
    step, steps = pl.program_id(0), pl.num_programs(0)
    buf = lax.rem(step, 2)

    def copy(k, at, b):
        rows = pl.ds(pl.multiple_of(at * blk, blk), blk)
        return pltpu.make_async_copy(narrow.at[b, k], out_ref.at[tab_ref[ROW * slot + k], rows, :], sem.at[b, k])

    for k in range(n_part):
        @pl.when(step >= 2)
        def _(k=k):
            copy(k, step - 2, buf).wait()

        narrow[buf, k] = parts[k][...].astype(BF16)
        copy(k, step, buf).start()

    @pl.when(step == steps - 1)
    def _():
        for k in range(n_part):
            copy(k, step - 1, 1 - buf).wait()
            copy(k, step, buf).wait()


def place_rows(table, parts, out, n_seq, slot, blk=64):
    rows, d = parts[0].shape
    any_spec = pl.BlockSpec(memory_space=pl.ANY)
    n_part = len(parts)
    args = [table, *parts]
    in_specs = [pl.BlockSpec((blk, d), lambda i, tab: (i, 0))] * n_part
    aliases = {}
    if out is not None:
        in_specs.append(any_spec)
        aliases = {n_part + 1: 0}
        args.append(out)
    return pl.pallas_call(
        functools.partial(place_kernel, slot, n_part, blk),
        out_shape=jax.ShapeDtypeStruct((n_seq, rows, d), BF16),
        grid_spec=pltpu.PrefetchScalarGridSpec(
            num_scalar_prefetch=1,
            grid=(rows // blk,),
            in_specs=in_specs,
            out_specs=any_spec,
            scratch_shapes=[pltpu.VMEM((2, n_part, blk, d), BF16), pltpu.SemaphoreType.DMA((2, n_part))],
        ),
        input_output_aliases=aliases,
        cost_estimate=pl.CostEstimate(flops=10_000_000, bytes_accessed=n_part * rows * d * 6, transcendentals=0),
    )(*args)


def solution(mesh):
    d2d = [(0, 1), (1, 0), (2, 3), (3, 2)]
    cross = [(0, 2), (1, 3), (2, 0), (3, 1)]

    def send(x, pairs, axis='cp'):
        return lax.ppermute(x, axis, pairs)

    def body(hidden, start_pos, cache_k, cache_v, w_q, w_k, w_v, w_o, w_gate, w_up, w_down, norm_attn, norm_mlp):
        n_seq, chunk_len, d = hidden.shape
        shard_len = cache_k.shape[1]
        i32 = jnp.int32
        me = lax.axis_index('cp').astype(i32)

        table, over, p1, p2, p3a, p3b, sib_src = plan_and_pack(start_pos, cache_k, cache_v)
        over = jnp.maximum(over, send(over, [(0, 1), (1, 0)], 'dp'))[0]
        p1d = send(p1, [(0, 2)])
        sib = send(sib_src, [(0, 1), (1, 0)])
        p1f = send(p1d, [(2, 3)])
        p2d = send(p2, [(0, 2)])
        p2f = send(p2d, [(2, 3)])
        p3ad = send(p3a, [(0, 2), (1, 3)])
        p3af = send(p3ad, [(2, 3), (3, 2)])
        p3bd = send(p3b, [(0, 2)])
        p3bf = send(p3bd, [(2, 3)])

        def send_all(_):
            sid = jnp.arange(n_seq, dtype=i32)
            before = (start_pos[None, :] < start_pos[:, None]) | (
                (start_pos[None, :] == start_pos[:, None]) & (sid[None, :] < sid[:, None]))
            rank = jnp.sum(before.astype(i32), axis=1)
            order = jnp.sum((rank[None, :] == sid[:, None]).astype(i32) * sid[None, :], axis=1)
            got = lax.ppermute(pack_full(order, cache_k, cache_v), 'cp', [(0, 2), (1, 3)])
            return got, lax.ppermute(got, 'cp', [(2, 3), (3, 2)])

        full, full_f = lax.cond(over[0] > 0, send_all, lambda _: tuple(blank(2)), 0)

        head_dim = w_q.shape[2]
        inv_freq = ROPE_BASE ** (-2.0 * jnp.arange(head_dim // 2, dtype=F32) / head_dim)
        my_len = jnp.stack([table[ROW * t + 4] for t in range(4)])
        own_pos = my_len[:, None] + jnp.arange(chunk_len, dtype=i32)[None, :]
        angles = own_pos.astype(F32)[:, :, None] * inv_freq
        cos, sin = jnp.cos(angles), jnp.sin(angles)
        win_lo = me * shard_len
        win_angles = (win_lo + jnp.arange(shard_len, dtype=i32)).astype(F32)[:, None] * inv_freq
        win_cos, win_sin = jnp.cos(win_angles), jnp.sin(win_angles)
        wq = w_q.transpose(1, 0, 2)
        wk = w_k.transpose(1, 0, 2)
        wv = w_v.transpose(1, 0, 2)
        wo = w_o.reshape(-1, d)
        ga, gm = norm_attn[None, :], norm_mlp[None, :]

        parts = []
        tab = table
        for t in range(4):
            pieces = (p1d, p1f, p2d, p2f, p3ad, p3af, p3bd, p3bf)[: (2, 4, 8, 8)[t]]
            own = run_layer(t, tab, over, hidden, ga, gm, cos, sin, wq, wk, wv, wo, w_gate, w_up, w_down,
                            cache_k, cache_v, sib, full, full_f, pieces)
            tab, own = lax.optimization_barrier((tab, own))
            crs = send(own, cross)
            near = send(own, d2d)
            dia = send(crs, d2d)
            parts.append((own, near, crs, dia))
        start_late, _ = lax.optimization_barrier((start_pos, tab))
        new_k, new_v = write_windows(start_late, hidden, ga, win_cos, win_sin, wk, wv, cache_k, cache_v)
        out = None
        for t in range(3):
            out = place_rows(tab, parts[t], out, n_seq, t)
        out = place_rows(tab, parts[3], out, n_seq, 3)
        return out, new_k, new_v

    group_spec = P('dp', None, None)
    cache_spec = P('dp', 'cp', None)
    whole_spec = P()
    return jax.shard_map(
        body,
        mesh=mesh,
        in_specs=(group_spec, P('dp'), cache_spec, cache_spec) + (whole_spec,) * 9,
        out_specs=(group_spec, cache_spec, cache_spec),
        check_vma=False,
    )
```

```python
import functools
import math

import jax
import jax.numpy as jnp
from jax import lax
from jax.experimental import pallas as pl
from jax.experimental.pallas import tpu as pltpu
from jax.sharding import PartitionSpec as P


NORM_EPS = 1e-6
ROPE_BASE = 1.0e4
MASK_FLOOR = -1.0e30
GELU_C = 0.7978845608028654

UNIT = 16
HALF = 128
HEAD = 2 * HALF
WIDE = 4 * HEAD
KV_WIDE = 2 * WIDE
PER_HALF = HALF // UNIT
A_UNITS, C_UNITS = 10, 5
WHOLE_B, WHOLE_D = (3, 4, 7), (5, 6)
A_ROWS, C_ROWS = A_UNITS * UNIT, C_UNITS * UNIT
B_ROWS, D_ROWS, S_ROWS = len(WHOLE_B) * HALF, len(WHOLE_D) * HALF, 4 * HALF
ROW = 16
OUT_BLK = 512
BLK = 768
VMEM_BESIDE = 48_100_000
VMEM_ALL = 66_900_000
DEPTH = 2
DEPTH_B = 3
F32 = jnp.float32
BF16 = jnp.bfloat16


def rms_norm(x, gain):
    inv = lax.rsqrt(jnp.mean(x * x, axis=-1, keepdims=True) + NORM_EPS)
    return (x * inv * (1.0 + gain)).astype(BF16)


def rotate(x, cos, sin):
    half = x.shape[-1] // 2
    first, second = x[:, :half], x[:, half:]
    return jnp.concatenate([first * cos - second * sin, second * cos + first * sin], axis=-1)


def gelu_tanh(x):
    return 0.5 * x * (1.0 + jnp.tanh(GELU_C * (x + 0.044715 * (x * x * x))))


def dot(a, b):
    return jnp.dot(a, b, preferred_element_type=F32)


def dot_t(a, b):
    return lax.dot_general(a, b, (((1,), (1,)), ((), ())), preferred_element_type=F32)


def sort_lengths(start_ref, order, length):
    starts = [start_ref[i] for i in range(16)]
    for i in range(16):
        rank = jnp.int32(0)
        for j in range(16):
            if j != i:
                ahead = (starts[j] <= starts[i]) if j < i else (starts[j] < starts[i])
                rank = rank + ahead.astype(jnp.int32)
        order[rank] = i
        length[rank] = starts[i]


def place_units(length, pos, cnt):
    over = jnp.int32(0)
    for half, places, room in ((0, (0,), 0), (0, (1, 2), A_UNITS), (1, (0, 1, 2, 3), 0), (1, (4, 7), C_UNITS), (1, (5, 6), C_UNITS)):
        at = jnp.int32(0)
        for j in places:
            n = jnp.clip((length[j] - half * HALF + UNIT - 1) // UNIT, 0, PER_HALF)
            pos[half * 8 + j] = at
            cnt[half * 8 + j] = n
            at = at + n
        over = over | (at > room).astype(jnp.int32)
    return over


def make_plan(start_ref, table, order, length, pos, cnt):
    me = lax.axis_index('cp')
    x_pos, core = me // 2, me % 2
    sort_lengths(start_ref, order, length)
    over = place_units(length, pos, cnt)
    for t in range(4):
        for k in range(4):
            xx = x_pos if k < 2 else 1 - x_pos
            cc = core if k % 2 == 0 else 1 - core
            place = 2 * t + (cc + t) % 2
            rank = 8 * (1 - xx) + place
            table[ROW * t + k] = order[rank]
            if k == 0:
                table[ROW * t + 4] = length[rank]
                table[ROW * t + 5] = x_pos
                table[ROW * t + 6] = core
                table[ROW * t + 7] = place
                for half in range(2):
                    table[ROW * t + 8 + half] = pos[half * 8 + place]
                    table[ROW * t + 10 + half] = jnp.clip((length[rank] - HALF * half + UNIT - 1) // UNIT, 0, PER_HALF)
    table[64] = over
    return x_pos, core, over


def pack_kernel(start_ref, ck_ref, cv_ref, ga_ref, gm_ref, table, over_ref, cos_ref, sin_ref, ga_out, gm_out, *rest):
    outs = rest[:6]
    order, length, pos, cnt, raw, wide, in_sem, out_sem = rest[6:]
    x_pos, core, over = make_plan(start_ref, table, order, length, pos, cnt)
    over_ref[0] = over
    first = dict(A=0, B=A_ROWS, D=A_ROWS + B_ROWS, E=0, O=C_ROWS, S=A_ROWS + B_ROWS + D_ROWS)
    size = dict(A=A_ROWS, B=B_ROWS, D=D_ROWS, E=C_ROWS, O=C_ROWS, S=S_ROWS)

    def copies(seq, row, to, rows, sem):
        return [pltpu.make_async_copy(src.at[seq, pl.ds(row, rows), :], raw.at[pl.ds(to, rows), pl.ds(side * WIDE, WIDE)],
                                      in_sem.at[sem, side]) for side, src in enumerate((ck_ref, cv_ref))]

    def units(half, j, to, sem, act):
        @pl.loop(0, PER_HALF)
        def _(u):
            at = pos[half * 8 + j] + u

            @pl.when((u < cnt[half * 8 + j]) & (at < (C_UNITS if half else A_UNITS)))
            def _():
                row = pl.multiple_of(u * UNIT, UNIT)
                for copy in copies(order[j], row, pl.multiple_of(to + at * UNIT, UNIT), UNIT, sem + at):
                    act(copy)

    def each(act):
        @pl.when(core == 0)
        def _():
            for j in (1, 2):
                units(0, j, first["A"], 0, act)

        @pl.when(core == 1)
        def _():
            for j in (4, 7):
                units(1, j, first["E"], 0, act)
            for j in (5, 6):
                units(1, j, first["O"], C_UNITS, act)

        for t in range(4):
            seq = order[8 + 2 * t + (1 - core + t) % 2]
            for copy in copies(seq, 0, first["S"] + t * HALF, HALF, A_UNITS + t):
                act(copy)

        @pl.when(core == 0)
        def _():
            for k, j in enumerate(WHOLE_B + WHOLE_D):
                for copy in copies(order[j], 0, first["B"] + k * HALF, HALF, A_UNITS + 4 + k):
                    act(copy)

    def out_copy(k, name):
        return pltpu.make_async_copy(wide.at[pl.ds(first[name], size[name]), :], outs[k], out_sem.at[k])

    def widen(k, name):
        @pl.loop(0, size[name] // UNIT)
        def _(u):
            rows = pl.ds(pl.multiple_of(first[name] + u * UNIT, UNIT), UNIT)
            wide[rows, :] = raw[rows, :].astype(F32)

        out_copy(k, name).start()

    @pl.when(x_pos == 0)
    def _():
        each(lambda copy: copy.start())

    ga_out[...] = ga_ref[...].astype(F32).reshape(ga_out.shape)
    gm_out[...] = gm_ref[...].astype(F32).reshape(gm_out.shape)
    half = cos_ref.shape[1]
    freq = lax.broadcasted_iota(jnp.int32, (1, half), 1).astype(F32)
    inv_freq = jnp.exp(freq * (-2.0 / (2 * half) * math.log(ROPE_BASE)))
    big = (16 * lax.broadcasted_iota(jnp.int32, (32, half), 0)).astype(F32) * inv_freq
    small = lax.broadcasted_iota(jnp.int32, (16, half), 0).astype(F32) * inv_freq
    cos_a, sin_a, cos_b, sin_b = jnp.cos(big), jnp.sin(big), jnp.cos(small), jnp.sin(small)
    for r in range(32):
        rows = slice(16 * r, 16 * r + 16)
        ca, sa = cos_a[r:r + 1], sin_a[r:r + 1]
        cos_ref[rows, :] = ca * cos_b - sa * sin_b
        sin_ref[rows, :] = sa * cos_b + ca * sin_b

    @pl.when(x_pos == 0)
    def _():
        each(lambda copy: copy.wait())

        @pl.when(core == 0)
        def _():
            widen(0, "A")
            widen(5, "S")
            widen(1, "B")
            widen(2, "D")
            for k, name in enumerate("ABD"):
                out_copy(k, name).wait()

        @pl.when(core == 1)
        def _():
            widen(5, "S")
            widen(3, "E")
            widen(4, "O")
            for k, name in enumerate("EO"):
                out_copy(3 + k, name).wait()

        out_copy(5, "S").wait()


def plan_and_pack(start_pos, cache_k, cache_v, ga, gm):
    any_spec = pl.BlockSpec(memory_space=pl.ANY)
    smem = pl.BlockSpec(memory_space=pltpu.SMEM)
    vmem = pl.BlockSpec(memory_space=pltpu.VMEM)
    total = A_ROWS + B_ROWS + D_ROWS + S_ROWS
    n_copy = A_UNITS + 4 + len(WHOLE_B + WHOLE_D)
    return pl.pallas_call(
        pack_kernel,
        out_shape=[jax.ShapeDtypeStruct((80,), jnp.int32), jax.ShapeDtypeStruct((1,), jnp.int32)]
        + [jax.ShapeDtypeStruct((2 * HEAD, HALF), F32)] * 2 + [jax.ShapeDtypeStruct((1, ga.shape[0]), F32)] * 2
        + [pltpu.HBM((n, KV_WIDE), F32) for n in (A_ROWS, B_ROWS, D_ROWS, C_ROWS, C_ROWS, S_ROWS)],
        in_specs=[smem, any_spec, any_spec, vmem, vmem],
        out_specs=[smem, smem] + [vmem] * 4 + [any_spec] * 6,
        scratch_shapes=[pltpu.SMEM((16,), jnp.int32)] * 4 + [
            pltpu.VMEM((total, KV_WIDE), BF16),
            pltpu.VMEM((total, KV_WIDE), F32),
            pltpu.SemaphoreType.DMA((n_copy, 2)),
            pltpu.SemaphoreType.DMA((6,)),
        ],
        compiler_params=pltpu.CompilerParams(vmem_limit_bytes=VMEM_ALL),
        cost_estimate=pl.CostEstimate(flops=20_000_000, bytes_accessed=16_000_000, transcendentals=0),
        name="pack",
    )(start_pos, cache_k, cache_v, ga, gm)


def pack_full_kernel(order_ref, ck_ref, cv_ref, out_ref, raw, wide, sem):
    d = WIDE

    @pl.loop(0, 8)
    def _(j):
        seq = order_ref[j]
        copies = (
            pltpu.make_async_copy(ck_ref.at[seq], raw.at[:, pl.ds(0, d)], sem.at[0]),
            pltpu.make_async_copy(cv_ref.at[seq], raw.at[:, pl.ds(d, d)], sem.at[1]),
        )
        for copy in copies:
            copy.start()
        for copy in copies:
            copy.wait()
        wide[...] = raw[...].astype(F32)
        out = pltpu.make_async_copy(wide, out_ref.at[j], sem.at[2])
        out.start()
        out.wait()


def pack_full(order, cache_k, cache_v):
    any_spec = pl.BlockSpec(memory_space=pl.ANY)
    return pl.pallas_call(
        pack_full_kernel,
        out_shape=jax.ShapeDtypeStruct((8, HALF, KV_WIDE), F32),
        in_specs=[pl.BlockSpec(memory_space=pltpu.SMEM), any_spec, any_spec],
        out_specs=any_spec,
        scratch_shapes=[
            pltpu.VMEM((HALF, KV_WIDE), BF16),
            pltpu.VMEM((HALF, KV_WIDE), F32),
            pltpu.SemaphoreType.DMA((3,)),
        ],
        name="pack_full",
    )(order, cache_k, cache_v)


def blank_kernel(*refs):
    pass


def blank(count):
    return pl.pallas_call(
        blank_kernel,
        out_shape=[jax.ShapeDtypeStruct((8, HALF, KV_WIDE), F32)] * count,
        out_specs=[pl.BlockSpec(memory_space=pl.ANY)] * count,
        name="blank",
    )()


W_CHUNK = 384
W_SLOTS = 3


def heads_kernel(q_ref, k_ref, v_ref, out_ref, raw_q, raw_k, raw_v, sem):
    n_chunk = q_ref.shape[0] // W_CHUNK

    def copies(i, b):
        rows = pl.ds(pl.multiple_of(i * W_CHUNK, W_CHUNK), W_CHUNK)
        return [pltpu.make_async_copy(src.at[rows], dst.at[b], sem.at[b, j])
                for j, (src, dst) in enumerate(((q_ref, raw_q), (k_ref, raw_k), (v_ref, raw_v)))]

    def sorter(n_head):
        per = HEAD // n_head
        want = lax.broadcasted_iota(jnp.int32, (HEAD, HEAD), 0)
        have = lax.broadcasted_iota(jnp.int32, (HEAD, HEAD), 1)
        return jnp.where((want % per) * n_head + want // per == have, 1.0, 0.0).astype(BF16)

    for i in range(W_SLOTS):
        for copy in copies(i, i):
            copy.start()
    sort8, sort4 = sorter(8), sorter(4)

    @pl.loop(0, n_chunk)
    def _(i):
        b = lax.rem(i, W_SLOTS)
        for copy in copies(i, b):
            copy.wait()
        for part in range(W_CHUNK // 64):
            to = pl.multiple_of(i * W_CHUNK, W_CHUNK) + part * 64
            for raw, n_head, sort, first in ((raw_q, 8, sort8, 0), (raw_k, 4, sort4, 2), (raw_v, 4, sort4, 3)):
                per = HEAD // n_head
                for sub in range(64 // per):
                    block = raw[b, part * 64 + sub * per:part * 64 + (sub + 1) * per].reshape(HEAD, HEAD)
                    moved = dot(sort, block).astype(BF16)
                    for h in range(n_head):
                        g, col = (h // 2, h % 2) if n_head == 8 else (h, first)
                        out_ref[g, pl.ds(to + sub * per, per), col * HEAD:(col + 1) * HEAD] = moved[h * per:(h + 1) * per]

        @pl.when(i + W_SLOTS < n_chunk)
        def _():
            for copy in copies(i + W_SLOTS, b):
                copy.start()


def split_heads(w_q, w_k, w_v):
    d = w_q.shape[0]
    any_spec = pl.BlockSpec(memory_space=pl.ANY)
    return pl.pallas_call(
        heads_kernel,
        out_shape=pltpu.VMEM((4, d, WIDE), BF16),
        in_specs=[any_spec] * 3,
        out_specs=pl.BlockSpec(memory_space=pltpu.VMEM),
        scratch_shapes=[
            pltpu.VMEM((W_SLOTS, W_CHUNK, 8, HEAD), BF16),
            pltpu.VMEM((W_SLOTS, W_CHUNK, 4, HEAD), BF16),
            pltpu.VMEM((W_SLOTS, W_CHUNK, 4, HEAD), BF16),
            pltpu.SemaphoreType.DMA((W_SLOTS, 3)),
        ],
        compiler_params=pltpu.CompilerParams(vmem_limit_bytes=VMEM_BESIDE),
        cost_estimate=pl.CostEstimate(flops=5_000_000_000, bytes_accessed=20_000_000, transcendentals=0),
        name="heads",
    )(w_q, w_k, w_v)


def layer_kernel(n_att, n_ff, n_out, slot, tab_ref, over_ref, ga_ref, gm_ref, cos_ref, sin_ref, wh_ref, h_ref, wo_ref,
                 wg_ref, wu_ref, wd_ref, ck_ref, cv_ref, sib_ref, full_ref, fullf_ref, *rest):
    refs = iter(rest)
    a_ref, b_ref, d_ref, e_ref, o_ref = [next(refs) for _ in range(5)]
    if slot > 0:
        next(refs)
    out_refs = [next(refs) for _ in range(n_out)]
    final_ref, h_rows, act, acc, stage, hist, ring_a, ring_b, sem, own_sem, ring_sem, out_sem = refs
    base = ROW * slot
    seq, start, x_pos, core = tab_ref[base], tab_ref[base + 4], tab_ref[base + 5], tab_ref[base + 6]
    place = tab_ref[base + 7]
    ovf = over_ref[0] > 0
    far = x_pos == 1

    def whole_copies(half):
        to = stage.at[pl.ds(half * HALF, HALF), :]
        fits = far & jnp.logical_not(ovf)
        found = [
            ((x_pos == 0) & (core != half), sib_ref.at[pl.ds(slot * HALF, HALF), :]),
            (far & ovf & (core == half), full_ref.at[place]),
            (far & ovf & (core != half), fullf_ref.at[place]),
        ]
        if half == 0:
            for who, places, ref in ((0, WHOLE_B, b_ref), (1, WHOLE_D, d_ref)):
                mine = 2 * slot + (who + slot) % 2
                if mine in places:
                    found.append((fits & (core == who), ref.at[pl.ds(places.index(mine) * HALF, HALF), :]))
        return [(c, pltpu.make_async_copy(src, to, sem.at[half])) for c, src in found]

    def unit_copies(half, u):
        at = pl.multiple_of((tab_ref[base + 8 + half] + u) * UNIT, UNIT)
        live = far & jnp.logical_not(ovf) & (u < tab_ref[base + 10 + half])
        to = stage.at[pl.ds(pl.multiple_of(half * HALF + u * UNIT, UNIT), UNIT), :]
        if half == 0:
            found = [(live & (core == 1), a_ref)] if slot < 2 else []
        else:
            found = [(live & (core == who), ref) for who, ref in ((0, e_ref), (1, o_ref))] if slot >= 2 else []
        return [(c, pltpu.make_async_copy(src.at[pl.ds(at, UNIT), :], to, sem.at[2 + u])) for c, src in found]

    def own_copies(half):
        rows = pl.ds(half * HALF, HALF)
        return (
            pltpu.make_async_copy(ck_ref.at[seq], hist.at[rows, pl.ds(0, WIDE)], own_sem.at[0]),
            pltpu.make_async_copy(cv_ref.at[seq], hist.at[rows, pl.ds(WIDE, WIDE)], own_sem.at[1]),
        )

    def history(act_on):
        for half in range(2):
            for cond, copy in whole_copies(half):
                @pl.when(cond)
                def _(copy=copy):
                    act_on(copy)

            @pl.when((x_pos == 0) & (core == half))
            def _(half=half):
                for copy in own_copies(half):
                    act_on(copy)

        packed = 0 if slot < 2 else 1

        @pl.loop(0, PER_HALF)
        def _(u):
            for cond, copy in unit_copies(packed, u):
                @pl.when(cond)
                def _(copy=copy):
                    act_on(copy)

    def up_copies(j):
        at = lax.rem(j, DEPTH)
        cols = pl.ds(pl.multiple_of(j * BLK, BLK), BLK)
        return [
            pltpu.make_async_copy(wg_ref.at[:, cols], ring_a.at[2 * at], ring_sem.at[at, 0]),
            pltpu.make_async_copy(wu_ref.at[:, cols], ring_a.at[2 * at + 1], ring_sem.at[at, 1]),
        ]

    def out_copy(i):
        at = lax.rem(i, DEPTH_B)
        rows = pl.ds(pl.multiple_of(i * OUT_BLK, OUT_BLK), OUT_BLK)
        return pltpu.make_async_copy(wo_ref.at[rows, :], ring_b.at[at, pl.ds(0, OUT_BLK), :], ring_sem.at[at, 2])

    def down_copy(j):
        at = lax.rem(j + n_att, DEPTH_B)
        rows = pl.ds(pl.multiple_of(j * BLK, BLK), BLK)
        return pltpu.make_async_copy(wd_ref.at[rows, :], ring_b.at[at], ring_sem.at[at, 2])

    row_copy = pltpu.make_async_copy(h_ref.at[seq], h_rows, own_sem.at[2])
    row_copy.start()
    history(lambda copy: copy.start())
    for i in range(DEPTH_B):
        out_copy(i).start()
    for j in range(DEPTH):
        for copy in up_copies(j):
            copy.start()
    row_copy.wait()
    act[...] = rms_norm(h_rows[...].astype(F32), ga_ref[...])
    acc[...] = h_rows[...].astype(F32)
    history(lambda copy: copy.wait())
    for half in range(2):
        @pl.when((x_pos == 1) | (core != half))
        def _(half=half):
            rows = pl.ds(half * HALF, HALF)
            hist[rows, :] = stage[rows, :].astype(BF16)

    @pl.loop(0, n_att)
    def _(i):
        out_copy(i).wait()
        cos, sin = cos_ref[pl.ds(start, HEAD), :], sin_ref[pl.ds(start, HEAD), :]
        a = act[...]
        off = pl.multiple_of(i * HEAD, HEAD)
        row = lax.broadcasted_iota(jnp.int32, (HEAD, HEAD), 0)
        v_old = jnp.where(row < start, hist[:, pl.ds(off + WIDE, HEAD)], jnp.zeros((), BF16))
        qkv = dot(a, wh_ref[i])
        kv = qkv[:, 512:]
        k_all = jnp.concatenate([hist[:, pl.ds(off, HEAD)], rotate(kv[:, :HEAD], cos, sin).astype(BF16)], axis=0)
        v_all = jnp.concatenate([v_old, kv[:, HEAD:].astype(BF16)], axis=0)
        qs = [(rotate(qkv[:, j * HEAD:(j + 1) * HEAD], cos, sin) * 0.0625).astype(BF16) for j in range(2)]
        row = lax.broadcasted_iota(jnp.int32, (HEAD, 512), 0)
        col = lax.broadcasted_iota(jnp.int32, (HEAD, 512), 1)
        ok = (col < start) | ((col >= HEAD) & (col - HEAD <= row))
        scores = [jnp.where(ok, dot_t(q, k_all), MASK_FLOOR) for q in qs]
        tops = [jnp.max(s, axis=-1, keepdims=True) for s in scores]
        probs = [jnp.exp(s - top) for s, top in zip(scores, tops)]
        dens = [jnp.sum(p, axis=-1, keepdims=True) for p in probs]
        nums = [dot(p.astype(BF16), v_all) for p in probs]
        heads = [(num / den).astype(BF16) for num, den in zip(nums, dens)]
        acc[...] += dot(jnp.concatenate(heads, axis=-1), ring_b[lax.rem(i, DEPTH_B), :OUT_BLK, :])

        @pl.when(i + DEPTH_B < n_att)
        def _():
            out_copy(i + DEPTH_B).start()

        @pl.when(i + DEPTH_B >= n_att)
        def _():
            down_copy(i + DEPTH_B - n_att).start()

    res = acc[...].astype(BF16).astype(F32)
    act[...] = rms_norm(res, gm_ref[...])
    acc[...] = res

    @pl.loop(0, n_ff)
    def _(j):
        at = lax.rem(j, DEPTH)
        for copy in up_copies(j):
            copy.wait()
        down_copy(j).wait()
        c = act[...]
        mid = (gelu_tanh(dot(c, ring_a[2 * at])) * dot(c, ring_a[2 * at + 1])).astype(BF16)
        acc[...] += dot(mid, ring_b[lax.rem(j + n_att, DEPTH_B)])

        @pl.when(j + DEPTH < n_ff)
        def _():
            for copy in up_copies(j + DEPTH):
                copy.start()

        @pl.when(j + DEPTH_B < n_ff)
        def _():
            down_copy(j + DEPTH_B).start()

    size = acc.shape[0] // n_out
    copies = []
    for k in range(n_out):
        rows = pl.ds(k * size, size)
        rounded = acc[rows, :].astype(BF16)
        act[rows, :] = rounded
        acc[rows, :] = rounded.astype(F32)
        copies.append(pltpu.make_async_copy(acc.at[rows, :], out_refs[k], out_sem.at[k]))
        copies[-1].start()
    copies.append(pltpu.make_async_copy(act, final_ref.at[seq], own_sem.at[3]))
    copies[-1].start()
    for copy in copies:
        copy.wait()


def run_layer(slot, table, over, hidden, ga, gm, cos, sin, wh, wo, wg, wu, wd, ck, cv, sib, full, fullf, pieces, final, n_out):
    n_ff = wg.shape[1] // BLK
    any_spec = pl.BlockSpec(memory_space=pl.ANY)
    smem = pl.BlockSpec(memory_space=pltpu.SMEM)
    vmem = pl.BlockSpec(memory_space=pltpu.VMEM)
    d = hidden.shape[2]
    args = list(pieces) + ([final] if final is not None else [])
    flops = 2 * HEAD * d * (KV_WIDE * 2 + WIDE * 2 + 3 * wg.shape[1]) + 1_100_000_000
    return pl.pallas_call(
        functools.partial(layer_kernel, 4, n_ff, n_out, slot),
        out_shape=[pltpu.HBM((HEAD // n_out, d), F32)] * n_out + [jax.ShapeDtypeStruct(hidden.shape, BF16)],
        in_specs=[smem, smem] + [vmem] * 5 + [any_spec] * (10 + len(args)),
        out_specs=[any_spec] * (n_out + 1),
        input_output_aliases={17 + len(pieces): n_out} if final is not None else {},
        scratch_shapes=[
            pltpu.VMEM((HEAD, d), BF16),
            pltpu.VMEM((HEAD, d), BF16),
            pltpu.VMEM((HEAD, d), F32),
            pltpu.VMEM((HEAD, KV_WIDE), F32),
            pltpu.VMEM((HEAD, KV_WIDE), BF16),
            pltpu.VMEM((2 * DEPTH, d, BLK), BF16),
            pltpu.VMEM((DEPTH_B, BLK, d), BF16),
            pltpu.SemaphoreType.DMA((2 + PER_HALF,)),
            pltpu.SemaphoreType.DMA((4,)),
            pltpu.SemaphoreType.DMA((DEPTH_B, 3)),
            pltpu.SemaphoreType.DMA((n_out,)),
        ],
        compiler_params=pltpu.CompilerParams(vmem_limit_bytes=VMEM_BESIDE),
        cost_estimate=pl.CostEstimate(flops=flops, bytes_accessed=160_000_000, transcendentals=0),
    )(table, over, ga, gm, cos, sin, wh, hidden, wo, wg, wu, wd, ck, cv, sib, full, fullf, *args)


def window_kernel(sc_ref, h_ref, ga_ref, cos_ref, sin_ref, wh_ref, ck_ref, cv_ref, ok_ref, ov_ref):
    step = pl.program_id(0)
    lo = lax.axis_index('cp') * HALF
    a_rows, inside = [], []
    for j in range(2):
        first = lo - sc_ref[2 * step + j]
        want = first + lax.broadcasted_iota(jnp.int32, (HALF, HEAD), 0)
        have = lax.broadcasted_iota(jnp.int32, (HALF, HEAD), 1)
        pick = jnp.where(want == have, 1.0, 0.0).astype(BF16)
        a_rows.append(dot(pick, h_ref[j]))
        idx = first + lax.broadcasted_iota(jnp.int32, (HALF, HEAD), 0)
        inside.append((idx >= 0) & (idx < HEAD))
    a = rms_norm(jnp.concatenate(a_rows, axis=0), ga_ref[...])
    here = pl.ds(pl.multiple_of(lo, HALF), HALF)
    cos = jnp.concatenate([cos_ref[here, :]] * 2, axis=0)
    sin = jnp.concatenate([sin_ref[here, :]] * 2, axis=0)
    for g in range(4):
        kv = dot(a, wh_ref[g, :, 512:])
        k = rotate(kv[:, :HEAD], cos, sin).astype(BF16)
        v = kv[:, HEAD:].astype(BF16)
        cols = slice(g * HEAD, (g + 1) * HEAD)
        for j in range(2):
            rows = slice(j * HALF, (j + 1) * HALF)
            ok_ref[j, :, cols] = jnp.where(inside[j], k[rows], ck_ref[j, :, cols])
            ov_ref[j, :, cols] = jnp.where(inside[j], v[rows], cv_ref[j, :, cols])


def write_windows(scalars, hidden, ga, cos, sin, wh, cache_k, cache_v):
    n_seq, rows, width = cache_k.shape
    d = hidden.shape[2]
    one = pl.Buffered(1)
    cache_spec = pl.BlockSpec((2, rows, width), lambda i, sc: (i, 0, 0))
    return pl.pallas_call(
        window_kernel,
        out_shape=[jax.ShapeDtypeStruct(cache_k.shape, BF16)] * 2,
        grid_spec=pltpu.PrefetchScalarGridSpec(
            num_scalar_prefetch=1,
            grid=(n_seq // 2,),
            in_specs=[
                pl.BlockSpec((2, HEAD, d), lambda i, sc: (i, 0, 0)),
                pl.BlockSpec((1, d), lambda i, sc: (0, 0), pipeline_mode=one),
                pl.BlockSpec((512, HALF), lambda i, sc: (0, 0), pipeline_mode=one),
                pl.BlockSpec((512, HALF), lambda i, sc: (0, 0), pipeline_mode=one),
                pl.BlockSpec(memory_space=pltpu.VMEM),
                cache_spec,
                cache_spec,
            ],
            out_specs=[cache_spec, cache_spec],
        ),
        compiler_params=pltpu.CompilerParams(vmem_limit_bytes=VMEM_BESIDE),
        cost_estimate=pl.CostEstimate(flops=2 * n_seq * rows * d * 2 * width, bytes_accessed=60_000_000, transcendentals=0),
        name="cache_window",
    )(scalars, hidden, ga, cos, sin, wh, cache_k, cache_v)


def place_kernel(where, blk, tab_ref, *rest):
    n_part = len(where)
    parts = rest[:n_part]
    out_ref, wide, narrow, in_sem, out_sem = rest[-5:]
    slots = wide.shape[0]
    jobs = [(k, b) for k in range(n_part) for b in range(parts[k].shape[0] // blk)]

    def load(n):
        k, b = jobs[n]
        return pltpu.make_async_copy(parts[k].at[pl.ds(b * blk, blk), :], wide.at[n % slots], in_sem.at[n % slots])

    def store(n):
        k, b = jobs[n]
        entry, first = where[k]
        return pltpu.make_async_copy(narrow.at[n % slots], out_ref.at[tab_ref[entry], pl.ds(first + b * blk, blk), :],
                                     out_sem.at[n % slots])

    for n in range(min(slots, len(jobs))):
        load(n).start()
    for n in range(len(jobs)):
        load(n).wait()
        if n >= slots:
            store(n - slots).wait()

        @pl.loop(0, blk // 16)
        def _(r, n=n):
            rows = pl.ds(pl.multiple_of(r * 16, 16), 16)
            narrow[n % slots, rows, :] = wide[n % slots, rows, :].astype(BF16)

        store(n).start()
        if n + slots < len(jobs):
            load(n + slots).start()
    for n in range(max(0, len(jobs) - slots), len(jobs)):
        store(n).wait()


def place_rows(table, parts, where, out, blk):
    d = parts[0].shape[1]
    any_spec = pl.BlockSpec(memory_space=pl.ANY)
    n_part = len(parts)
    slots = min(8, sum(p.shape[0] // blk for p in parts))
    return pl.pallas_call(
        functools.partial(place_kernel, where, blk),
        out_shape=jax.ShapeDtypeStruct(out.shape, BF16),
        in_specs=[pl.BlockSpec(memory_space=pltpu.SMEM)] + [any_spec] * (n_part + 1),
        out_specs=any_spec,
        scratch_shapes=[
            pltpu.VMEM((slots, blk, d), F32),
            pltpu.VMEM((slots, blk, d), BF16),
            pltpu.SemaphoreType.DMA((slots,)),
            pltpu.SemaphoreType.DMA((slots,)),
        ],
        input_output_aliases={n_part + 1: 0},
        compiler_params=pltpu.CompilerParams(vmem_limit_bytes=VMEM_ALL),
        cost_estimate=pl.CostEstimate(flops=10_000_000, bytes_accessed=sum(p.size for p in parts) * 6, transcendentals=0),
    )(table, *parts, out)


def solution(mesh):
    d2d = [(0, 1), (1, 0), (2, 3), (3, 2)]
    cross = [(0, 2), (1, 3), (2, 0), (3, 1)]

    def send(x, pairs, axis='cp'):
        x = lax.ppermute(x, axis, pairs)
        return x

    def body(hidden, start_pos, cache_k, cache_v, w_q, w_k, w_v, w_o, w_gate, w_up, w_down, norm_attn, norm_mlp):
        n_seq, _, d = hidden.shape
        i32 = jnp.int32
        table, over, cos, sin, ga, gm, *mine = plan_and_pack(start_pos, cache_k, cache_v, norm_attn, norm_mlp)
        piece_a, piece_b, piece_d, piece_e, piece_o, piece_s = mine
        got_a = send(piece_a, [(0, 3)])
        sib = send(piece_s, [(0, 1), (1, 0)])
        got_b = send(piece_b, [(0, 2)])
        got_d = send(piece_d, [(0, 3)])
        got_a, piece_e, piece_o = lax.optimization_barrier((got_a, piece_e, piece_o))
        got_e = send(piece_e, [(1, 2)])
        got_o = send(piece_o, [(1, 3)])

        def send_all(_):
            sid = jnp.arange(n_seq, dtype=i32)
            before = (start_pos[None, :] < start_pos[:, None]) | (
                (start_pos[None, :] == start_pos[:, None]) & (sid[None, :] < sid[:, None]))
            rank = jnp.sum(before.astype(i32), axis=1)
            order = jnp.sum((rank[None, :] == sid[:, None]).astype(i32) * sid[None, :], axis=1)
            got = lax.ppermute(pack_full(order, cache_k, cache_v), 'cp', [(0, 2), (1, 3)])
            return got, lax.ppermute(got, 'cp', [(2, 3), (3, 2)])

        full, full_f = lax.cond(over[0] > 0, send_all, lambda _: tuple(blank(2)), 0)

        w_q, w_k, w_v, full, full_f = lax.optimization_barrier((w_q, w_k, w_v, full, full_f))
        wh = pltpu.with_memory_space_constraint(split_heads(w_q, w_k, w_v), pltpu.VMEM)
        wo = w_o.reshape(-1, d)

        out = None
        tab = table
        parts, where = [], []
        for t in range(4):
            pieces = (got_a, got_b if t > 0 else got_a) + ((got_d, got_e, got_o) if t > 1 else (got_a,) * 3)
            *own, out = run_layer(t, tab, over, hidden, ga, gm, cos, sin, wh, wo, w_gate, w_up, w_down,
                                  cache_k, cache_v, sib, full, full_f, pieces, out, 1)
            tab, own = lax.optimization_barrier((tab, own))
            for rows in own:
                crs = send(rows, cross)
                near = send(rows, d2d)
                dia = send(crs, d2d)
                parts.append((near, crs, dia))
                where.append([(ROW * t + k, 0) for k in (1, 2, 3)])
        start_late, _ = lax.optimization_barrier((start_pos, tab))
        new_k, new_v = write_windows(start_late, hidden, ga, cos, sin, wh, cache_k, cache_v)
        early = [(t, k) for t in range(4) for k in range(3) if t < 3 or k == 0]
        for chosen, blk in ((early, HALF), ([(3, 1)], 32), ([(3, 2)], 32)):
            out = place_rows(tab, [parts[c][k] for c, k in chosen], [where[c][k] for c, k in chosen], out, blk)
        return out, new_k, new_v

    group_spec = P('dp', None, None)
    cache_spec = P('dp', 'cp', None)
    whole_spec = P()
    return jax.shard_map(
        body,
        mesh=mesh,
        in_specs=(group_spec, P('dp'), cache_spec, cache_spec) + (whole_spec,) * 9,
        out_specs=(group_spec, cache_spec, cache_spec),
        check_vma=False,
    )
```

```python
import functools
import math

import jax
import jax.numpy as jnp
from jax import lax
from jax.experimental import pallas as pl
from jax.experimental.pallas import tpu as pltpu
from jax.sharding import PartitionSpec as P


NORM_EPS = 1e-6
ROPE_BASE = 1.0e4
MASK_FLOOR = -1.0e30
GELU_C = 0.7978845608028654

UNIT = 16
HALF = 128
HEAD = 2 * HALF
WIDE = 4 * HEAD
KV_WIDE = 2 * WIDE
PER_HALF = HALF // UNIT
A_UNITS, C_UNITS = 10, 5
WHOLE_B, WHOLE_D = (3, 4, 7), (5, 6)
A_ROWS, C_ROWS = A_UNITS * UNIT, C_UNITS * UNIT
B_ROWS, D_ROWS, S_ROWS = len(WHOLE_B) * HALF, len(WHOLE_D) * HALF, 4 * HALF
ROW = 16
OUT_BLK = 512
STEP_ROWS = 64
BLK = 768
VMEM_BESIDE = 48_100_000
VMEM_ALL = 66_900_000
DEPTH = 2
DEPTH_B = 3
F32 = jnp.float32
BF16 = jnp.bfloat16


def rms_norm(x, gain):
    inv = lax.rsqrt(jnp.mean(x * x, axis=-1, keepdims=True) + NORM_EPS)
    return (x * inv * (1.0 + gain)).astype(BF16)


def rotate(x, cos, sin):
    half = x.shape[-1] // 2
    first, second = x[:, :half], x[:, half:]
    return jnp.concatenate([first * cos - second * sin, second * cos + first * sin], axis=-1)


def gelu_tanh(x):
    return 0.5 * x * (1.0 + jnp.tanh(GELU_C * (x + 0.044715 * (x * x * x))))


def dot(a, b):
    return jnp.dot(a, b, preferred_element_type=F32)


def dot_t(a, b):
    return lax.dot_general(a, b, (((1,), (1,)), ((), ())), preferred_element_type=F32)


def sort_lengths(start_ref, order, length):
    starts = [start_ref[i] for i in range(16)]
    for i in range(16):
        rank = jnp.int32(0)
        for j in range(16):
            if j != i:
                ahead = (starts[j] <= starts[i]) if j < i else (starts[j] < starts[i])
                rank = rank + ahead.astype(jnp.int32)
        order[rank] = i
        length[rank] = starts[i]


def place_units(length, pos, cnt):
    over = jnp.int32(0)
    for half, places, room in ((0, (0,), 0), (0, (1, 2), A_UNITS), (1, (0, 1, 2, 3), 0), (1, (4, 7), C_UNITS), (1, (5, 6), C_UNITS)):
        at = jnp.int32(0)
        for j in places:
            n = jnp.clip((length[j] - half * HALF + UNIT - 1) // UNIT, 0, PER_HALF)
            pos[half * 8 + j] = at
            cnt[half * 8 + j] = n
            at = at + n
        over = over | (at > room).astype(jnp.int32)
    return over


def make_plan(start_ref, table, order, length, pos, cnt):
    me = lax.axis_index('cp')
    x_pos, core = me // 2, me % 2
    sort_lengths(start_ref, order, length)
    over = place_units(length, pos, cnt)
    for t in range(4):
        for k in range(4):
            xx = x_pos if k < 2 else 1 - x_pos
            cc = core if k % 2 == 0 else 1 - core
            place = 2 * t + (cc + t) % 2
            rank = 8 * (1 - xx) + place
            table[ROW * t + k] = order[rank]
            if k == 0:
                table[ROW * t + 4] = length[rank]
                table[ROW * t + 5] = x_pos
                table[ROW * t + 6] = core
                table[ROW * t + 7] = place
                for half in range(2):
                    table[ROW * t + 8 + half] = pos[half * 8 + place]
                    table[ROW * t + 10 + half] = jnp.clip((length[rank] - HALF * half + UNIT - 1) // UNIT, 0, PER_HALF)
    table[64] = over
    return x_pos, core, over


def pack_kernel(start_ref, ck_ref, cv_ref, ga_ref, gm_ref, table, over_ref, cos_ref, sin_ref, ga_out, gm_out, *rest):
    outs = rest[:6]
    order, length, pos, cnt, raw, wide, in_sem, out_sem = rest[6:]
    x_pos, core, over = make_plan(start_ref, table, order, length, pos, cnt)
    over_ref[0] = over
    first = dict(A=0, B=A_ROWS, D=A_ROWS + B_ROWS, E=0, O=C_ROWS, S=A_ROWS + B_ROWS + D_ROWS)
    size = dict(A=A_ROWS, B=B_ROWS, D=D_ROWS, E=C_ROWS, O=C_ROWS, S=S_ROWS)

    def copies(seq, row, to, rows, sem):
        return [pltpu.make_async_copy(src.at[seq, pl.ds(row, rows), :], raw.at[pl.ds(to, rows), pl.ds(side * WIDE, WIDE)],
                                      in_sem.at[sem, side]) for side, src in enumerate((ck_ref, cv_ref))]

    def units(half, j, to, sem, act):
        @pl.loop(0, PER_HALF)
        def _(u):
            at = pos[half * 8 + j] + u

            @pl.when((u < cnt[half * 8 + j]) & (at < (C_UNITS if half else A_UNITS)))
            def _():
                row = pl.multiple_of(u * UNIT, UNIT)
                for copy in copies(order[j], row, pl.multiple_of(to + at * UNIT, UNIT), UNIT, sem + at):
                    act(copy)

    def reads(name, act):
        if name == "A":
            for j in (1, 2):
                units(0, j, first["A"], 0, act)
        elif name == "E":
            for j in (4, 7):
                units(1, j, first["E"], 0, act)
        elif name == "O":
            for j in (5, 6):
                units(1, j, first["O"], C_UNITS, act)
        elif name == "S":
            for t in range(4):
                seq = order[8 + 2 * t + (1 - core + t) % 2]
                for copy in copies(seq, 0, first["S"] + t * HALF, HALF, A_UNITS + t):
                    act(copy)
        else:
            places, sem = (WHOLE_B, A_UNITS + 4) if name == "B" else (WHOLE_D, A_UNITS + 4 + len(WHOLE_B))
            for k, j in enumerate(places):
                for copy in copies(order[j], 0, first[name] + k * HALF, HALF, sem + k):
                    act(copy)

    def out_copy(k, name):
        return pltpu.make_async_copy(wide.at[pl.ds(first[name], size[name]), :], outs[k], out_sem.at[k])

    def widen(k, name):
        reads(name, lambda copy: copy.wait())

        @pl.loop(0, size[name] // UNIT)
        def _(u):
            rows = pl.ds(pl.multiple_of(first[name] + u * UNIT, UNIT), UNIT)
            wide[rows, :] = raw[rows, :].astype(F32)

        out_copy(k, name).start()

    for who, names in enumerate(("ASBD", "SEO")):
        @pl.when((x_pos == 0) & (core == who))
        def _(names=names):
            for name in names:
                reads(name, lambda copy: copy.start())

    ga_out[...] = ga_ref[...].astype(F32).reshape(ga_out.shape)
    gm_out[...] = gm_ref[...].astype(F32).reshape(gm_out.shape)
    half = cos_ref.shape[1]
    freq = lax.broadcasted_iota(jnp.int32, (1, half), 1).astype(F32)
    inv_freq = jnp.exp(freq * (-2.0 / (2 * half) * math.log(ROPE_BASE)))
    big = (16 * lax.broadcasted_iota(jnp.int32, (32, half), 0)).astype(F32) * inv_freq
    small = lax.broadcasted_iota(jnp.int32, (16, half), 0).astype(F32) * inv_freq
    cos_a, sin_a, cos_b, sin_b = jnp.cos(big), jnp.sin(big), jnp.cos(small), jnp.sin(small)
    for r in range(32):
        rows = slice(16 * r, 16 * r + 16)
        ca, sa = cos_a[r:r + 1], sin_a[r:r + 1]
        cos_ref[rows, :] = ca * cos_b - sa * sin_b
        sin_ref[rows, :] = sa * cos_b + ca * sin_b

    for who, names in enumerate(("ASBD", "SEO")):
        @pl.when((x_pos == 0) & (core == who))
        def _(names=names):
            for name in names:
                widen("ABDEOS".index(name), name)
            for name in names:
                out_copy("ABDEOS".index(name), name).wait()


def plan_and_pack(start_pos, cache_k, cache_v, ga, gm):
    any_spec = pl.BlockSpec(memory_space=pl.ANY)
    smem = pl.BlockSpec(memory_space=pltpu.SMEM)
    vmem = pl.BlockSpec(memory_space=pltpu.VMEM)
    total = A_ROWS + B_ROWS + D_ROWS + S_ROWS
    n_copy = A_UNITS + 4 + len(WHOLE_B + WHOLE_D)
    return pl.pallas_call(
        pack_kernel,
        out_shape=[jax.ShapeDtypeStruct((80,), jnp.int32), jax.ShapeDtypeStruct((1,), jnp.int32)]
        + [jax.ShapeDtypeStruct((2 * HEAD, HALF), F32)] * 2 + [jax.ShapeDtypeStruct((1, ga.shape[0]), F32)] * 2
        + [pltpu.HBM((n, KV_WIDE), F32) for n in (A_ROWS, B_ROWS, D_ROWS, C_ROWS, C_ROWS, S_ROWS)],
        in_specs=[smem, any_spec, any_spec, vmem, vmem],
        out_specs=[smem, smem] + [vmem] * 4 + [any_spec] * 6,
        scratch_shapes=[pltpu.SMEM((16,), jnp.int32)] * 4 + [
            pltpu.VMEM((total, KV_WIDE), BF16),
            pltpu.VMEM((total, KV_WIDE), F32),
            pltpu.SemaphoreType.DMA((n_copy, 2)),
            pltpu.SemaphoreType.DMA((6,)),
        ],
        compiler_params=pltpu.CompilerParams(vmem_limit_bytes=VMEM_ALL),
        cost_estimate=pl.CostEstimate(flops=20_000_000, bytes_accessed=16_000_000, transcendentals=0),
        name="pack",
    )(start_pos, cache_k, cache_v, ga, gm)


def pack_full_kernel(order_ref, ck_ref, cv_ref, out_ref, raw, wide, sem):
    d = WIDE

    @pl.loop(0, 8)
    def _(j):
        seq = order_ref[j]
        copies = (
            pltpu.make_async_copy(ck_ref.at[seq], raw.at[:, pl.ds(0, d)], sem.at[0]),
            pltpu.make_async_copy(cv_ref.at[seq], raw.at[:, pl.ds(d, d)], sem.at[1]),
        )
        for copy in copies:
            copy.start()
        for copy in copies:
            copy.wait()
        wide[...] = raw[...].astype(F32)
        out = pltpu.make_async_copy(wide, out_ref.at[j], sem.at[2])
        out.start()
        out.wait()


def pack_full(order, cache_k, cache_v):
    any_spec = pl.BlockSpec(memory_space=pl.ANY)
    return pl.pallas_call(
        pack_full_kernel,
        out_shape=jax.ShapeDtypeStruct((8, HALF, KV_WIDE), F32),
        in_specs=[pl.BlockSpec(memory_space=pltpu.SMEM), any_spec, any_spec],
        out_specs=any_spec,
        scratch_shapes=[
            pltpu.VMEM((HALF, KV_WIDE), BF16),
            pltpu.VMEM((HALF, KV_WIDE), F32),
            pltpu.SemaphoreType.DMA((3,)),
        ],
        name="pack_full",
    )(order, cache_k, cache_v)


def blank_kernel(*refs):
    pass


def blank(count):
    return pl.pallas_call(
        blank_kernel,
        out_shape=[jax.ShapeDtypeStruct((8, HALF, KV_WIDE), F32)] * count,
        out_specs=[pl.BlockSpec(memory_space=pl.ANY)] * count,
        name="blank",
    )()


W_CHUNK = 384
W_SLOTS = 3


def heads_kernel(q_ref, k_ref, v_ref, out_ref, raw_q, raw_k, raw_v, sem):
    n_chunk = q_ref.shape[0] // W_CHUNK

    def copies(i, b):
        rows = pl.ds(pl.multiple_of(i * W_CHUNK, W_CHUNK), W_CHUNK)
        return [pltpu.make_async_copy(src.at[rows], dst.at[b], sem.at[b, j])
                for j, (src, dst) in enumerate(((q_ref, raw_q), (k_ref, raw_k), (v_ref, raw_v)))]

    def sorter(n_head):
        per = HEAD // n_head
        want = lax.broadcasted_iota(jnp.int32, (HEAD, HEAD), 0)
        have = lax.broadcasted_iota(jnp.int32, (HEAD, HEAD), 1)
        return jnp.where((want % per) * n_head + want // per == have, 1.0, 0.0).astype(BF16)

    for i in range(W_SLOTS):
        for copy in copies(i, i):
            copy.start()
    sort8, sort4 = sorter(8), sorter(4)

    @pl.loop(0, n_chunk)
    def _(i):
        b = lax.rem(i, W_SLOTS)
        for copy in copies(i, b):
            copy.wait()
        for part in range(W_CHUNK // 64):
            to = pl.multiple_of(i * W_CHUNK, W_CHUNK) + part * 64
            for raw, n_head, sort, first in ((raw_q, 8, sort8, 0), (raw_k, 4, sort4, 2), (raw_v, 4, sort4, 3)):
                per = HEAD // n_head
                for sub in range(64 // per):
                    block = raw[b, part * 64 + sub * per:part * 64 + (sub + 1) * per].reshape(HEAD, HEAD)
                    moved = dot(sort, block).astype(BF16)
                    for h in range(n_head):
                        g, col = (h // 2, h % 2) if n_head == 8 else (h, first)
                        out_ref[g, pl.ds(to + sub * per, per), col * HEAD:(col + 1) * HEAD] = moved[h * per:(h + 1) * per]

        @pl.when(i + W_SLOTS < n_chunk)
        def _():
            for copy in copies(i + W_SLOTS, b):
                copy.start()


def split_heads(w_q, w_k, w_v):
    d = w_q.shape[0]
    any_spec = pl.BlockSpec(memory_space=pl.ANY)
    return pl.pallas_call(
        heads_kernel,
        out_shape=pltpu.VMEM((4, d, WIDE), BF16),
        in_specs=[any_spec] * 3,
        out_specs=pl.BlockSpec(memory_space=pltpu.VMEM),
        scratch_shapes=[
            pltpu.VMEM((W_SLOTS, W_CHUNK, 8, HEAD), BF16),
            pltpu.VMEM((W_SLOTS, W_CHUNK, 4, HEAD), BF16),
            pltpu.VMEM((W_SLOTS, W_CHUNK, 4, HEAD), BF16),
            pltpu.SemaphoreType.DMA((W_SLOTS, 3)),
        ],
        compiler_params=pltpu.CompilerParams(vmem_limit_bytes=VMEM_BESIDE),
        cost_estimate=pl.CostEstimate(flops=5_000_000_000, bytes_accessed=20_000_000, transcendentals=0),
        name="heads",
    )(w_q, w_k, w_v)


def layer_kernel(n_att, n_ff, sizes, slot, tab_ref, over_ref, ga_ref, gm_ref, cos_ref, sin_ref, wh_ref, h_ref, wo_ref,
                 wg_ref, wu_ref, wd_ref, ck_ref, cv_ref, sib_ref, full_ref, fullf_ref, *rest):
    refs = iter(rest)
    a_ref, b_ref, d_ref, e_ref, o_ref = [next(refs) for _ in range(5)]
    if slot > 0:
        next(refs)
    out_refs = [next(refs) for _ in sizes]
    final_ref, h_rows, act, acc, stage, hist, ring_a, ring_b, sem, own_sem, ring_sem, out_sem = refs
    base = ROW * slot
    seq, start, x_pos, core = tab_ref[base], tab_ref[base + 4], tab_ref[base + 5], tab_ref[base + 6]
    place = tab_ref[base + 7]
    ovf = over_ref[0] > 0
    far = x_pos == 1

    def whole_copies(half):
        to = stage.at[pl.ds(half * HALF, HALF), :]
        fits = far & jnp.logical_not(ovf)
        found = [
            ((x_pos == 0) & (core != half), sib_ref.at[pl.ds(slot * HALF, HALF), :]),
            (far & ovf & (core == half), full_ref.at[place]),
            (far & ovf & (core != half), fullf_ref.at[place]),
        ]
        if half == 0:
            for who, places, ref in ((0, WHOLE_B, b_ref), (1, WHOLE_D, d_ref)):
                mine = 2 * slot + (who + slot) % 2
                if mine in places:
                    found.append((fits & (core == who), ref.at[pl.ds(places.index(mine) * HALF, HALF), :]))
        return [(c, pltpu.make_async_copy(src, to, sem.at[half])) for c, src in found]

    def unit_copies(half, u):
        at = pl.multiple_of((tab_ref[base + 8 + half] + u) * UNIT, UNIT)
        live = far & jnp.logical_not(ovf) & (u < tab_ref[base + 10 + half])
        to = stage.at[pl.ds(pl.multiple_of(half * HALF + u * UNIT, UNIT), UNIT), :]
        if half == 0:
            found = [(live & (core == 1), a_ref)] if slot < 2 else []
        else:
            found = [(live & (core == who), ref) for who, ref in ((0, e_ref), (1, o_ref))] if slot >= 2 else []
        return [(c, pltpu.make_async_copy(src.at[pl.ds(at, UNIT), :], to, sem.at[2 + u])) for c, src in found]

    def own_copies(half):
        rows = pl.ds(half * HALF, HALF)
        return (
            pltpu.make_async_copy(ck_ref.at[seq], hist.at[rows, pl.ds(0, WIDE)], own_sem.at[0]),
            pltpu.make_async_copy(cv_ref.at[seq], hist.at[rows, pl.ds(WIDE, WIDE)], own_sem.at[1]),
        )

    def history(act_on):
        for half in range(2):
            for cond, copy in whole_copies(half):
                @pl.when(cond)
                def _(copy=copy):
                    act_on(copy)

            @pl.when((x_pos == 0) & (core == half))
            def _(half=half):
                for copy in own_copies(half):
                    act_on(copy)

        packed = 0 if slot < 2 else 1

        @pl.loop(0, PER_HALF)
        def _(u):
            for cond, copy in unit_copies(packed, u):
                @pl.when(cond)
                def _(copy=copy):
                    act_on(copy)

    def up_copies(j):
        at = lax.rem(j, DEPTH)
        cols = pl.ds(pl.multiple_of(j * BLK, BLK), BLK)
        return [
            pltpu.make_async_copy(wg_ref.at[:, cols], ring_a.at[2 * at], ring_sem.at[at, 0]),
            pltpu.make_async_copy(wu_ref.at[:, cols], ring_a.at[2 * at + 1], ring_sem.at[at, 1]),
        ]

    def out_copy(i):
        at = lax.rem(i, DEPTH_B)
        rows = pl.ds(pl.multiple_of(i * OUT_BLK, OUT_BLK), OUT_BLK)
        return pltpu.make_async_copy(wo_ref.at[rows, :], ring_b.at[at, pl.ds(0, OUT_BLK), :], ring_sem.at[at, 2])

    def down_copy(j):
        at = lax.rem(j + n_att, DEPTH_B)
        rows = pl.ds(pl.multiple_of(j * BLK, BLK), BLK)
        return pltpu.make_async_copy(wd_ref.at[rows, :], ring_b.at[at], ring_sem.at[at, 2])

    row_copy = pltpu.make_async_copy(h_ref.at[seq], h_rows, own_sem.at[2])
    row_copy.start()
    history(lambda copy: copy.start())
    for i in range(DEPTH_B):
        out_copy(i).start()
    for j in range(DEPTH):
        for copy in up_copies(j):
            copy.start()
    row_copy.wait()
    act[...] = rms_norm(h_rows[...].astype(F32), ga_ref[...])

    @pl.loop(0, HEAD // UNIT)
    def _(u):
        rows = pl.ds(pl.multiple_of(u * UNIT, UNIT), UNIT)
        acc[rows, :] = h_rows[rows, :].astype(F32)

    history(lambda copy: copy.wait())
    for half in range(2):
        @pl.when((x_pos == 1) | (core != half))
        def _(half=half):
            @pl.loop(0, PER_HALF)
            def _(u):
                rows = pl.ds(pl.multiple_of(half * HALF + u * UNIT, UNIT), UNIT)
                hist[rows, :] = stage[rows, :].astype(BF16)

    @pl.loop(0, n_att)
    def _(i):
        out_copy(i).wait()
        cos, sin = cos_ref[pl.ds(start, HEAD), :], sin_ref[pl.ds(start, HEAD), :]
        a = act[...]
        off = pl.multiple_of(i * HEAD, HEAD)
        row = lax.broadcasted_iota(jnp.int32, (HEAD, HEAD), 0)
        v_old = jnp.where(row < start, hist[:, pl.ds(off + WIDE, HEAD)], jnp.zeros((), BF16))
        qkv = dot(a, wh_ref[i])
        kv = qkv[:, 512:]
        k_all = jnp.concatenate([hist[:, pl.ds(off, HEAD)], rotate(kv[:, :HEAD], cos, sin).astype(BF16)], axis=0)
        v_all = jnp.concatenate([v_old, kv[:, HEAD:].astype(BF16)], axis=0)
        qs = [(rotate(qkv[:, j * HEAD:(j + 1) * HEAD], cos, sin) * 0.0625).astype(BF16) for j in range(2)]
        row = lax.broadcasted_iota(jnp.int32, (HEAD, 512), 0)
        col = lax.broadcasted_iota(jnp.int32, (HEAD, 512), 1)
        ok = (col < start) | ((col >= HEAD) & (col - HEAD <= row))
        scores = [jnp.where(ok, dot_t(q, k_all), MASK_FLOOR) for q in qs]
        tops = [jnp.max(s, axis=-1, keepdims=True) for s in scores]
        probs = [jnp.exp(s - top) for s, top in zip(scores, tops)]
        dens = [jnp.sum(p, axis=-1, keepdims=True) for p in probs]
        nums = [dot(p.astype(BF16), v_all) for p in probs]
        heads = [(num / den).astype(BF16) for num, den in zip(nums, dens)]
        acc[...] += dot(jnp.concatenate(heads, axis=-1), ring_b[lax.rem(i, DEPTH_B), :OUT_BLK, :])

        @pl.when(i + DEPTH_B < n_att)
        def _():
            out_copy(i + DEPTH_B).start()

        @pl.when(i + DEPTH_B >= n_att)
        def _():
            down_copy(i + DEPTH_B - n_att).start()

    res = acc[...].astype(BF16).astype(F32)
    act[...] = rms_norm(res, gm_ref[...])
    acc[...] = res

    @pl.loop(0, n_ff)
    def _(j):
        at = lax.rem(j, DEPTH)
        for copy in up_copies(j):
            copy.wait()
        down_copy(j).wait()
        c = act[...]
        mid = (gelu_tanh(dot(c, ring_a[2 * at])) * dot(c, ring_a[2 * at + 1])).astype(BF16)
        acc[...] += dot(mid, ring_b[lax.rem(j + n_att, DEPTH_B)])

        @pl.when(j + DEPTH < n_ff)
        def _():
            for copy in up_copies(j + DEPTH):
                copy.start()

        @pl.when(j + DEPTH_B < n_ff)
        def _():
            down_copy(j + DEPTH_B).start()

    copies = []
    first = 0
    for k, size in enumerate(sizes):
        for r in range(0, size, STEP_ROWS):
            block = first // STEP_ROWS

            @pl.loop(0, STEP_ROWS // UNIT)
            def _(u, first=first):
                rows = pl.ds(pl.multiple_of(first + u * UNIT, UNIT), UNIT)
                rounded = acc[rows, :].astype(BF16)
                act[rows, :] = rounded
                acc[rows, :] = rounded.astype(F32)

            rows, to = pl.ds(first, STEP_ROWS), pl.ds(r, STEP_ROWS)
            copies.append(pltpu.make_async_copy(acc.at[rows, :], out_refs[k].at[to, :], out_sem.at[block, 0]))
            copies.append(pltpu.make_async_copy(act.at[rows, :], final_ref.at[seq, rows, :], out_sem.at[block, 1]))
            for copy in copies[-2:]:
                copy.start()
            first += STEP_ROWS
    for copy in copies:
        copy.wait()


def run_layer(slot, table, over, hidden, ga, gm, cos, sin, wh, wo, wg, wu, wd, ck, cv, sib, full, fullf, pieces, final, sizes):
    n_ff = wg.shape[1] // BLK
    any_spec = pl.BlockSpec(memory_space=pl.ANY)
    smem = pl.BlockSpec(memory_space=pltpu.SMEM)
    vmem = pl.BlockSpec(memory_space=pltpu.VMEM)
    d = hidden.shape[2]
    args = list(pieces) + ([final] if final is not None else [])
    flops = 2 * HEAD * d * (KV_WIDE * 2 + WIDE * 2 + 3 * wg.shape[1]) + 1_100_000_000
    return pl.pallas_call(
        functools.partial(layer_kernel, 4, n_ff, sizes, slot),
        out_shape=[pltpu.HBM((n, d), F32) for n in sizes] + [jax.ShapeDtypeStruct(hidden.shape, BF16)],
        in_specs=[smem, smem] + [vmem] * 5 + [any_spec] * (10 + len(args)),
        out_specs=[any_spec] * (len(sizes) + 1),
        input_output_aliases={17 + len(pieces): len(sizes)} if final is not None else {},
        scratch_shapes=[
            pltpu.VMEM((HEAD, d), BF16),
            pltpu.VMEM((HEAD, d), BF16),
            pltpu.VMEM((HEAD, d), F32),
            pltpu.VMEM((HEAD, KV_WIDE), F32),
            pltpu.VMEM((HEAD, KV_WIDE), BF16),
            pltpu.VMEM((2 * DEPTH, d, BLK), BF16),
            pltpu.VMEM((DEPTH_B, BLK, d), BF16),
            pltpu.SemaphoreType.DMA((2 + PER_HALF,)),
            pltpu.SemaphoreType.DMA((3,)),
            pltpu.SemaphoreType.DMA((DEPTH_B, 3)),
            pltpu.SemaphoreType.DMA((HEAD // STEP_ROWS, 2)),
        ],
        compiler_params=pltpu.CompilerParams(vmem_limit_bytes=VMEM_BESIDE),
        cost_estimate=pl.CostEstimate(flops=flops, bytes_accessed=160_000_000, transcendentals=0),
    )(table, over, ga, gm, cos, sin, wh, hidden, wo, wg, wu, wd, ck, cv, sib, full, fullf, *args)


def window_kernel(sc_ref, h_ref, ga_ref, cos_ref, sin_ref, wh_ref, ck_ref, cv_ref, ok_ref, ov_ref):
    step = pl.program_id(0)
    lo = lax.axis_index('cp') * HALF
    a_rows, inside = [], []
    for j in range(2):
        first = lo - sc_ref[2 * step + j]
        want = first + lax.broadcasted_iota(jnp.int32, (HALF, HEAD), 0)
        have = lax.broadcasted_iota(jnp.int32, (HALF, HEAD), 1)
        pick = jnp.where(want == have, 1.0, 0.0).astype(BF16)
        a_rows.append(dot(pick, h_ref[j]))
        idx = first + lax.broadcasted_iota(jnp.int32, (HALF, HEAD), 0)
        inside.append((idx >= 0) & (idx < HEAD))
    a = rms_norm(jnp.concatenate(a_rows, axis=0), ga_ref[...])
    here = pl.ds(pl.multiple_of(lo, HALF), HALF)
    cos = jnp.concatenate([cos_ref[here, :]] * 2, axis=0)
    sin = jnp.concatenate([sin_ref[here, :]] * 2, axis=0)
    for g in range(4):
        kv = dot(a, wh_ref[g, :, 512:])
        k = rotate(kv[:, :HEAD], cos, sin).astype(BF16)
        v = kv[:, HEAD:].astype(BF16)
        cols = slice(g * HEAD, (g + 1) * HEAD)
        for j in range(2):
            rows = slice(j * HALF, (j + 1) * HALF)
            ok_ref[j, :, cols] = jnp.where(inside[j], k[rows], ck_ref[j, :, cols])
            ov_ref[j, :, cols] = jnp.where(inside[j], v[rows], cv_ref[j, :, cols])


def write_windows(scalars, hidden, ga, cos, sin, wh, cache_k, cache_v):
    n_seq, rows, width = cache_k.shape
    d = hidden.shape[2]
    one = pl.Buffered(1)
    cache_spec = pl.BlockSpec((2, rows, width), lambda i, sc: (i, 0, 0))
    return pl.pallas_call(
        window_kernel,
        out_shape=[jax.ShapeDtypeStruct(cache_k.shape, BF16)] * 2,
        grid_spec=pltpu.PrefetchScalarGridSpec(
            num_scalar_prefetch=1,
            grid=(n_seq // 2,),
            in_specs=[
                pl.BlockSpec((2, HEAD, d), lambda i, sc: (i, 0, 0)),
                pl.BlockSpec((1, d), lambda i, sc: (0, 0), pipeline_mode=one),
                pl.BlockSpec((512, HALF), lambda i, sc: (0, 0), pipeline_mode=one),
                pl.BlockSpec((512, HALF), lambda i, sc: (0, 0), pipeline_mode=one),
                pl.BlockSpec(memory_space=pltpu.VMEM),
                cache_spec,
                cache_spec,
            ],
            out_specs=[cache_spec, cache_spec],
        ),
        compiler_params=pltpu.CompilerParams(vmem_limit_bytes=VMEM_BESIDE),
        cost_estimate=pl.CostEstimate(flops=2 * n_seq * rows * d * 2 * width, bytes_accessed=60_000_000, transcendentals=0),
        name="cache_window",
    )(scalars, hidden, ga, cos, sin, wh, cache_k, cache_v)


def place_kernel(where, blk, tab_ref, *rest):
    n_part = len(where)
    parts = rest[:n_part]
    out_ref, wide, narrow, in_sem, out_sem = rest[-5:]
    slots = wide.shape[0]
    jobs = [(k, b) for k in range(n_part) for b in range(parts[k].shape[0] // blk)]

    def load(n):
        k, b = jobs[n]
        return pltpu.make_async_copy(parts[k].at[pl.ds(b * blk, blk), :], wide.at[n % slots], in_sem.at[n % slots])

    def store(n):
        k, b = jobs[n]
        entry, first = where[k]
        return pltpu.make_async_copy(narrow.at[n % slots], out_ref.at[tab_ref[entry], pl.ds(first + b * blk, blk), :],
                                     out_sem.at[n % slots])

    for n in range(min(slots, len(jobs))):
        load(n).start()
    for n in range(len(jobs)):
        load(n).wait()
        if n >= slots:
            store(n - slots).wait()

        @pl.loop(0, blk // 16)
        def _(r, n=n):
            rows = pl.ds(pl.multiple_of(r * 16, 16), 16)
            narrow[n % slots, rows, :] = wide[n % slots, rows, :].astype(BF16)

        store(n).start()
        if n + slots < len(jobs):
            load(n + slots).start()
    for n in range(max(0, len(jobs) - slots), len(jobs)):
        store(n).wait()


def place_rows(table, parts, where, out, blk):
    d = parts[0].shape[1]
    any_spec = pl.BlockSpec(memory_space=pl.ANY)
    n_part = len(parts)
    slots = min(8, sum(p.shape[0] // blk for p in parts))
    return pl.pallas_call(
        functools.partial(place_kernel, where, blk),
        out_shape=jax.ShapeDtypeStruct(out.shape, BF16),
        in_specs=[pl.BlockSpec(memory_space=pltpu.SMEM)] + [any_spec] * (n_part + 1),
        out_specs=any_spec,
        scratch_shapes=[
            pltpu.VMEM((slots, blk, d), F32),
            pltpu.VMEM((slots, blk, d), BF16),
            pltpu.SemaphoreType.DMA((slots,)),
            pltpu.SemaphoreType.DMA((slots,)),
        ],
        input_output_aliases={n_part + 1: 0},
        compiler_params=pltpu.CompilerParams(vmem_limit_bytes=VMEM_ALL),
        cost_estimate=pl.CostEstimate(flops=10_000_000, bytes_accessed=sum(p.size for p in parts) * 6, transcendentals=0),
    )(table, *parts, out)


def solution(mesh):
    d2d = [(0, 1), (1, 0), (2, 3), (3, 2)]
    cross = [(0, 2), (1, 3), (2, 0), (3, 1)]

    def send(x, pairs, axis='cp'):
        x = lax.ppermute(x, axis, pairs)
        return x

    def body(hidden, start_pos, cache_k, cache_v, w_q, w_k, w_v, w_o, w_gate, w_up, w_down, norm_attn, norm_mlp):
        n_seq, _, d = hidden.shape
        i32 = jnp.int32
        table, over, cos, sin, ga, gm, *mine = plan_and_pack(start_pos, cache_k, cache_v, norm_attn, norm_mlp)
        piece_a, piece_b, piece_d, piece_e, piece_o, piece_s = mine
        got_a = send(piece_a, [(0, 3)])
        sib = send(piece_s, [(0, 1), (1, 0)])
        got_b = send(piece_b, [(0, 2)])
        got_d = send(piece_d, [(0, 3)])
        got_a, piece_e, piece_o = lax.optimization_barrier((got_a, piece_e, piece_o))
        got_e = send(piece_e, [(1, 2)])
        got_o = send(piece_o, [(1, 3)])

        def send_all(_):
            sid = jnp.arange(n_seq, dtype=i32)
            before = (start_pos[None, :] < start_pos[:, None]) | (
                (start_pos[None, :] == start_pos[:, None]) & (sid[None, :] < sid[:, None]))
            rank = jnp.sum(before.astype(i32), axis=1)
            order = jnp.sum((rank[None, :] == sid[:, None]).astype(i32) * sid[None, :], axis=1)
            got = lax.ppermute(pack_full(order, cache_k, cache_v), 'cp', [(0, 2), (1, 3)])
            return got, lax.ppermute(got, 'cp', [(2, 3), (3, 2)])

        full, full_f = lax.cond(over[0] > 0, send_all, lambda _: tuple(blank(2)), 0)

        w_q, w_k, w_v, full, full_f = lax.optimization_barrier((w_q, w_k, w_v, full, full_f))
        wh = pltpu.with_memory_space_constraint(split_heads(w_q, w_k, w_v), pltpu.VMEM)
        wo = w_o.reshape(-1, d)

        out = None
        tab = table
        parts, where = [], []
        for t in range(4):
            pieces = (got_a, got_b if t > 0 else got_a) + ((got_d, got_e, got_o) if t > 1 else (got_a,) * 3)
            *own, out = run_layer(t, tab, over, hidden, ga, gm, cos, sin, wh, wo, w_gate, w_up, w_down,
                                  cache_k, cache_v, sib, full, full_f, pieces, out, (192, 64) if t == 3 else (HEAD,))
            tab, own = lax.optimization_barrier((tab, own))
            if t < 3:
                crs = send(own[0], cross)
                near = send(own[0], d2d)
                dia = send(crs, d2d)
                parts += [near, crs, dia]
                where += [(ROW * t + k, 0) for k in (1, 2, 3)]
        most, rest = own
        crs_most, near_most = send(most, cross), send(most, d2d)
        start_late, _ = lax.optimization_barrier((start_pos, tab))
        new_k, new_v = write_windows(start_late, hidden, ga, cos, sin, wh, cache_k, cache_v)
        rest, new_k = lax.optimization_barrier((rest, new_k))
        crs_rest, near_rest = send(rest, cross), send(rest, d2d)
        dia_most, dia_rest = send(crs_most, d2d), send(crs_rest, d2d)
        last = ROW * 3
        out = place_rows(tab, parts + [near_most], where + [(last + 1, 0)], out, 64)
        out = place_rows(tab, [crs_most, near_rest], [(last + 2, 0), (last + 1, 192)], out, 64)
        out = place_rows(tab, [dia_most], [(last + 3, 0)], out, 64)
        out = place_rows(tab, [crs_rest], [(last + 2, 192)], out, 16)
        out = place_rows(tab, [dia_rest], [(last + 3, 192)], out, 16)
        return out, new_k, new_v

    group_spec = P('dp', None, None)
    cache_spec = P('dp', 'cp', None)
    whole_spec = P()
    return jax.shard_map(
        body,
        mesh=mesh,
        in_specs=(group_spec, P('dp'), cache_spec, cache_spec) + (whole_spec,) * 9,
        out_specs=(group_spec, cache_spec, cache_spec),
        check_vma=False,
    )
```

```python
import functools
import math

import jax
import jax.numpy as jnp
from jax import lax
from jax.experimental import pallas as pl
from jax.experimental.pallas import tpu as pltpu
from jax.sharding import PartitionSpec as P


NORM_EPS = 1e-6
ROPE_BASE = 1.0e4
MASK_FLOOR = -1.0e30
GELU_C = 0.7978845608028654

UNIT = 16
HALF = 128
HEAD = 2 * HALF
WIDE = 4 * HEAD
KV_WIDE = 2 * WIDE
PER_HALF = HALF // UNIT
A_UNITS, C_UNITS = 10, 5
WHOLE_B, WHOLE_D = (3, 4, 7), (5, 6)
A_ROWS, C_ROWS = A_UNITS * UNIT, C_UNITS * UNIT
B_ROWS, D_ROWS, S_ROWS = len(WHOLE_B) * HALF, len(WHOLE_D) * HALF, 4 * HALF
ROW = 16
OUT_BLK = 512
STEP_ROWS = 64
BLK = 768
VMEM_BESIDE = 47_500_000
VMEM_ALL = 66_900_000
DEPTH = 2
DEPTH_B = 3
F32 = jnp.float32
BF16 = jnp.bfloat16


def rms_norm(x, gain):
    inv = lax.rsqrt(jnp.mean(x * x, axis=-1, keepdims=True) + NORM_EPS)
    return (x * inv * (1.0 + gain)).astype(BF16)


def rotate(x, cos, sin):
    half = x.shape[-1] // 2
    first, second = x[:, :half], x[:, half:]
    return jnp.concatenate([first * cos - second * sin, second * cos + first * sin], axis=-1)


def gelu_tanh(x):
    return 0.5 * x * (1.0 + jnp.tanh(GELU_C * (x + 0.044715 * (x * x * x))))


def dot(a, b):
    return jnp.dot(a, b, preferred_element_type=F32)


def dot_t(a, b):
    return lax.dot_general(a, b, (((1,), (1,)), ((), ())), preferred_element_type=F32)


def sort_lengths(start_ref, order, length):
    starts = [start_ref[i] for i in range(16)]
    for i in range(16):
        rank = jnp.int32(0)
        for j in range(16):
            if j != i:
                ahead = (starts[j] <= starts[i]) if j < i else (starts[j] < starts[i])
                rank = rank + ahead.astype(jnp.int32)
        order[rank] = i
        length[rank] = starts[i]


def place_units(length, pos, cnt):
    over = jnp.int32(0)
    for half, places, room in ((0, (0,), 0), (0, (1, 2), A_UNITS), (1, (0, 1, 2, 3), 0), (1, (4, 7), C_UNITS), (1, (5, 6), C_UNITS)):
        at = jnp.int32(0)
        for j in places:
            n = jnp.clip((length[j] - half * HALF + UNIT - 1) // UNIT, 0, PER_HALF)
            pos[half * 8 + j] = at
            cnt[half * 8 + j] = n
            at = at + n
        over = over | (at > room).astype(jnp.int32)
    return over


def make_plan(start_ref, table, order, length, pos, cnt):
    me = lax.axis_index('cp')
    x_pos, core = me // 2, me % 2
    sort_lengths(start_ref, order, length)
    over = place_units(length, pos, cnt)
    for t in range(4):
        for k in range(4):
            xx = x_pos if k < 2 else 1 - x_pos
            cc = core if k % 2 == 0 else 1 - core
            place = 2 * t + (cc + t) % 2
            rank = 8 * (1 - xx) + place
            table[ROW * t + k] = order[rank]
            if k == 0:
                table[ROW * t + 4] = length[rank]
                table[ROW * t + 5] = x_pos
                table[ROW * t + 6] = core
                table[ROW * t + 7] = place
                for half in range(2):
                    table[ROW * t + 8 + half] = pos[half * 8 + place]
                    table[ROW * t + 10 + half] = jnp.clip((length[rank] - HALF * half + UNIT - 1) // UNIT, 0, PER_HALF)
    return over


PIECE_ROWS = dict(A=A_ROWS, B=B_ROWS, D=D_ROWS, E=C_ROWS, O=C_ROWS, S=S_ROWS)


def pack_kernel(by_core, first, ck_ref, cv_ref, table, order, pos, cnt, outs, raw, wide, in_sem, out_sem):
    me = lax.axis_index('cp')
    x_pos, core = me // 2, me % 2

    def copies(seq, row, to, rows, sem):
        return [pltpu.make_async_copy(src.at[seq, pl.ds(row, rows), :], raw.at[pl.ds(to, rows), pl.ds(side * WIDE, WIDE)],
                                      in_sem.at[sem, side]) for side, src in enumerate((ck_ref, cv_ref))]

    def units(half, j, to, sem, act):
        @pl.loop(0, PER_HALF)
        def _(u):
            at = pos[half * 8 + j] + u

            @pl.when((u < cnt[half * 8 + j]) & (at < (C_UNITS if half else A_UNITS)))
            def _():
                row = pl.multiple_of(u * UNIT, UNIT)
                for copy in copies(order[j], row, pl.multiple_of(to + at * UNIT, UNIT), UNIT, sem + at):
                    act(copy)

    def reads(name, act):
        if name in "AEO":
            half, places, sem = dict(A=(0, (1, 2), 0), E=(1, (4, 7), 0), O=(1, (5, 6), C_UNITS))[name]
            for j in places:
                units(half, j, first[name], sem, act)
            return
        if name == "S":
            seqs, sem = [table[ROW * t + 1] for t in range(4)], 0
        elif name == "D":
            seqs, sem = [table[ROW * t + 3] for t in (2, 3)], 4
        else:
            seqs, sem = [order[j] for j in WHOLE_B], A_UNITS
        for k, seq in enumerate(seqs):
            for copy in copies(seq, 0, first[name] + k * HALF, HALF, sem + k):
                act(copy)

    def out_copy(name):
        k = list(outs).index(name)
        return pltpu.make_async_copy(wide.at[pl.ds(first[name], PIECE_ROWS[name]), :], outs[name], out_sem.at[k])

    def widen(name):
        reads(name, lambda copy: copy.wait())

        @pl.loop(0, PIECE_ROWS[name] // UNIT)
        def _(u):
            rows = pl.ds(pl.multiple_of(first[name] + u * UNIT, UNIT), UNIT)
            wide[rows, :] = raw[rows, :].astype(F32)

        out_copy(name).start()

    for who, names in enumerate(by_core):
        @pl.when((x_pos == 0) & (core == who))
        def _(names=names):
            for name in names:
                reads(name, lambda copy: copy.start())
            for name in names:
                widen(name)
            for name in names:
                out_copy(name).wait()


def pack_first_kernel(start_ref, ck_ref, cv_ref, table, over_ref, a_out, b_out, e_out, o_out, order, length, pos, cnt, *work):
    over_ref[0] = make_plan(start_ref, table, order, length, pos, cnt)
    outs = dict(A=a_out, B=b_out, E=e_out, O=o_out)
    pack_kernel(("AB", "EO"), dict(A=0, B=A_ROWS, E=0, O=C_ROWS), ck_ref, cv_ref, table, order, pos, cnt, outs, *work)


def pack_second_kernel(table, ck_ref, cv_ref, s_out, d_out, *work):
    outs = dict(S=s_out, D=d_out)
    pack_kernel(("SD", "S"), dict(S=0, D=S_ROWS), ck_ref, cv_ref, table, table, None, None, outs, *work)


def pack_call(kernel, n_scalar, names, rows, n_copy):
    any_spec = pl.BlockSpec(memory_space=pl.ANY)
    smem = pl.BlockSpec(memory_space=pltpu.SMEM)
    planned = n_scalar > 0
    return pl.pallas_call(
        kernel,
        out_shape=([pltpu.SMEM((80,), jnp.int32), pltpu.SMEM((1,), jnp.int32)] if planned else [])
        + [pltpu.HBM((PIECE_ROWS[n], KV_WIDE), F32) for n in names],
        in_specs=[smem, any_spec, any_spec],
        out_specs=([smem] * 2 if planned else []) + [any_spec] * len(names),
        scratch_shapes=[pltpu.SMEM((16,), jnp.int32)] * n_scalar + [
            pltpu.VMEM((rows, KV_WIDE), BF16),
            pltpu.VMEM((rows, KV_WIDE), F32),
            pltpu.SemaphoreType.DMA((n_copy, 2)),
            pltpu.SemaphoreType.DMA((len(names),)),
        ],
        compiler_params=pltpu.CompilerParams(vmem_limit_bytes=VMEM_ALL),
        cost_estimate=pl.CostEstimate(flops=10_000_000, bytes_accessed=8_000_000, transcendentals=0),
    )


def pack_full_kernel(order_ref, ck_ref, cv_ref, out_ref, raw, wide, sem):
    d = WIDE

    @pl.loop(0, 8)
    def _(j):
        seq = order_ref[j]
        copies = (
            pltpu.make_async_copy(ck_ref.at[seq], raw.at[:, pl.ds(0, d)], sem.at[0]),
            pltpu.make_async_copy(cv_ref.at[seq], raw.at[:, pl.ds(d, d)], sem.at[1]),
        )
        for copy in copies:
            copy.start()
        for copy in copies:
            copy.wait()
        wide[...] = raw[...].astype(F32)
        out = pltpu.make_async_copy(wide, out_ref.at[j], sem.at[2])
        out.start()
        out.wait()


def pack_full(order, cache_k, cache_v):
    any_spec = pl.BlockSpec(memory_space=pl.ANY)
    return pl.pallas_call(
        pack_full_kernel,
        out_shape=jax.ShapeDtypeStruct((8, HALF, KV_WIDE), F32),
        in_specs=[pl.BlockSpec(memory_space=pltpu.SMEM), any_spec, any_spec],
        out_specs=any_spec,
        scratch_shapes=[
            pltpu.VMEM((HALF, KV_WIDE), BF16),
            pltpu.VMEM((HALF, KV_WIDE), F32),
            pltpu.SemaphoreType.DMA((3,)),
        ],
        name="pack_full",
    )(order, cache_k, cache_v)


def blank_kernel(*refs):
    pass


def blank(count):
    return pl.pallas_call(
        blank_kernel,
        out_shape=[jax.ShapeDtypeStruct((8, HALF, KV_WIDE), F32)] * count,
        out_specs=[pl.BlockSpec(memory_space=pl.ANY)] * count,
        name="blank",
    )()


W_CHUNK = 384
W_SLOTS = 3


def heads_kernel(q_ref, k_ref, v_ref, ga_ref, gm_ref, out_ref, cos_ref, sin_ref, ga_out, gm_out, raw_q, raw_k, raw_v,
                 gain_a, gain_m, sem, gain_sem):
    n_chunk = q_ref.shape[0] // W_CHUNK

    def copies(i, b):
        rows = pl.ds(pl.multiple_of(i * W_CHUNK, W_CHUNK), W_CHUNK)
        return [pltpu.make_async_copy(src.at[rows], dst.at[b], sem.at[b, j])
                for j, (src, dst) in enumerate(((q_ref, raw_q), (k_ref, raw_k), (v_ref, raw_v)))]

    def sorter(n_head):
        per = HEAD // n_head
        want = lax.broadcasted_iota(jnp.int32, (HEAD, HEAD), 0)
        have = lax.broadcasted_iota(jnp.int32, (HEAD, HEAD), 1)
        return jnp.where((want % per) * n_head + want // per == have, 1.0, 0.0).astype(BF16)

    for i in range(W_SLOTS):
        for copy in copies(i, i):
            copy.start()
    gains = [pltpu.make_async_copy(src, dst, gain_sem.at[k])
             for k, (src, dst) in enumerate(((ga_ref, gain_a), (gm_ref, gain_m)))]
    for copy in gains:
        copy.start()
    half = cos_ref.shape[1]
    freq = lax.broadcasted_iota(jnp.int32, (1, half), 1).astype(F32)
    inv_freq = jnp.exp(freq * (-2.0 / (2 * half) * math.log(ROPE_BASE)))
    big = (16 * lax.broadcasted_iota(jnp.int32, (32, half), 0)).astype(F32) * inv_freq
    small = lax.broadcasted_iota(jnp.int32, (16, half), 0).astype(F32) * inv_freq
    cos_a, sin_a, cos_b, sin_b = jnp.cos(big), jnp.sin(big), jnp.cos(small), jnp.sin(small)
    for r in range(32):
        rows = slice(16 * r, 16 * r + 16)
        ca, sa = cos_a[r:r + 1], sin_a[r:r + 1]
        cos_ref[rows, :] = ca * cos_b - sa * sin_b
        sin_ref[rows, :] = sa * cos_b + ca * sin_b

    sort8, sort4 = sorter(8), sorter(4)

    @pl.loop(0, n_chunk)
    def _(i):
        b = lax.rem(i, W_SLOTS)
        for copy in copies(i, b):
            copy.wait()
        for part in range(W_CHUNK // 64):
            to = pl.multiple_of(i * W_CHUNK, W_CHUNK) + part * 64
            for raw, n_head, sort, first in ((raw_q, 8, sort8, 0), (raw_k, 4, sort4, 2), (raw_v, 4, sort4, 3)):
                per = HEAD // n_head
                for sub in range(64 // per):
                    block = raw[b, part * 64 + sub * per:part * 64 + (sub + 1) * per].reshape(HEAD, HEAD)
                    moved = dot(sort, block).astype(BF16)
                    for h in range(n_head):
                        g, col = (h // 2, h % 2) if n_head == 8 else (h, first)
                        out_ref[g, pl.ds(to + sub * per, per), col * HEAD:(col + 1) * HEAD] = moved[h * per:(h + 1) * per]

        @pl.when(i + W_SLOTS < n_chunk)
        def _():
            for copy in copies(i + W_SLOTS, b):
                copy.start()

    for copy, src, dst in zip(gains, (gain_a, gain_m), (ga_out, gm_out)):
        copy.wait()
        dst[...] = src[...].astype(F32).reshape(dst.shape)


def split_heads(w_q, w_k, w_v, ga, gm):
    d = w_q.shape[0]
    vmem = pl.BlockSpec(memory_space=pltpu.VMEM)
    any_spec = pl.BlockSpec(memory_space=pl.ANY)
    return pl.pallas_call(
        heads_kernel,
        out_shape=[pltpu.VMEM((4, d, WIDE), BF16)] + [pltpu.VMEM((2 * HEAD, HALF), F32)] * 2 + [pltpu.VMEM((1, d), F32)] * 2,
        in_specs=[any_spec] * 5,
        out_specs=[vmem] * 5,
        scratch_shapes=[
            pltpu.VMEM((W_SLOTS, W_CHUNK, 8, HEAD), BF16),
            pltpu.VMEM((W_SLOTS, W_CHUNK, 4, HEAD), BF16),
            pltpu.VMEM((W_SLOTS, W_CHUNK, 4, HEAD), BF16),
            pltpu.VMEM((d,), BF16),
            pltpu.VMEM((d,), BF16),
            pltpu.SemaphoreType.DMA((W_SLOTS, 3)),
            pltpu.SemaphoreType.DMA((2,)),
        ],
        compiler_params=pltpu.CompilerParams(vmem_limit_bytes=VMEM_BESIDE),
        cost_estimate=pl.CostEstimate(flops=5_000_000_000, bytes_accessed=20_000_000, transcendentals=0),
        name="heads",
    )(w_q, w_k, w_v, ga, gm)


def layer_kernel(n_att, n_ff, sizes, slot, tab_ref, over_ref, ga_ref, gm_ref, cos_ref, sin_ref, wh_ref, h_ref, wo_ref,
                 wg_ref, wu_ref, wd_ref, ck_ref, cv_ref, sib_ref, full_ref, fullf_ref, *rest):
    refs = iter(rest)
    a_ref, b_ref, d_ref, e_ref, o_ref = [next(refs) for _ in range(5)]
    if slot > 0:
        next(refs)
    out_refs = [next(refs) for _ in sizes]
    final_ref, h_rows, act, acc, stage, hist, ring_a, ring_b, sem, own_sem, ring_sem, out_sem = refs
    base = ROW * slot
    seq, start, x_pos, core = tab_ref[base], tab_ref[base + 4], tab_ref[base + 5], tab_ref[base + 6]
    place = tab_ref[base + 7]
    ovf = over_ref[0] > 0
    far = x_pos == 1

    def whole_copies(half):
        to = stage.at[pl.ds(half * HALF, HALF), :]
        fits = far & jnp.logical_not(ovf)
        found = [
            ((x_pos == 0) & (core != half), sib_ref.at[pl.ds(slot * HALF, HALF), :]),
            (far & ovf & (core == half), full_ref.at[place]),
            (far & ovf & (core != half), fullf_ref.at[place]),
        ]
        if half == 0:
            for who, places, ref in ((0, WHOLE_B, b_ref), (1, WHOLE_D, d_ref)):
                mine = 2 * slot + (who + slot) % 2
                if mine in places:
                    found.append((fits & (core == who), ref.at[pl.ds(places.index(mine) * HALF, HALF), :]))
        return [(c, pltpu.make_async_copy(src, to, sem.at[half])) for c, src in found]

    def unit_copies(half, u):
        at = pl.multiple_of((tab_ref[base + 8 + half] + u) * UNIT, UNIT)
        live = far & jnp.logical_not(ovf) & (u < tab_ref[base + 10 + half])
        to = stage.at[pl.ds(pl.multiple_of(half * HALF + u * UNIT, UNIT), UNIT), :]
        if half == 0:
            found = [(live & (core == 1), a_ref)] if slot < 2 else []
        else:
            found = [(live & (core == who), ref) for who, ref in ((0, e_ref), (1, o_ref))] if slot >= 2 else []
        return [(c, pltpu.make_async_copy(src.at[pl.ds(at, UNIT), :], to, sem.at[2 + u])) for c, src in found]

    def own_copies(half):
        rows = pl.ds(half * HALF, HALF)
        return (
            pltpu.make_async_copy(ck_ref.at[seq], hist.at[rows, pl.ds(0, WIDE)], own_sem.at[0]),
            pltpu.make_async_copy(cv_ref.at[seq], hist.at[rows, pl.ds(WIDE, WIDE)], own_sem.at[1]),
        )

    def history(act_on):
        for half in range(2):
            for cond, copy in whole_copies(half):
                @pl.when(cond)
                def _(copy=copy):
                    act_on(copy)

            @pl.when((x_pos == 0) & (core == half))
            def _(half=half):
                for copy in own_copies(half):
                    act_on(copy)

        packed = 0 if slot < 2 else 1

        @pl.loop(0, PER_HALF)
        def _(u):
            for cond, copy in unit_copies(packed, u):
                @pl.when(cond)
                def _(copy=copy):
                    act_on(copy)

    def up_copies(j):
        at = lax.rem(j, DEPTH)
        cols = pl.ds(pl.multiple_of(j * BLK, BLK), BLK)
        return [
            pltpu.make_async_copy(wg_ref.at[:, cols], ring_a.at[2 * at], ring_sem.at[at, 0]),
            pltpu.make_async_copy(wu_ref.at[:, cols], ring_a.at[2 * at + 1], ring_sem.at[at, 1]),
        ]

    def out_copy(i):
        at = lax.rem(i, DEPTH_B)
        rows = pl.ds(pl.multiple_of(i * OUT_BLK, OUT_BLK), OUT_BLK)
        return pltpu.make_async_copy(wo_ref.at[rows, :], ring_b.at[at, pl.ds(0, OUT_BLK), :], ring_sem.at[at, 2])

    def down_copy(j):
        at = lax.rem(j + n_att, DEPTH_B)
        rows = pl.ds(pl.multiple_of(j * BLK, BLK), BLK)
        return pltpu.make_async_copy(wd_ref.at[rows, :], ring_b.at[at], ring_sem.at[at, 2])

    row_copy = pltpu.make_async_copy(h_ref.at[seq], h_rows, own_sem.at[2])
    row_copy.start()
    history(lambda copy: copy.start())
    for i in range(DEPTH_B):
        out_copy(i).start()
    for j in range(DEPTH):
        for copy in up_copies(j):
            copy.start()
    row_copy.wait()
    act[...] = rms_norm(h_rows[...].astype(F32), ga_ref[...])

    @pl.loop(0, HEAD // UNIT)
    def _(u):
        rows = pl.ds(pl.multiple_of(u * UNIT, UNIT), UNIT)
        acc[rows, :] = h_rows[rows, :].astype(F32)

    history(lambda copy: copy.wait())
    for half in range(2):
        @pl.when((x_pos == 1) | (core != half))
        def _(half=half):
            @pl.loop(0, PER_HALF)
            def _(u):
                rows = pl.ds(pl.multiple_of(half * HALF + u * UNIT, UNIT), UNIT)
                hist[rows, :] = stage[rows, :].astype(BF16)

    @pl.loop(0, n_att)
    def _(i):
        out_copy(i).wait()
        cos, sin = cos_ref[pl.ds(start, HEAD), :], sin_ref[pl.ds(start, HEAD), :]
        a = act[...]
        off = pl.multiple_of(i * HEAD, HEAD)
        row = lax.broadcasted_iota(jnp.int32, (HEAD, HEAD), 0)
        v_old = jnp.where(row < start, hist[:, pl.ds(off + WIDE, HEAD)], jnp.zeros((), BF16))
        qkv = dot(a, wh_ref[i])
        kv = qkv[:, 512:]
        k_all = jnp.concatenate([hist[:, pl.ds(off, HEAD)], rotate(kv[:, :HEAD], cos, sin).astype(BF16)], axis=0)
        v_all = jnp.concatenate([v_old, kv[:, HEAD:].astype(BF16)], axis=0)
        qs = [(rotate(qkv[:, j * HEAD:(j + 1) * HEAD], cos, sin) * 0.0625).astype(BF16) for j in range(2)]
        row = lax.broadcasted_iota(jnp.int32, (HEAD, 512), 0)
        col = lax.broadcasted_iota(jnp.int32, (HEAD, 512), 1)
        ok = (col < start) | ((col >= HEAD) & (col - HEAD <= row))
        scores = [jnp.where(ok, dot_t(q, k_all), MASK_FLOOR) for q in qs]
        tops = [jnp.max(s, axis=-1, keepdims=True) for s in scores]
        probs = [jnp.exp(s - top) for s, top in zip(scores, tops)]
        dens = [jnp.sum(p, axis=-1, keepdims=True) for p in probs]
        nums = [dot(p.astype(BF16), v_all) for p in probs]
        heads = [(num / den).astype(BF16) for num, den in zip(nums, dens)]
        acc[...] += dot(jnp.concatenate(heads, axis=-1), ring_b[lax.rem(i, DEPTH_B), :OUT_BLK, :])

        @pl.when(i + DEPTH_B < n_att)
        def _():
            out_copy(i + DEPTH_B).start()

        @pl.when(i + DEPTH_B >= n_att)
        def _():
            down_copy(i + DEPTH_B - n_att).start()

    res = acc[...].astype(BF16).astype(F32)
    act[...] = rms_norm(res, gm_ref[...])
    acc[...] = res

    @pl.loop(0, n_ff)
    def _(j):
        at = lax.rem(j, DEPTH)
        for copy in up_copies(j):
            copy.wait()
        down_copy(j).wait()
        c = act[...]
        mid = (gelu_tanh(dot(c, ring_a[2 * at])) * dot(c, ring_a[2 * at + 1])).astype(BF16)
        acc[...] += dot(mid, ring_b[lax.rem(j + n_att, DEPTH_B)])

        @pl.when(j + DEPTH < n_ff)
        def _():
            for copy in up_copies(j + DEPTH):
                copy.start()

        @pl.when(j + DEPTH_B < n_ff)
        def _():
            down_copy(j + DEPTH_B).start()

    copies = []
    first = 0
    for k, size in enumerate(sizes):
        for r in range(0, size, STEP_ROWS):
            block = first // STEP_ROWS

            @pl.loop(0, STEP_ROWS // UNIT)
            def _(u, first=first):
                rows = pl.ds(pl.multiple_of(first + u * UNIT, UNIT), UNIT)
                rounded = acc[rows, :].astype(BF16)
                act[rows, :] = rounded
                acc[rows, :] = rounded.astype(F32)

            rows, to = pl.ds(first, STEP_ROWS), pl.ds(r, STEP_ROWS)
            copies.append(pltpu.make_async_copy(acc.at[rows, :], out_refs[k].at[to, :], out_sem.at[block, 0]))
            copies.append(pltpu.make_async_copy(act.at[rows, :], final_ref.at[seq, rows, :], out_sem.at[block, 1]))
            for copy in copies[-2:]:
                copy.start()
            first += STEP_ROWS
    for copy in copies:
        copy.wait()


def run_layer(slot, table, over, hidden, ga, gm, cos, sin, wh, wo, wg, wu, wd, ck, cv, sib, full, fullf, pieces, final, sizes):
    n_ff = wg.shape[1] // BLK
    any_spec = pl.BlockSpec(memory_space=pl.ANY)
    smem = pl.BlockSpec(memory_space=pltpu.SMEM)
    vmem = pl.BlockSpec(memory_space=pltpu.VMEM)
    d = hidden.shape[2]
    args = list(pieces) + ([final] if final is not None else [])
    flops = 2 * HEAD * d * (KV_WIDE * 2 + WIDE * 2 + 3 * wg.shape[1]) + 1_100_000_000
    return pl.pallas_call(
        functools.partial(layer_kernel, 4, n_ff, sizes, slot),
        out_shape=[pltpu.HBM((n, d), F32) for n in sizes] + [jax.ShapeDtypeStruct(hidden.shape, BF16)],
        in_specs=[smem, smem] + [vmem] * 5 + [any_spec] * (10 + len(args)),
        out_specs=[any_spec] * (len(sizes) + 1),
        input_output_aliases={17 + len(pieces): len(sizes)} if final is not None else {},
        scratch_shapes=[
            pltpu.VMEM((HEAD, d), BF16),
            pltpu.VMEM((HEAD, d), BF16),
            pltpu.VMEM((HEAD, d), F32),
            pltpu.VMEM((HEAD, KV_WIDE), F32),
            pltpu.VMEM((HEAD, KV_WIDE), BF16),
            pltpu.VMEM((2 * DEPTH, d, BLK), BF16),
            pltpu.VMEM((DEPTH_B, BLK, d), BF16),
            pltpu.SemaphoreType.DMA((2 + PER_HALF,)),
            pltpu.SemaphoreType.DMA((3,)),
            pltpu.SemaphoreType.DMA((DEPTH_B, 3)),
            pltpu.SemaphoreType.DMA((HEAD // STEP_ROWS, 2)),
        ],
        compiler_params=pltpu.CompilerParams(vmem_limit_bytes=VMEM_BESIDE),
        cost_estimate=pl.CostEstimate(flops=flops, bytes_accessed=160_000_000, transcendentals=0),
    )(table, over, ga, gm, cos, sin, wh, hidden, wo, wg, wu, wd, ck, cv, sib, full, fullf, *args)


def window_kernel(sc_ref, h_ref, ga_ref, cos_ref, sin_ref, wh_ref, ck_ref, cv_ref, ok_ref, ov_ref):
    step = pl.program_id(0)
    lo = lax.axis_index('cp') * HALF
    a_rows, inside = [], []
    for j in range(2):
        first = lo - sc_ref[2 * step + j]
        want = first + lax.broadcasted_iota(jnp.int32, (HALF, HEAD), 0)
        have = lax.broadcasted_iota(jnp.int32, (HALF, HEAD), 1)
        pick = jnp.where(want == have, 1.0, 0.0).astype(BF16)
        a_rows.append(dot(pick, h_ref[j]))
        idx = first + lax.broadcasted_iota(jnp.int32, (HALF, HEAD), 0)
        inside.append((idx >= 0) & (idx < HEAD))
    a = rms_norm(jnp.concatenate(a_rows, axis=0), ga_ref[...])
    here = pl.ds(pl.multiple_of(lo, HALF), HALF)
    cos = jnp.concatenate([cos_ref[here, :]] * 2, axis=0)
    sin = jnp.concatenate([sin_ref[here, :]] * 2, axis=0)
    for g in range(4):
        kv = dot(a, wh_ref[g, :, 512:])
        k = rotate(kv[:, :HEAD], cos, sin).astype(BF16)
        v = kv[:, HEAD:].astype(BF16)
        cols = slice(g * HEAD, (g + 1) * HEAD)
        for j in range(2):
            rows = slice(j * HALF, (j + 1) * HALF)
            ok_ref[j, :, cols] = jnp.where(inside[j], k[rows], ck_ref[j, :, cols])
            ov_ref[j, :, cols] = jnp.where(inside[j], v[rows], cv_ref[j, :, cols])


def write_windows(scalars, hidden, ga, cos, sin, wh, cache_k, cache_v):
    n_seq, rows, width = cache_k.shape
    d = hidden.shape[2]
    one = pl.Buffered(1)
    cache_spec = pl.BlockSpec((2, rows, width), lambda i, sc: (i, 0, 0))
    return pl.pallas_call(
        window_kernel,
        out_shape=[jax.ShapeDtypeStruct(cache_k.shape, BF16)] * 2,
        grid_spec=pltpu.PrefetchScalarGridSpec(
            num_scalar_prefetch=1,
            grid=(n_seq // 2,),
            in_specs=[
                pl.BlockSpec((2, HEAD, d), lambda i, sc: (i, 0, 0)),
                pl.BlockSpec(memory_space=pltpu.VMEM),
                pl.BlockSpec(memory_space=pltpu.VMEM),
                pl.BlockSpec(memory_space=pltpu.VMEM),
                pl.BlockSpec(memory_space=pltpu.VMEM),
                cache_spec,
                cache_spec,
            ],
            out_specs=[cache_spec, cache_spec],
        ),
        compiler_params=pltpu.CompilerParams(vmem_limit_bytes=VMEM_BESIDE),
        cost_estimate=pl.CostEstimate(flops=2 * n_seq * rows * d * 2 * width, bytes_accessed=60_000_000, transcendentals=0),
        name="cache_window",
    )(scalars, hidden, ga, cos, sin, wh, cache_k, cache_v)


def place_kernel(where, blk, tab_ref, *rest):
    n_part = len(where)
    parts = rest[:n_part]
    out_ref, wide, narrow, in_sem, out_sem = rest[-5:]
    slots = wide.shape[0]
    jobs = [(k, b) for k in range(n_part) for b in range(parts[k].shape[0] // blk)]

    def load(n):
        k, b = jobs[n]
        return pltpu.make_async_copy(parts[k].at[pl.ds(b * blk, blk), :], wide.at[n % slots], in_sem.at[n % slots])

    def store(n):
        k, b = jobs[n]
        entry, first = where[k]
        return pltpu.make_async_copy(narrow.at[n % slots], out_ref.at[tab_ref[entry], pl.ds(first + b * blk, blk), :],
                                     out_sem.at[n % slots])

    for n in range(min(slots, len(jobs))):
        load(n).start()
    for n in range(len(jobs)):
        load(n).wait()
        if n >= slots:
            store(n - slots).wait()

        @pl.loop(0, blk // 16)
        def _(r, n=n):
            rows = pl.ds(pl.multiple_of(r * 16, 16), 16)
            narrow[n % slots, rows, :] = wide[n % slots, rows, :].astype(BF16)

        store(n).start()
        if n + slots < len(jobs):
            load(n + slots).start()
    for n in range(max(0, len(jobs) - slots), len(jobs)):
        store(n).wait()


def place_rows(table, parts, where, out, blk):
    d = parts[0].shape[1]
    any_spec = pl.BlockSpec(memory_space=pl.ANY)
    n_part = len(parts)
    slots = min(8, sum(p.shape[0] // blk for p in parts))
    return pl.pallas_call(
        functools.partial(place_kernel, where, blk),
        out_shape=jax.ShapeDtypeStruct(out.shape, BF16),
        in_specs=[pl.BlockSpec(memory_space=pltpu.SMEM)] + [any_spec] * (n_part + 1),
        out_specs=any_spec,
        scratch_shapes=[
            pltpu.VMEM((slots, blk, d), F32),
            pltpu.VMEM((slots, blk, d), BF16),
            pltpu.SemaphoreType.DMA((slots,)),
            pltpu.SemaphoreType.DMA((slots,)),
        ],
        input_output_aliases={n_part + 1: 0},
        compiler_params=pltpu.CompilerParams(vmem_limit_bytes=VMEM_ALL),
        cost_estimate=pl.CostEstimate(flops=10_000_000, bytes_accessed=sum(p.size for p in parts) * 6, transcendentals=0),
    )(table, *parts, out)


def solution(mesh):
    d2d = [(0, 1), (1, 0), (2, 3), (3, 2)]
    cross = [(0, 2), (1, 3), (2, 0), (3, 1)]

    def send(x, pairs, axis='cp'):
        x = lax.ppermute(x, axis, pairs)
        return x

    def body(hidden, start_pos, cache_k, cache_v, w_q, w_k, w_v, w_o, w_gate, w_up, w_down, norm_attn, norm_mlp):
        n_seq, _, d = hidden.shape
        i32 = jnp.int32
        table, over, piece_a, piece_b, piece_e, piece_o = pack_call(
            pack_first_kernel, 4, "ABEO", A_ROWS + B_ROWS, A_UNITS + len(WHOLE_B))(start_pos, cache_k, cache_v)
        in_smem = lambda x: pltpu.with_memory_space_constraint(x, pltpu.SMEM)
        got_a = send(piece_a, [(0, 3)])
        got_b = send(piece_b, [(0, 2), (2, 0), (3, 1)])
        piece_s, piece_d = pack_call(
            pack_second_kernel, 0, "SD", S_ROWS + D_ROWS, 4 + len(WHOLE_D))(in_smem(table), cache_k, cache_v)
        sib = send(piece_s, [(0, 1), (1, 0)])
        got_d = send(piece_d, [(0, 3)])
        got_a, piece_e, piece_o = lax.optimization_barrier((got_a, piece_e, piece_o))
        got_e = send(piece_e, [(1, 2)])
        got_o = send(piece_o, [(1, 3)])

        def send_all(_):
            sid = jnp.arange(n_seq, dtype=i32)
            before = (start_pos[None, :] < start_pos[:, None]) | (
                (start_pos[None, :] == start_pos[:, None]) & (sid[None, :] < sid[:, None]))
            rank = jnp.sum(before.astype(i32), axis=1)
            order = jnp.sum((rank[None, :] == sid[:, None]).astype(i32) * sid[None, :], axis=1)
            got = lax.ppermute(pack_full(order, cache_k, cache_v), 'cp', [(0, 2), (1, 3)])
            return got, lax.ppermute(got, 'cp', [(2, 3), (3, 2)])

        full, full_f = lax.cond(over[0] > 0, send_all, lambda _: tuple(blank(2)), 0)

        w_q, w_k, w_v, full, full_f = lax.optimization_barrier((w_q, w_k, w_v, full, full_f))
        kept = split_heads(w_q, w_k, w_v, norm_attn, norm_mlp)
        wh, cos, sin, ga, gm = [pltpu.with_memory_space_constraint(x, pltpu.VMEM) for x in kept]
        wo = w_o.reshape(-1, d)

        out = None
        tab = table
        parts, where = [], []
        for t in range(4):
            pieces = (got_a, got_b if t > 0 else got_a) + ((got_d, got_e, got_o) if t > 1 else (got_a,) * 3)
            *own, out = run_layer(t, in_smem(tab), in_smem(over), hidden, ga, gm, cos, sin, wh, wo, w_gate, w_up, w_down,
                                  cache_k, cache_v, sib, full, full_f, pieces, out, (192, 64) if t == 3 else (HEAD,))
            tab, own = lax.optimization_barrier((tab, own))
            if t < 3:
                crs = send(own[0], cross)
                near = send(own[0], d2d)
                dia = send(crs, d2d)
                parts += [near, crs, dia]
                where += [(ROW * t + k, 0) for k in (1, 2, 3)]
        most, rest = own
        crs_most, near_most = send(most, cross), send(most, d2d)
        start_late, _ = lax.optimization_barrier((start_pos, tab))
        new_k, new_v = write_windows(start_late, hidden, ga, cos, sin, wh, cache_k, cache_v)
        rest, new_k = lax.optimization_barrier((rest, new_k))
        crs_rest, near_rest = send(rest, cross), send(rest, d2d)
        dia_most, dia_rest = send(crs_most, d2d), send(crs_rest, d2d)
        last = ROW * 3
        out = place_rows(in_smem(tab), parts + [near_most], where + [(last + 1, 0)], out, 64)
        out = place_rows(in_smem(tab), [crs_most, near_rest], [(last + 2, 0), (last + 1, 192)], out, 64)
        out = place_rows(in_smem(tab), [dia_most], [(last + 3, 0)], out, 64)
        out = place_rows(in_smem(tab), [crs_rest], [(last + 2, 192)], out, 16)
        out = place_rows(in_smem(tab), [dia_rest], [(last + 3, 192)], out, 16)
        return out, new_k, new_v

    group_spec = P('dp', None, None)
    cache_spec = P('dp', 'cp', None)
    whole_spec = P()
    return jax.shard_map(
        body,
        mesh=mesh,
        in_specs=(group_spec, P('dp'), cache_spec, cache_spec) + (whole_spec,) * 9,
        out_specs=(group_spec, cache_spec, cache_spec),
        check_vma=False,
    )
```

```python
import functools
import math

import jax
import jax.numpy as jnp
from jax import lax
from jax.experimental import pallas as pl
from jax.experimental.pallas import tpu as pltpu
from jax.sharding import PartitionSpec as P


NORM_EPS = 1e-6
ROPE_BASE = 1.0e4
MASK_FLOOR = -1.0e30
GELU_C = 0.7978845608028654

UNIT = 16
HALF = 128
HEAD = 2 * HALF
WIDE = 4 * HEAD
KV_WIDE = 2 * WIDE
PER_HALF = HALF // UNIT
A_UNITS, C_UNITS = 10, 5
WHOLE_B, WHOLE_D = (3, 4, 7), (5, 6)
A_ROWS, C_ROWS = A_UNITS * UNIT, C_UNITS * UNIT
B_ROWS, D_ROWS, S_ROWS = len(WHOLE_B) * HALF, len(WHOLE_D) * HALF, 4 * HALF
ROW = 16
OUT_BLK = 512
STEP_ROWS = 64
BLK = 768
VMEM_BESIDE = 47_500_000
VMEM_ALL = 66_900_000
DEPTH = 2
DEPTH_B = 3
F32 = jnp.float32
BF16 = jnp.bfloat16


def rms_norm(x, gain):
    inv = lax.rsqrt(jnp.mean(x * x, axis=-1, keepdims=True) + NORM_EPS)
    return (x * inv * (1.0 + gain)).astype(BF16)


def rotate(x, cos, sin):
    half = x.shape[-1] // 2
    first, second = x[:, :half], x[:, half:]
    return jnp.concatenate([first * cos - second * sin, second * cos + first * sin], axis=-1)


def gelu_tanh(x):
    return 0.5 * x * (1.0 + jnp.tanh(GELU_C * (x + 0.044715 * (x * x * x))))


def dot(a, b):
    return jnp.dot(a, b, preferred_element_type=F32)


def dot_t(a, b):
    return lax.dot_general(a, b, (((1,), (1,)), ((), ())), preferred_element_type=F32)


def sort_lengths(start_ref, order, length):
    starts = [start_ref[i] for i in range(16)]
    for i in range(16):
        rank = jnp.int32(0)
        for j in range(16):
            if j != i:
                ahead = (starts[j] <= starts[i]) if j < i else (starts[j] < starts[i])
                rank = rank + ahead.astype(jnp.int32)
        order[rank] = i
        length[rank] = starts[i]


def place_units(length, pos, cnt):
    over = jnp.int32(0)
    for half, places, room in ((0, (0,), 0), (0, (1, 2), A_UNITS), (1, (0, 1, 2, 3), 0), (1, (4, 7), C_UNITS), (1, (5, 6), C_UNITS)):
        at = jnp.int32(0)
        for j in places:
            n = jnp.clip((length[j] - half * HALF + UNIT - 1) // UNIT, 0, PER_HALF)
            pos[half * 8 + j] = at
            cnt[half * 8 + j] = n
            at = at + n
        over = over | (at > room).astype(jnp.int32)
    return over


def make_plan(start_ref, table, order, length, pos, cnt):
    me = lax.axis_index('cp')
    x_pos, core = me // 2, me % 2
    sort_lengths(start_ref, order, length)
    over = place_units(length, pos, cnt)
    for t in range(4):
        for k in range(4):
            xx = x_pos if k < 2 else 1 - x_pos
            cc = core if k % 2 == 0 else 1 - core
            place = 2 * t + (cc + t) % 2
            rank = 8 * (1 - xx) + place
            table[ROW * t + k] = order[rank]
            if k == 0:
                table[ROW * t + 4] = length[rank]
                table[ROW * t + 5] = x_pos
                table[ROW * t + 6] = core
                table[ROW * t + 7] = place
                for half in range(2):
                    table[ROW * t + 8 + half] = pos[half * 8 + place]
                    table[ROW * t + 10 + half] = jnp.clip((length[rank] - HALF * half + UNIT - 1) // UNIT, 0, PER_HALF)
    return over


PIECE_ROWS = dict(A=A_ROWS, B=B_ROWS, D=D_ROWS, E=C_ROWS, O=C_ROWS, S=S_ROWS)


def pack_kernel(by_core, first, ck_ref, cv_ref, table, order, pos, cnt, outs, raw, wide, in_sem, out_sem):
    me = lax.axis_index('cp')
    x_pos, core = me // 2, me % 2

    def copies(seq, row, to, rows, sem):
        return [pltpu.make_async_copy(src.at[seq, pl.ds(row, rows), :], raw.at[pl.ds(to, rows), pl.ds(side * WIDE, WIDE)],
                                      in_sem.at[sem, side]) for side, src in enumerate((ck_ref, cv_ref))]

    def units(half, j, to, sem, act):
        @pl.loop(0, PER_HALF)
        def _(u):
            at = pos[half * 8 + j] + u

            @pl.when((u < cnt[half * 8 + j]) & (at < (C_UNITS if half else A_UNITS)))
            def _():
                row = pl.multiple_of(u * UNIT, UNIT)
                for copy in copies(order[j], row, pl.multiple_of(to + at * UNIT, UNIT), UNIT, sem + at):
                    act(copy)

    def reads(name, act):
        if name in "AEO":
            half, places, sem = dict(A=(0, (1, 2), 0), E=(1, (4, 7), 0), O=(1, (5, 6), C_UNITS))[name]
            for j in places:
                units(half, j, first[name], sem, act)
            return
        if name == "S":
            seqs, sem = [table[ROW * t + 1] for t in range(4)], 0
        elif name == "D":
            seqs, sem = [table[ROW * t + 3] for t in (2, 3)], 4
        else:
            seqs, sem = [order[j] for j in WHOLE_B], A_UNITS
        for k, seq in enumerate(seqs):
            for copy in copies(seq, 0, first[name] + k * HALF, HALF, sem + k):
                act(copy)

    def out_copy(name):
        k = list(outs).index(name)
        return pltpu.make_async_copy(wide.at[pl.ds(first[name], PIECE_ROWS[name]), :], outs[name], out_sem.at[k])

    def widen(name):
        reads(name, lambda copy: copy.wait())

        @pl.loop(0, PIECE_ROWS[name] // UNIT)
        def _(u):
            rows = pl.ds(pl.multiple_of(first[name] + u * UNIT, UNIT), UNIT)
            wide[rows, :] = raw[rows, :].astype(F32)

        out_copy(name).start()

    def begin(name):
        reads(name, lambda copy: copy.start())

    def end(name):
        out_copy(name).wait()

    def phase(do):
        for who, names in enumerate(by_core):
            @pl.when((x_pos == 0) & (core == who))
            def _(names=names):
                for name in names:
                    do(name)

    return [functools.partial(phase, do) for do in (begin, widen, end)]


def pack_first_kernel(start_ref, ck_ref, cv_ref, table, over_ref, a_out, b_out, e_out, o_out, order, length, pos, cnt, *work):
    over_ref[0] = make_plan(start_ref, table, order, length, pos, cnt)
    outs = dict(A=a_out, B=b_out, E=e_out, O=o_out)
    for phase in pack_kernel(("AB", "EO"), dict(A=0, B=A_ROWS, E=0, O=C_ROWS), ck_ref, cv_ref, table, order, pos, cnt, outs, *work):
        phase()


def pack_work(rows, n_copy, n_out):
    return [
        pltpu.VMEM((rows, KV_WIDE), BF16),
        pltpu.VMEM((rows, KV_WIDE), F32),
        pltpu.SemaphoreType.DMA((n_copy, 2)),
        pltpu.SemaphoreType.DMA((n_out,)),
    ]


def plan_and_pack(start_pos, cache_k, cache_v):
    any_spec = pl.BlockSpec(memory_space=pl.ANY)
    smem = pl.BlockSpec(memory_space=pltpu.SMEM)
    return pl.pallas_call(
        pack_first_kernel,
        out_shape=[pltpu.SMEM((80,), jnp.int32), pltpu.SMEM((1,), jnp.int32)]
        + [pltpu.HBM((PIECE_ROWS[n], KV_WIDE), F32) for n in "ABEO"],
        in_specs=[smem, any_spec, any_spec],
        out_specs=[smem] * 2 + [any_spec] * 4,
        scratch_shapes=[pltpu.SMEM((16,), jnp.int32)] * 4 + pack_work(A_ROWS + B_ROWS, A_UNITS + len(WHOLE_B), 4),
        compiler_params=pltpu.CompilerParams(vmem_limit_bytes=VMEM_ALL),
        cost_estimate=pl.CostEstimate(flops=10_000_000, bytes_accessed=8_000_000, transcendentals=0),
        name="pack",
    )(start_pos, cache_k, cache_v)


def pack_full_kernel(order_ref, ck_ref, cv_ref, out_ref, raw, wide, sem):
    d = WIDE

    @pl.loop(0, 8)
    def _(j):
        seq = order_ref[j]
        copies = (
            pltpu.make_async_copy(ck_ref.at[seq], raw.at[:, pl.ds(0, d)], sem.at[0]),
            pltpu.make_async_copy(cv_ref.at[seq], raw.at[:, pl.ds(d, d)], sem.at[1]),
        )
        for copy in copies:
            copy.start()
        for copy in copies:
            copy.wait()
        wide[...] = raw[...].astype(F32)
        out = pltpu.make_async_copy(wide, out_ref.at[j], sem.at[2])
        out.start()
        out.wait()


def pack_full(order, cache_k, cache_v):
    any_spec = pl.BlockSpec(memory_space=pl.ANY)
    return pl.pallas_call(
        pack_full_kernel,
        out_shape=jax.ShapeDtypeStruct((8, HALF, KV_WIDE), F32),
        in_specs=[pl.BlockSpec(memory_space=pltpu.SMEM), any_spec, any_spec],
        out_specs=any_spec,
        scratch_shapes=[
            pltpu.VMEM((HALF, KV_WIDE), BF16),
            pltpu.VMEM((HALF, KV_WIDE), F32),
            pltpu.SemaphoreType.DMA((3,)),
        ],
        name="pack_full",
    )(order, cache_k, cache_v)


def blank_kernel(*refs):
    pass


def blank(count):
    return pl.pallas_call(
        blank_kernel,
        out_shape=[jax.ShapeDtypeStruct((8, HALF, KV_WIDE), F32)] * count,
        out_specs=[pl.BlockSpec(memory_space=pl.ANY)] * count,
        name="blank",
    )()


W_CHUNK = 384
W_SLOTS = 3


def heads_kernel(table, ck_ref, cv_ref, q_ref, k_ref, v_ref, ga_ref, gm_ref, out_ref, cos_ref, sin_ref, ga_out, gm_out,
                 s_out, d_out, raw_q, raw_k, raw_v, gain_a, gain_m, sem, gain_sem, *work):
    begin, widen, end = pack_kernel(("SD", "S"), dict(S=0, D=S_ROWS), ck_ref, cv_ref, table, table, None, None,
                                    dict(S=s_out, D=d_out), *work)
    begin()
    n_chunk = q_ref.shape[0] // W_CHUNK

    def copies(i, b):
        rows = pl.ds(pl.multiple_of(i * W_CHUNK, W_CHUNK), W_CHUNK)
        return [pltpu.make_async_copy(src.at[rows], dst.at[b], sem.at[b, j])
                for j, (src, dst) in enumerate(((q_ref, raw_q), (k_ref, raw_k), (v_ref, raw_v)))]

    def sorter(n_head):
        per = HEAD // n_head
        want = lax.broadcasted_iota(jnp.int32, (HEAD, HEAD), 0)
        have = lax.broadcasted_iota(jnp.int32, (HEAD, HEAD), 1)
        return jnp.where((want % per) * n_head + want // per == have, 1.0, 0.0).astype(BF16)

    for i in range(W_SLOTS):
        for copy in copies(i, i):
            copy.start()
    gains = [pltpu.make_async_copy(src, dst, gain_sem.at[k])
             for k, (src, dst) in enumerate(((ga_ref, gain_a), (gm_ref, gain_m)))]
    for copy in gains:
        copy.start()
    half = cos_ref.shape[1]
    freq = lax.broadcasted_iota(jnp.int32, (1, half), 1).astype(F32)
    inv_freq = jnp.exp(freq * (-2.0 / (2 * half) * math.log(ROPE_BASE)))
    big = (16 * lax.broadcasted_iota(jnp.int32, (32, half), 0)).astype(F32) * inv_freq
    small = lax.broadcasted_iota(jnp.int32, (16, half), 0).astype(F32) * inv_freq
    cos_a, sin_a, cos_b, sin_b = jnp.cos(big), jnp.sin(big), jnp.cos(small), jnp.sin(small)
    for r in range(32):
        rows = slice(16 * r, 16 * r + 16)
        ca, sa = cos_a[r:r + 1], sin_a[r:r + 1]
        cos_ref[rows, :] = ca * cos_b - sa * sin_b
        sin_ref[rows, :] = sa * cos_b + ca * sin_b

    sort8, sort4 = sorter(8), sorter(4)

    @pl.loop(0, n_chunk)
    def _(i):
        b = lax.rem(i, W_SLOTS)
        for copy in copies(i, b):
            copy.wait()
        for part in range(W_CHUNK // 64):
            to = pl.multiple_of(i * W_CHUNK, W_CHUNK) + part * 64
            for raw, n_head, sort, first in ((raw_q, 8, sort8, 0), (raw_k, 4, sort4, 2), (raw_v, 4, sort4, 3)):
                per = HEAD // n_head
                for sub in range(64 // per):
                    block = raw[b, part * 64 + sub * per:part * 64 + (sub + 1) * per].reshape(HEAD, HEAD)
                    moved = dot(sort, block).astype(BF16)
                    for h in range(n_head):
                        g, col = (h // 2, h % 2) if n_head == 8 else (h, first)
                        out_ref[g, pl.ds(to + sub * per, per), col * HEAD:(col + 1) * HEAD] = moved[h * per:(h + 1) * per]

        @pl.when(i + W_SLOTS < n_chunk)
        def _():
            for copy in copies(i + W_SLOTS, b):
                copy.start()

        @pl.when(i == 0)
        def _():
            widen()

    for copy, src, dst in zip(gains, (gain_a, gain_m), (ga_out, gm_out)):
        copy.wait()
        dst[...] = src[...].astype(F32).reshape(dst.shape)
    end()


def split_heads(table, cache_k, cache_v, w_q, w_k, w_v, ga, gm):
    d = w_q.shape[0]
    vmem = pl.BlockSpec(memory_space=pltpu.VMEM)
    any_spec = pl.BlockSpec(memory_space=pl.ANY)
    return pl.pallas_call(
        heads_kernel,
        out_shape=[pltpu.VMEM((4, d, WIDE), BF16)] + [pltpu.VMEM((2 * HEAD, HALF), F32)] * 2 + [pltpu.VMEM((1, d), F32)] * 2
        + [pltpu.HBM((PIECE_ROWS[n], KV_WIDE), F32) for n in "SD"],
        in_specs=[pl.BlockSpec(memory_space=pltpu.SMEM)] + [any_spec] * 7,
        out_specs=[vmem] * 5 + [any_spec] * 2,
        scratch_shapes=[
            pltpu.VMEM((W_SLOTS, W_CHUNK, 8, HEAD), BF16),
            pltpu.VMEM((W_SLOTS, W_CHUNK, 4, HEAD), BF16),
            pltpu.VMEM((W_SLOTS, W_CHUNK, 4, HEAD), BF16),
            pltpu.VMEM((d,), BF16),
            pltpu.VMEM((d,), BF16),
            pltpu.SemaphoreType.DMA((W_SLOTS, 3)),
            pltpu.SemaphoreType.DMA((2,)),
        ] + pack_work(S_ROWS + D_ROWS, 4 + len(WHOLE_D), 2),
        compiler_params=pltpu.CompilerParams(vmem_limit_bytes=VMEM_BESIDE),
        cost_estimate=pl.CostEstimate(flops=5_000_000_000, bytes_accessed=20_000_000, transcendentals=0),
        name="heads",
    )(table, cache_k, cache_v, w_q, w_k, w_v, ga, gm)


def layer_kernel(n_att, n_ff, sizes, slot, tab_ref, over_ref, ga_ref, gm_ref, cos_ref, sin_ref, wh_ref, h_ref, wo_ref,
                 wg_ref, wu_ref, wd_ref, ck_ref, cv_ref, sib_ref, full_ref, fullf_ref, *rest):
    refs = iter(rest)
    a_ref, b_ref, d_ref, e_ref, o_ref = [next(refs) for _ in range(5)]
    if slot > 0:
        next(refs)
    out_refs = [next(refs) for _ in sizes]
    final_ref, h_rows, act, acc, stage, hist, ring_a, ring_b, sem, own_sem, ring_sem, out_sem = refs
    base = ROW * slot
    seq, start, x_pos, core = tab_ref[base], tab_ref[base + 4], tab_ref[base + 5], tab_ref[base + 6]
    place = tab_ref[base + 7]
    ovf = over_ref[0] > 0
    far = x_pos == 1

    def whole_copies(half):
        to = stage.at[pl.ds(half * HALF, HALF), :]
        fits = far & jnp.logical_not(ovf)
        found = [
            ((x_pos == 0) & (core != half), sib_ref.at[pl.ds(slot * HALF, HALF), :]),
            (far & ovf & (core == half), full_ref.at[place]),
            (far & ovf & (core != half), fullf_ref.at[place]),
        ]
        if half == 0:
            for who, places, ref in ((0, WHOLE_B, b_ref), (1, WHOLE_D, d_ref)):
                mine = 2 * slot + (who + slot) % 2
                if mine in places:
                    found.append((fits & (core == who), ref.at[pl.ds(places.index(mine) * HALF, HALF), :]))
        return [(c, pltpu.make_async_copy(src, to, sem.at[half])) for c, src in found]

    def unit_copies(half, u):
        at = pl.multiple_of((tab_ref[base + 8 + half] + u) * UNIT, UNIT)
        live = far & jnp.logical_not(ovf) & (u < tab_ref[base + 10 + half])
        to = stage.at[pl.ds(pl.multiple_of(half * HALF + u * UNIT, UNIT), UNIT), :]
        if half == 0:
            found = [(live & (core == 1), a_ref)] if slot < 2 else []
        else:
            found = [(live & (core == who), ref) for who, ref in ((0, e_ref), (1, o_ref))] if slot >= 2 else []
        return [(c, pltpu.make_async_copy(src.at[pl.ds(at, UNIT), :], to, sem.at[2 + u])) for c, src in found]

    def own_copies(half):
        rows = pl.ds(half * HALF, HALF)
        return (
            pltpu.make_async_copy(ck_ref.at[seq], hist.at[rows, pl.ds(0, WIDE)], own_sem.at[0]),
            pltpu.make_async_copy(cv_ref.at[seq], hist.at[rows, pl.ds(WIDE, WIDE)], own_sem.at[1]),
        )

    def history(act_on):
        for half in range(2):
            for cond, copy in whole_copies(half):
                @pl.when(cond)
                def _(copy=copy):
                    act_on(copy)

            @pl.when((x_pos == 0) & (core == half))
            def _(half=half):
                for copy in own_copies(half):
                    act_on(copy)

        packed = 0 if slot < 2 else 1

        @pl.loop(0, PER_HALF)
        def _(u):
            for cond, copy in unit_copies(packed, u):
                @pl.when(cond)
                def _(copy=copy):
                    act_on(copy)

    def up_copies(j):
        at = lax.rem(j, DEPTH)
        cols = pl.ds(pl.multiple_of(j * BLK, BLK), BLK)
        return [
            pltpu.make_async_copy(wg_ref.at[:, cols], ring_a.at[2 * at], ring_sem.at[at, 0]),
            pltpu.make_async_copy(wu_ref.at[:, cols], ring_a.at[2 * at + 1], ring_sem.at[at, 1]),
        ]

    def out_copy(i):
        at = lax.rem(i, DEPTH_B)
        rows = pl.ds(pl.multiple_of(i * OUT_BLK, OUT_BLK), OUT_BLK)
        return pltpu.make_async_copy(wo_ref.at[rows, :], ring_b.at[at, pl.ds(0, OUT_BLK), :], ring_sem.at[at, 2])

    def down_copy(j):
        at = lax.rem(j + n_att, DEPTH_B)
        rows = pl.ds(pl.multiple_of(j * BLK, BLK), BLK)
        return pltpu.make_async_copy(wd_ref.at[rows, :], ring_b.at[at], ring_sem.at[at, 2])

    row_copy = pltpu.make_async_copy(h_ref.at[seq], h_rows, own_sem.at[2])
    row_copy.start()
    history(lambda copy: copy.start())
    for i in range(DEPTH_B):
        out_copy(i).start()
    for j in range(DEPTH):
        for copy in up_copies(j):
            copy.start()
    row_copy.wait()
    act[...] = rms_norm(h_rows[...].astype(F32), ga_ref[...])

    @pl.loop(0, HEAD // UNIT)
    def _(u):
        rows = pl.ds(pl.multiple_of(u * UNIT, UNIT), UNIT)
        acc[rows, :] = h_rows[rows, :].astype(F32)

    history(lambda copy: copy.wait())
    for half in range(2):
        @pl.when((x_pos == 1) | (core != half))
        def _(half=half):
            @pl.loop(0, PER_HALF)
            def _(u):
                rows = pl.ds(pl.multiple_of(half * HALF + u * UNIT, UNIT), UNIT)
                hist[rows, :] = stage[rows, :].astype(BF16)

    @pl.loop(0, n_att)
    def _(i):
        out_copy(i).wait()
        cos, sin = cos_ref[pl.ds(start, HEAD), :], sin_ref[pl.ds(start, HEAD), :]
        a = act[...]
        off = pl.multiple_of(i * HEAD, HEAD)
        row = lax.broadcasted_iota(jnp.int32, (HEAD, HEAD), 0)
        v_old = jnp.where(row < start, hist[:, pl.ds(off + WIDE, HEAD)], jnp.zeros((), BF16))
        qkv = dot(a, wh_ref[i])
        kv = qkv[:, 512:]
        k_all = jnp.concatenate([hist[:, pl.ds(off, HEAD)], rotate(kv[:, :HEAD], cos, sin).astype(BF16)], axis=0)
        v_all = jnp.concatenate([v_old, kv[:, HEAD:].astype(BF16)], axis=0)
        qs = [(rotate(qkv[:, j * HEAD:(j + 1) * HEAD], cos, sin) * 0.0625).astype(BF16) for j in range(2)]
        row = lax.broadcasted_iota(jnp.int32, (HEAD, 512), 0)
        col = lax.broadcasted_iota(jnp.int32, (HEAD, 512), 1)
        ok = (col < start) | ((col >= HEAD) & (col - HEAD <= row))
        scores = [jnp.where(ok, dot_t(q, k_all), MASK_FLOOR) for q in qs]
        tops = [jnp.max(s, axis=-1, keepdims=True) for s in scores]
        probs = [jnp.exp(s - top) for s, top in zip(scores, tops)]
        dens = [jnp.sum(p, axis=-1, keepdims=True) for p in probs]
        nums = [dot(p.astype(BF16), v_all) for p in probs]
        heads = [(num / den).astype(BF16) for num, den in zip(nums, dens)]
        acc[...] += dot(jnp.concatenate(heads, axis=-1), ring_b[lax.rem(i, DEPTH_B), :OUT_BLK, :])

        @pl.when(i + DEPTH_B < n_att)
        def _():
            out_copy(i + DEPTH_B).start()

        @pl.when(i + DEPTH_B >= n_att)
        def _():
            down_copy(i + DEPTH_B - n_att).start()

    res = acc[...].astype(BF16).astype(F32)
    act[...] = rms_norm(res, gm_ref[...])
    acc[...] = res

    @pl.loop(0, n_ff)
    def _(j):
        at = lax.rem(j, DEPTH)
        for copy in up_copies(j):
            copy.wait()
        down_copy(j).wait()
        c = act[...]
        mid = (gelu_tanh(dot(c, ring_a[2 * at])) * dot(c, ring_a[2 * at + 1])).astype(BF16)
        acc[...] += dot(mid, ring_b[lax.rem(j + n_att, DEPTH_B)])

        @pl.when(j + DEPTH < n_ff)
        def _():
            for copy in up_copies(j + DEPTH):
                copy.start()

        @pl.when(j + DEPTH_B < n_ff)
        def _():
            down_copy(j + DEPTH_B).start()

    copies = []
    first = 0
    for k, size in enumerate(sizes):
        for r in range(0, size, STEP_ROWS):
            block = first // STEP_ROWS

            @pl.loop(0, STEP_ROWS // UNIT)
            def _(u, first=first):
                rows = pl.ds(pl.multiple_of(first + u * UNIT, UNIT), UNIT)
                rounded = acc[rows, :].astype(BF16)
                act[rows, :] = rounded
                acc[rows, :] = rounded.astype(F32)

            rows, to = pl.ds(first, STEP_ROWS), pl.ds(r, STEP_ROWS)
            copies.append(pltpu.make_async_copy(acc.at[rows, :], out_refs[k].at[to, :], out_sem.at[block, 0]))
            copies.append(pltpu.make_async_copy(act.at[rows, :], final_ref.at[seq, rows, :], out_sem.at[block, 1]))
            for copy in copies[-2:]:
                copy.start()
            first += STEP_ROWS
    for copy in copies:
        copy.wait()


def run_layer(slot, table, over, hidden, ga, gm, cos, sin, wh, wo, wg, wu, wd, ck, cv, sib, full, fullf, pieces, final, sizes):
    n_ff = wg.shape[1] // BLK
    any_spec = pl.BlockSpec(memory_space=pl.ANY)
    smem = pl.BlockSpec(memory_space=pltpu.SMEM)
    vmem = pl.BlockSpec(memory_space=pltpu.VMEM)
    d = hidden.shape[2]
    args = list(pieces) + ([final] if final is not None else [])
    flops = 2 * HEAD * d * (KV_WIDE * 2 + WIDE * 2 + 3 * wg.shape[1]) + 1_100_000_000
    return pl.pallas_call(
        functools.partial(layer_kernel, 4, n_ff, sizes, slot),
        out_shape=[pltpu.HBM((n, d), F32) for n in sizes] + [jax.ShapeDtypeStruct(hidden.shape, BF16)],
        in_specs=[smem, smem] + [vmem] * 5 + [any_spec] * (10 + len(args)),
        out_specs=[any_spec] * (len(sizes) + 1),
        input_output_aliases={17 + len(pieces): len(sizes)} if final is not None else {},
        scratch_shapes=[
            pltpu.VMEM((HEAD, d), BF16),
            pltpu.VMEM((HEAD, d), BF16),
            pltpu.VMEM((HEAD, d), F32),
            pltpu.VMEM((HEAD, KV_WIDE), F32),
            pltpu.VMEM((HEAD, KV_WIDE), BF16),
            pltpu.VMEM((2 * DEPTH, d, BLK), BF16),
            pltpu.VMEM((DEPTH_B, BLK, d), BF16),
            pltpu.SemaphoreType.DMA((2 + PER_HALF,)),
            pltpu.SemaphoreType.DMA((3,)),
            pltpu.SemaphoreType.DMA((DEPTH_B, 3)),
            pltpu.SemaphoreType.DMA((HEAD // STEP_ROWS, 2)),
        ],
        compiler_params=pltpu.CompilerParams(vmem_limit_bytes=VMEM_BESIDE),
        cost_estimate=pl.CostEstimate(flops=flops, bytes_accessed=160_000_000, transcendentals=0),
    )(table, over, ga, gm, cos, sin, wh, hidden, wo, wg, wu, wd, ck, cv, sib, full, fullf, *args)


def window_kernel(sc_ref, h_ref, ga_ref, cos_ref, sin_ref, wh_ref, ck_ref, cv_ref, ok_ref, ov_ref):
    step = pl.program_id(0)
    lo = lax.axis_index('cp') * HALF
    a_rows, inside = [], []
    for j in range(2):
        first = lo - sc_ref[2 * step + j]
        want = first + lax.broadcasted_iota(jnp.int32, (HALF, HEAD), 0)
        have = lax.broadcasted_iota(jnp.int32, (HALF, HEAD), 1)
        pick = jnp.where(want == have, 1.0, 0.0).astype(BF16)
        a_rows.append(dot(pick, h_ref[j]))
        idx = first + lax.broadcasted_iota(jnp.int32, (HALF, HEAD), 0)
        inside.append((idx >= 0) & (idx < HEAD))
    a = rms_norm(jnp.concatenate(a_rows, axis=0), ga_ref[...])
    here = pl.ds(pl.multiple_of(lo, HALF), HALF)
    cos = jnp.concatenate([cos_ref[here, :]] * 2, axis=0)
    sin = jnp.concatenate([sin_ref[here, :]] * 2, axis=0)
    for g in range(4):
        kv = dot(a, wh_ref[g, :, 512:])
        k = rotate(kv[:, :HEAD], cos, sin).astype(BF16)
        v = kv[:, HEAD:].astype(BF16)
        cols = slice(g * HEAD, (g + 1) * HEAD)
        for j in range(2):
            rows = slice(j * HALF, (j + 1) * HALF)
            ok_ref[j, :, cols] = jnp.where(inside[j], k[rows], ck_ref[j, :, cols])
            ov_ref[j, :, cols] = jnp.where(inside[j], v[rows], cv_ref[j, :, cols])


def write_windows(scalars, hidden, ga, cos, sin, wh, cache_k, cache_v):
    n_seq, rows, width = cache_k.shape
    d = hidden.shape[2]
    one = pl.Buffered(1)
    cache_spec = pl.BlockSpec((2, rows, width), lambda i, sc: (i, 0, 0))
    return pl.pallas_call(
        window_kernel,
        out_shape=[jax.ShapeDtypeStruct(cache_k.shape, BF16)] * 2,
        grid_spec=pltpu.PrefetchScalarGridSpec(
            num_scalar_prefetch=1,
            grid=(n_seq // 2,),
            in_specs=[
                pl.BlockSpec((2, HEAD, d), lambda i, sc: (i, 0, 0)),
                pl.BlockSpec(memory_space=pltpu.VMEM),
                pl.BlockSpec(memory_space=pltpu.VMEM),
                pl.BlockSpec(memory_space=pltpu.VMEM),
                pl.BlockSpec(memory_space=pltpu.VMEM),
                cache_spec,
                cache_spec,
            ],
            out_specs=[cache_spec, cache_spec],
        ),
        compiler_params=pltpu.CompilerParams(vmem_limit_bytes=VMEM_BESIDE),
        cost_estimate=pl.CostEstimate(flops=2 * n_seq * rows * d * 2 * width, bytes_accessed=60_000_000, transcendentals=0),
        name="cache_window",
    )(scalars, hidden, ga, cos, sin, wh, cache_k, cache_v)


def place_kernel(where, blk, tab_ref, *rest):
    n_part = len(where)
    parts = rest[:n_part]
    out_ref, wide, narrow, in_sem, out_sem = rest[-5:]
    slots = wide.shape[0]
    jobs = [(k, b) for k in range(n_part) for b in range(parts[k].shape[0] // blk)]

    def load(n):
        k, b = jobs[n]
        return pltpu.make_async_copy(parts[k].at[pl.ds(b * blk, blk), :], wide.at[n % slots], in_sem.at[n % slots])

    def store(n):
        k, b = jobs[n]
        entry, first = where[k]
        return pltpu.make_async_copy(narrow.at[n % slots], out_ref.at[tab_ref[entry], pl.ds(first + b * blk, blk), :],
                                     out_sem.at[n % slots])

    for n in range(min(slots, len(jobs))):
        load(n).start()
    for n in range(len(jobs)):
        load(n).wait()
        if n >= slots:
            store(n - slots).wait()

        @pl.loop(0, blk // 16)
        def _(r, n=n):
            rows = pl.ds(pl.multiple_of(r * 16, 16), 16)
            narrow[n % slots, rows, :] = wide[n % slots, rows, :].astype(BF16)

        store(n).start()
        if n + slots < len(jobs):
            load(n + slots).start()
    for n in range(max(0, len(jobs) - slots), len(jobs)):
        store(n).wait()


def place_rows(table, parts, where, out, blk):
    d = parts[0].shape[1]
    any_spec = pl.BlockSpec(memory_space=pl.ANY)
    n_part = len(parts)
    slots = min(8, sum(p.shape[0] // blk for p in parts))
    return pl.pallas_call(
        functools.partial(place_kernel, where, blk),
        out_shape=jax.ShapeDtypeStruct(out.shape, BF16),
        in_specs=[pl.BlockSpec(memory_space=pltpu.SMEM)] + [any_spec] * (n_part + 1),
        out_specs=any_spec,
        scratch_shapes=[
            pltpu.VMEM((slots, blk, d), F32),
            pltpu.VMEM((slots, blk, d), BF16),
            pltpu.SemaphoreType.DMA((slots,)),
            pltpu.SemaphoreType.DMA((slots,)),
        ],
        input_output_aliases={n_part + 1: 0},
        compiler_params=pltpu.CompilerParams(vmem_limit_bytes=VMEM_ALL),
        cost_estimate=pl.CostEstimate(flops=10_000_000, bytes_accessed=sum(p.size for p in parts) * 6, transcendentals=0),
    )(table, *parts, out)


def solution(mesh):
    d2d = [(0, 1), (1, 0), (2, 3), (3, 2)]
    cross = [(0, 2), (1, 3), (2, 0), (3, 1)]

    def send(x, pairs, axis='cp'):
        x = lax.ppermute(x, axis, pairs)
        return x

    def body(hidden, start_pos, cache_k, cache_v, w_q, w_k, w_v, w_o, w_gate, w_up, w_down, norm_attn, norm_mlp):
        n_seq, _, d = hidden.shape
        i32 = jnp.int32
        table, over, piece_a, piece_b, piece_e, piece_o = plan_and_pack(start_pos, cache_k, cache_v)
        in_smem = lambda x: pltpu.with_memory_space_constraint(x, pltpu.SMEM)
        got_a = send(piece_a, [(0, 3)])
        got_b = send(piece_b, [(0, 2), (2, 0), (3, 1)])
        got_a, piece_e, piece_o = lax.optimization_barrier((got_a, piece_e, piece_o))
        got_e = send(piece_e, [(1, 2)])
        got_o = send(piece_o, [(1, 3)])

        def send_all(_):
            sid = jnp.arange(n_seq, dtype=i32)
            before = (start_pos[None, :] < start_pos[:, None]) | (
                (start_pos[None, :] == start_pos[:, None]) & (sid[None, :] < sid[:, None]))
            rank = jnp.sum(before.astype(i32), axis=1)
            order = jnp.sum((rank[None, :] == sid[:, None]).astype(i32) * sid[None, :], axis=1)
            got = lax.ppermute(pack_full(order, cache_k, cache_v), 'cp', [(0, 2), (1, 3)])
            return got, lax.ppermute(got, 'cp', [(2, 3), (3, 2)])

        full, full_f = lax.cond(over[0] > 0, send_all, lambda _: tuple(blank(2)), 0)

        w_q, w_k, w_v, full, full_f = lax.optimization_barrier((w_q, w_k, w_v, full, full_f))
        *kept, piece_s, piece_d = split_heads(in_smem(table), cache_k, cache_v, w_q, w_k, w_v, norm_attn, norm_mlp)
        sib = send(piece_s, [(0, 1), (1, 0)])
        got_d = send(piece_d, [(0, 3)])
        wh, cos, sin, ga, gm = [pltpu.with_memory_space_constraint(x, pltpu.VMEM) for x in kept]
        wo = w_o.reshape(-1, d)

        out = None
        tab = table
        parts, where = [], []
        for t in range(4):
            pieces = (got_a, got_b if t > 0 else got_a) + ((got_d, got_e, got_o) if t > 1 else (got_a,) * 3)
            *own, out = run_layer(t, in_smem(tab), in_smem(over), hidden, ga, gm, cos, sin, wh, wo, w_gate, w_up, w_down,
                                  cache_k, cache_v, sib, full, full_f, pieces, out, (192, 64) if t == 3 else (HEAD,))
            tab, own = lax.optimization_barrier((tab, own))
            if t < 3:
                crs = send(own[0], cross)
                near = send(own[0], d2d)
                dia = send(crs, d2d)
                parts += [near, crs, dia]
                where += [(ROW * t + k, 0) for k in (1, 2, 3)]
        most, rest = own
        crs_most, near_most = send(most, cross), send(most, d2d)
        start_late, _ = lax.optimization_barrier((start_pos, tab))
        new_k, new_v = write_windows(start_late, hidden, ga, cos, sin, wh, cache_k, cache_v)
        rest, new_k = lax.optimization_barrier((rest, new_k))
        crs_rest, near_rest = send(rest, cross), send(rest, d2d)
        dia_most, dia_rest = send(crs_most, d2d), send(crs_rest, d2d)
        last = ROW * 3
        out = place_rows(in_smem(tab), parts + [near_most], where + [(last + 1, 0)], out, 64)
        out = place_rows(in_smem(tab), [crs_most, near_rest], [(last + 2, 0), (last + 1, 192)], out, 64)
        out = place_rows(in_smem(tab), [dia_most], [(last + 3, 0)], out, 64)
        out = place_rows(in_smem(tab), [crs_rest], [(last + 2, 192)], out, 16)
        out = place_rows(in_smem(tab), [dia_rest], [(last + 3, 192)], out, 16)
        return out, new_k, new_v

    group_spec = P('dp', None, None)
    cache_spec = P('dp', 'cp', None)
    whole_spec = P()
    return jax.shard_map(
        body,
        mesh=mesh,
        in_specs=(group_spec, P('dp'), cache_spec, cache_spec) + (whole_spec,) * 9,
        out_specs=(group_spec, cache_spec, cache_spec),
        check_vma=False,
    )
```

```python
import functools
import math

import jax
import jax.numpy as jnp
from jax import lax
from jax.experimental import pallas as pl
from jax.experimental.pallas import tpu as pltpu
from jax.sharding import PartitionSpec as P


NORM_EPS = 1e-6
ROPE_BASE = 1.0e4
MASK_FLOOR = -1.0e30
GELU_C = 0.7978845608028654

UNIT = 16
HALF = 128
HEAD = 2 * HALF
WIDE = 4 * HEAD
KV_WIDE = 2 * WIDE
PER_HALF = HALF // UNIT
A_UNITS, C_UNITS = 10, 5
WHOLE_B, WHOLE_D = (3, 4, 7), (5, 6)
A_ROWS, C_ROWS = A_UNITS * UNIT, C_UNITS * UNIT
B_ROWS, D_ROWS, S_ROWS = len(WHOLE_B) * HALF, len(WHOLE_D) * HALF, 4 * HALF
ROW = 16
OUT_BLK = 512
STEP_ROWS = 64
BLK = 768
VMEM_BESIDE = 47_500_000
VMEM_ALL = 66_900_000
DEPTH = 2
DEPTH_B = 3
F32 = jnp.float32
BF16 = jnp.bfloat16


def rms_norm(x, gain):
    inv = lax.rsqrt(jnp.mean(x * x, axis=-1, keepdims=True) + NORM_EPS)
    return (x * inv * (1.0 + gain)).astype(BF16)


def rotate(x, cos, sin):
    half = x.shape[-1] // 2
    first, second = x[:, :half], x[:, half:]
    return jnp.concatenate([first * cos - second * sin, second * cos + first * sin], axis=-1)


def gelu_tanh(x):
    return 0.5 * x * (1.0 + jnp.tanh(GELU_C * (x + 0.044715 * (x * x * x))))


def dot(a, b):
    return jnp.dot(a, b, preferred_element_type=F32)


def dot_t(a, b):
    return lax.dot_general(a, b, (((1,), (1,)), ((), ())), preferred_element_type=F32)


def sort_lengths(start_ref, order, length):
    starts = [start_ref[i] for i in range(16)]
    for i in range(16):
        rank = jnp.int32(0)
        for j in range(16):
            if j != i:
                ahead = (starts[j] <= starts[i]) if j < i else (starts[j] < starts[i])
                rank = rank + ahead.astype(jnp.int32)
        order[rank] = i
        length[rank] = starts[i]


def place_units(length, pos, cnt):
    over = jnp.int32(0)
    for half, places, room in ((0, (0,), 0), (0, (1, 2), A_UNITS), (1, (0, 1, 2, 3), 0), (1, (4, 7), C_UNITS), (1, (5, 6), C_UNITS)):
        at = jnp.int32(0)
        for j in places:
            n = jnp.clip((length[j] - half * HALF + UNIT - 1) // UNIT, 0, PER_HALF)
            pos[half * 8 + j] = at
            cnt[half * 8 + j] = n
            at = at + n
        over = over | (at > room).astype(jnp.int32)
    return over


def make_plan(start_ref, table, order, length, pos, cnt):
    me = lax.axis_index('cp')
    x_pos, core = me // 2, me % 2
    sort_lengths(start_ref, order, length)
    over = place_units(length, pos, cnt)
    for t in range(4):
        for k in range(4):
            xx = x_pos if k < 2 else 1 - x_pos
            cc = core if k % 2 == 0 else 1 - core
            place = 2 * t + (cc + t) % 2
            rank = 8 * (1 - xx) + place
            table[ROW * t + k] = order[rank]
            if k == 0:
                table[ROW * t + 4] = length[rank]
                table[ROW * t + 5] = x_pos
                table[ROW * t + 6] = core
                table[ROW * t + 7] = place
                for half in range(2):
                    table[ROW * t + 8 + half] = pos[half * 8 + place]
                    table[ROW * t + 10 + half] = jnp.clip((length[rank] - HALF * half + UNIT - 1) // UNIT, 0, PER_HALF)
    return over


PIECE_ROWS = dict(A=A_ROWS, B=B_ROWS, D=D_ROWS, E=C_ROWS, O=C_ROWS, S=S_ROWS)


def pack_kernel(by_core, first, ck_ref, cv_ref, table, order, pos, cnt, outs, raw, wide, in_sem, out_sem):
    me = lax.axis_index('cp')
    x_pos, core = me // 2, me % 2

    def copies(seq, row, to, rows, sem):
        return [pltpu.make_async_copy(src.at[seq, pl.ds(row, rows), :], raw.at[pl.ds(to, rows), pl.ds(side * WIDE, WIDE)],
                                      in_sem.at[sem, side]) for side, src in enumerate((ck_ref, cv_ref))]

    def units(half, j, to, sem, act):
        @pl.loop(0, PER_HALF)
        def _(u):
            at = pos[half * 8 + j] + u

            @pl.when((u < cnt[half * 8 + j]) & (at < (C_UNITS if half else A_UNITS)))
            def _():
                row = pl.multiple_of(u * UNIT, UNIT)
                for copy in copies(order[j], row, pl.multiple_of(to + at * UNIT, UNIT), UNIT, sem + at):
                    act(copy)

    def reads(name, act):
        if name in "AEO":
            half, places, sem = dict(A=(0, (1, 2), 0), E=(1, (4, 7), 0), O=(1, (5, 6), C_UNITS))[name]
            for j in places:
                units(half, j, first[name], sem, act)
            return
        if name == "S":
            seqs, sem = [table[ROW * t + 1] for t in range(4)], 0
        elif name == "D":
            seqs, sem = [table[ROW * t + 3] for t in (2, 3)], 4
        else:
            seqs, sem = [order[j] for j in WHOLE_B], A_UNITS
        for k, seq in enumerate(seqs):
            for copy in copies(seq, 0, first[name] + k * HALF, HALF, sem + k):
                act(copy)

    def out_copy(name):
        k = list(outs).index(name)
        return pltpu.make_async_copy(wide.at[pl.ds(first[name], PIECE_ROWS[name]), :], outs[name], out_sem.at[k])

    def widen(name):
        reads(name, lambda copy: copy.wait())

        @pl.loop(0, PIECE_ROWS[name] // UNIT)
        def _(u):
            rows = pl.ds(pl.multiple_of(first[name] + u * UNIT, UNIT), UNIT)
            wide[rows, :] = raw[rows, :].astype(F32)

        out_copy(name).start()

    def begin(name):
        reads(name, lambda copy: copy.start())

    def end(name):
        out_copy(name).wait()

    def phase(do):
        for who, names in enumerate(by_core):
            @pl.when((x_pos == 0) & (core == who))
            def _(names=names):
                for name in names:
                    do(name)

    return [functools.partial(phase, do) for do in (begin, widen, end)]


def pack_first_kernel(start_ref, ck_ref, cv_ref, table, over_ref, a_out, b_out, e_out, o_out, order, length, pos, cnt, *work):
    over_ref[0] = make_plan(start_ref, table, order, length, pos, cnt)
    outs = dict(A=a_out, B=b_out, E=e_out, O=o_out)
    for phase in pack_kernel(("AB", "EO"), dict(A=0, B=A_ROWS, E=0, O=C_ROWS), ck_ref, cv_ref, table, order, pos, cnt, outs, *work):
        phase()


def pack_work(rows, n_copy, n_out):
    return [
        pltpu.VMEM((rows, KV_WIDE), BF16),
        pltpu.VMEM((rows, KV_WIDE), F32),
        pltpu.SemaphoreType.DMA((n_copy, 2)),
        pltpu.SemaphoreType.DMA((n_out,)),
    ]


def plan_and_pack(start_pos, cache_k, cache_v):
    any_spec = pl.BlockSpec(memory_space=pl.ANY)
    smem = pl.BlockSpec(memory_space=pltpu.SMEM)
    return pl.pallas_call(
        pack_first_kernel,
        out_shape=[pltpu.SMEM((80,), jnp.int32), pltpu.SMEM((1,), jnp.int32)]
        + [pltpu.HBM((PIECE_ROWS[n], KV_WIDE), F32) for n in "ABEO"],
        in_specs=[smem, any_spec, any_spec],
        out_specs=[smem] * 2 + [any_spec] * 4,
        scratch_shapes=[pltpu.SMEM((16,), jnp.int32)] * 4 + pack_work(A_ROWS + B_ROWS, A_UNITS + len(WHOLE_B), 4),
        compiler_params=pltpu.CompilerParams(vmem_limit_bytes=VMEM_ALL),
        cost_estimate=pl.CostEstimate(flops=10_000_000, bytes_accessed=8_000_000, transcendentals=0),
        name="pack",
    )(start_pos, cache_k, cache_v)


def pack_full_kernel(order_ref, ck_ref, cv_ref, out_ref, raw, wide, sem):
    d = WIDE

    @pl.loop(0, 8)
    def _(j):
        seq = order_ref[j]
        copies = (
            pltpu.make_async_copy(ck_ref.at[seq], raw.at[:, pl.ds(0, d)], sem.at[0]),
            pltpu.make_async_copy(cv_ref.at[seq], raw.at[:, pl.ds(d, d)], sem.at[1]),
        )
        for copy in copies:
            copy.start()
        for copy in copies:
            copy.wait()
        wide[...] = raw[...].astype(F32)
        out = pltpu.make_async_copy(wide, out_ref.at[j], sem.at[2])
        out.start()
        out.wait()


def pack_full(order, cache_k, cache_v):
    any_spec = pl.BlockSpec(memory_space=pl.ANY)
    return pl.pallas_call(
        pack_full_kernel,
        out_shape=jax.ShapeDtypeStruct((8, HALF, KV_WIDE), F32),
        in_specs=[pl.BlockSpec(memory_space=pltpu.SMEM), any_spec, any_spec],
        out_specs=any_spec,
        scratch_shapes=[
            pltpu.VMEM((HALF, KV_WIDE), BF16),
            pltpu.VMEM((HALF, KV_WIDE), F32),
            pltpu.SemaphoreType.DMA((3,)),
        ],
        name="pack_full",
    )(order, cache_k, cache_v)


def blank_kernel(*refs):
    pass


def blank(count):
    return pl.pallas_call(
        blank_kernel,
        out_shape=[jax.ShapeDtypeStruct((8, HALF, KV_WIDE), F32)] * count,
        out_specs=[pl.BlockSpec(memory_space=pl.ANY)] * count,
        name="blank",
    )()


W_CHUNK = 384
W_SLOTS = 3


def heads_kernel(table, ck_ref, cv_ref, q_ref, k_ref, v_ref, ga_ref, gm_ref, out_ref, cos_ref, sin_ref, ga_out, gm_out,
                 s_out, d_out, raw_q, raw_k, raw_v, gain_a, gain_m, sem, gain_sem, *work):
    begin, widen, end = pack_kernel(("SD", "S"), dict(S=0, D=S_ROWS), ck_ref, cv_ref, table, table, None, None,
                                    dict(S=s_out, D=d_out), *work)
    begin()
    n_chunk = q_ref.shape[0] // W_CHUNK

    def copies(i, b):
        rows = pl.ds(pl.multiple_of(i * W_CHUNK, W_CHUNK), W_CHUNK)
        return [pltpu.make_async_copy(src.at[rows], dst.at[b], sem.at[b, j])
                for j, (src, dst) in enumerate(((q_ref, raw_q), (k_ref, raw_k), (v_ref, raw_v)))]

    def sorter(n_head):
        per = HEAD // n_head
        want = lax.broadcasted_iota(jnp.int32, (HEAD, HEAD), 0)
        have = lax.broadcasted_iota(jnp.int32, (HEAD, HEAD), 1)
        return jnp.where((want % per) * n_head + want // per == have, 1.0, 0.0).astype(BF16)

    for i in range(W_SLOTS):
        for copy in copies(i, i):
            copy.start()
    gains = [pltpu.make_async_copy(src, dst, gain_sem.at[k])
             for k, (src, dst) in enumerate(((ga_ref, gain_a), (gm_ref, gain_m)))]
    for copy in gains:
        copy.start()
    half = cos_ref.shape[1]
    freq = lax.broadcasted_iota(jnp.int32, (1, half), 1).astype(F32)
    inv_freq = jnp.exp(freq * (-2.0 / (2 * half) * math.log(ROPE_BASE)))
    big = (16 * lax.broadcasted_iota(jnp.int32, (32, half), 0)).astype(F32) * inv_freq
    small = lax.broadcasted_iota(jnp.int32, (16, half), 0).astype(F32) * inv_freq
    cos_a, sin_a, cos_b, sin_b = jnp.cos(big), jnp.sin(big), jnp.cos(small), jnp.sin(small)
    for r in range(32):
        rows = slice(16 * r, 16 * r + 16)
        ca, sa = cos_a[r:r + 1], sin_a[r:r + 1]
        cos_ref[rows, :] = ca * cos_b - sa * sin_b
        sin_ref[rows, :] = sa * cos_b + ca * sin_b

    sort8, sort4 = sorter(8), sorter(4)

    @pl.loop(0, n_chunk)
    def _(i):
        b = lax.rem(i, W_SLOTS)
        for copy in copies(i, b):
            copy.wait()
        for part in range(W_CHUNK // 64):
            to = pl.multiple_of(i * W_CHUNK, W_CHUNK) + part * 64
            for raw, n_head, sort, first in ((raw_q, 8, sort8, 0), (raw_k, 4, sort4, 2), (raw_v, 4, sort4, 3)):
                per = HEAD // n_head
                for sub in range(64 // per):
                    block = raw[b, part * 64 + sub * per:part * 64 + (sub + 1) * per].reshape(HEAD, HEAD)
                    moved = dot(sort, block).astype(BF16)
                    for h in range(n_head):
                        g, col = (h // 2, h % 2) if n_head == 8 else (h, first)
                        out_ref[g, pl.ds(to + sub * per, per), col * HEAD:(col + 1) * HEAD] = moved[h * per:(h + 1) * per]

        @pl.when(i + W_SLOTS < n_chunk)
        def _():
            for copy in copies(i + W_SLOTS, b):
                copy.start()

        @pl.when(i == 2)
        def _():
            widen()

    for copy, src, dst in zip(gains, (gain_a, gain_m), (ga_out, gm_out)):
        copy.wait()
        dst[...] = src[...].astype(F32).reshape(dst.shape)
    end()


def split_heads(table, cache_k, cache_v, w_q, w_k, w_v, ga, gm):
    d = w_q.shape[0]
    vmem = pl.BlockSpec(memory_space=pltpu.VMEM)
    any_spec = pl.BlockSpec(memory_space=pl.ANY)
    return pl.pallas_call(
        heads_kernel,
        out_shape=[pltpu.VMEM((4, d, WIDE), BF16)] + [pltpu.VMEM((2 * HEAD, HALF), F32)] * 2 + [pltpu.VMEM((1, d), F32)] * 2
        + [pltpu.HBM((PIECE_ROWS[n], KV_WIDE), F32) for n in "SD"],
        in_specs=[pl.BlockSpec(memory_space=pltpu.SMEM)] + [any_spec] * 7,
        out_specs=[vmem] * 5 + [any_spec] * 2,
        scratch_shapes=[
            pltpu.VMEM((W_SLOTS, W_CHUNK, 8, HEAD), BF16),
            pltpu.VMEM((W_SLOTS, W_CHUNK, 4, HEAD), BF16),
            pltpu.VMEM((W_SLOTS, W_CHUNK, 4, HEAD), BF16),
            pltpu.VMEM((d,), BF16),
            pltpu.VMEM((d,), BF16),
            pltpu.SemaphoreType.DMA((W_SLOTS, 3)),
            pltpu.SemaphoreType.DMA((2,)),
        ] + pack_work(S_ROWS + D_ROWS, 4 + len(WHOLE_D), 2),
        compiler_params=pltpu.CompilerParams(vmem_limit_bytes=VMEM_BESIDE),
        cost_estimate=pl.CostEstimate(flops=5_000_000_000, bytes_accessed=20_000_000, transcendentals=0),
        name="heads",
    )(table, cache_k, cache_v, w_q, w_k, w_v, ga, gm)


def layer_kernel(n_att, n_ff, sizes, slot, tab_ref, over_ref, ga_ref, gm_ref, cos_ref, sin_ref, wh_ref, h_ref, wo_ref,
                 wg_ref, wu_ref, wd_ref, ck_ref, cv_ref, sib_ref, full_ref, fullf_ref, *rest):
    refs = iter(rest)
    a_ref, b_ref, d_ref, e_ref, o_ref = [next(refs) for _ in range(5)]
    if slot > 0:
        next(refs)
    out_refs = [next(refs) for _ in sizes]
    final_ref, h_rows, act, acc, stage, hist, ring_a, ring_b, sem, own_sem, ring_sem, out_sem = refs
    base = ROW * slot
    seq, start, x_pos, core = tab_ref[base], tab_ref[base + 4], tab_ref[base + 5], tab_ref[base + 6]
    place = tab_ref[base + 7]
    ovf = over_ref[0] > 0
    far = x_pos == 1

    def whole_copies(half):
        to = stage.at[pl.ds(half * HALF, HALF), :]
        fits = far & jnp.logical_not(ovf)
        found = [
            ((x_pos == 0) & (core != half), sib_ref.at[pl.ds(slot * HALF, HALF), :]),
            (far & ovf & (core == half), full_ref.at[place]),
            (far & ovf & (core != half), fullf_ref.at[place]),
        ]
        if half == 0:
            for who, places, ref in ((0, WHOLE_B, b_ref), (1, WHOLE_D, d_ref)):
                mine = 2 * slot + (who + slot) % 2
                if mine in places:
                    found.append((fits & (core == who), ref.at[pl.ds(places.index(mine) * HALF, HALF), :]))
        return [(c, pltpu.make_async_copy(src, to, sem.at[half])) for c, src in found]

    def unit_copies(half, u):
        at = pl.multiple_of((tab_ref[base + 8 + half] + u) * UNIT, UNIT)
        live = far & jnp.logical_not(ovf) & (u < tab_ref[base + 10 + half])
        to = stage.at[pl.ds(pl.multiple_of(half * HALF + u * UNIT, UNIT), UNIT), :]
        if half == 0:
            found = [(live & (core == 1), a_ref)] if slot < 2 else []
        else:
            found = [(live & (core == who), ref) for who, ref in ((0, e_ref), (1, o_ref))] if slot >= 2 else []
        return [(c, pltpu.make_async_copy(src.at[pl.ds(at, UNIT), :], to, sem.at[2 + u])) for c, src in found]

    def own_copies(half):
        rows = pl.ds(half * HALF, HALF)
        return (
            pltpu.make_async_copy(ck_ref.at[seq], hist.at[rows, pl.ds(0, WIDE)], own_sem.at[0]),
            pltpu.make_async_copy(cv_ref.at[seq], hist.at[rows, pl.ds(WIDE, WIDE)], own_sem.at[1]),
        )

    def history(act_on):
        for half in range(2):
            for cond, copy in whole_copies(half):
                @pl.when(cond)
                def _(copy=copy):
                    act_on(copy)

            @pl.when((x_pos == 0) & (core == half))
            def _(half=half):
                for copy in own_copies(half):
                    act_on(copy)

        packed = 0 if slot < 2 else 1

        @pl.loop(0, PER_HALF)
        def _(u):
            for cond, copy in unit_copies(packed, u):
                @pl.when(cond)
                def _(copy=copy):
                    act_on(copy)

    def up_copies(j):
        at = lax.rem(j, DEPTH)
        cols = pl.ds(pl.multiple_of(j * BLK, BLK), BLK)
        return [
            pltpu.make_async_copy(wg_ref.at[:, cols], ring_a.at[2 * at], ring_sem.at[at, 0]),
            pltpu.make_async_copy(wu_ref.at[:, cols], ring_a.at[2 * at + 1], ring_sem.at[at, 1]),
        ]

    def out_copy(i):
        at = lax.rem(i, DEPTH_B)
        rows = pl.ds(pl.multiple_of(i * OUT_BLK, OUT_BLK), OUT_BLK)
        return pltpu.make_async_copy(wo_ref.at[rows, :], ring_b.at[at, pl.ds(0, OUT_BLK), :], ring_sem.at[at, 2])

    def down_copy(j):
        at = lax.rem(j + n_att, DEPTH_B)
        rows = pl.ds(pl.multiple_of(j * BLK, BLK), BLK)
        return pltpu.make_async_copy(wd_ref.at[rows, :], ring_b.at[at], ring_sem.at[at, 2])

    row_copy = pltpu.make_async_copy(h_ref.at[seq], h_rows, own_sem.at[2])
    row_copy.start()
    history(lambda copy: copy.start())
    for i in range(DEPTH_B):
        out_copy(i).start()
    for j in range(DEPTH):
        for copy in up_copies(j):
            copy.start()
    row_copy.wait()
    act[...] = rms_norm(h_rows[...].astype(F32), ga_ref[...])

    @pl.loop(0, HEAD // UNIT)
    def _(u):
        rows = pl.ds(pl.multiple_of(u * UNIT, UNIT), UNIT)
        acc[rows, :] = h_rows[rows, :].astype(F32)

    history(lambda copy: copy.wait())
    for half in range(2):
        @pl.when((x_pos == 1) | (core != half))
        def _(half=half):
            @pl.loop(0, PER_HALF)
            def _(u):
                rows = pl.ds(pl.multiple_of(half * HALF + u * UNIT, UNIT), UNIT)
                hist[rows, :] = stage[rows, :].astype(BF16)

    @pl.loop(0, n_att)
    def _(i):
        out_copy(i).wait()
        cos, sin = cos_ref[pl.ds(start, HEAD), :], sin_ref[pl.ds(start, HEAD), :]
        a = act[...]
        off = pl.multiple_of(i * HEAD, HEAD)
        row = lax.broadcasted_iota(jnp.int32, (HEAD, HEAD), 0)
        v_old = jnp.where(row < start, hist[:, pl.ds(off + WIDE, HEAD)], jnp.zeros((), BF16))
        qkv = dot(a, wh_ref[i])
        kv = qkv[:, 512:]
        k_all = jnp.concatenate([hist[:, pl.ds(off, HEAD)], rotate(kv[:, :HEAD], cos, sin).astype(BF16)], axis=0)
        v_all = jnp.concatenate([v_old, kv[:, HEAD:].astype(BF16)], axis=0)
        qs = [(rotate(qkv[:, j * HEAD:(j + 1) * HEAD], cos, sin) * 0.0625).astype(BF16) for j in range(2)]
        row = lax.broadcasted_iota(jnp.int32, (HEAD, 512), 0)
        col = lax.broadcasted_iota(jnp.int32, (HEAD, 512), 1)
        ok = (col < start) | ((col >= HEAD) & (col - HEAD <= row))
        scores = [jnp.where(ok, dot_t(q, k_all), MASK_FLOOR) for q in qs]
        tops = [jnp.max(s, axis=-1, keepdims=True) for s in scores]
        probs = [jnp.exp(s - top) for s, top in zip(scores, tops)]
        dens = [jnp.sum(p, axis=-1, keepdims=True) for p in probs]
        nums = [dot(p.astype(BF16), v_all) for p in probs]
        heads = [(num / den).astype(BF16) for num, den in zip(nums, dens)]
        acc[...] += dot(jnp.concatenate(heads, axis=-1), ring_b[lax.rem(i, DEPTH_B), :OUT_BLK, :])

        @pl.when(i + DEPTH_B < n_att)
        def _():
            out_copy(i + DEPTH_B).start()

        @pl.when(i + DEPTH_B >= n_att)
        def _():
            down_copy(i + DEPTH_B - n_att).start()

    res = acc[...].astype(BF16).astype(F32)
    act[...] = rms_norm(res, gm_ref[...])
    acc[...] = res

    @pl.loop(0, n_ff)
    def _(j):
        at = lax.rem(j, DEPTH)
        for copy in up_copies(j):
            copy.wait()
        down_copy(j).wait()
        c = act[...]
        mid = (gelu_tanh(dot(c, ring_a[2 * at])) * dot(c, ring_a[2 * at + 1])).astype(BF16)
        acc[...] += dot(mid, ring_b[lax.rem(j + n_att, DEPTH_B)])

        @pl.when(j + DEPTH < n_ff)
        def _():
            for copy in up_copies(j + DEPTH):
                copy.start()

        @pl.when(j + DEPTH_B < n_ff)
        def _():
            down_copy(j + DEPTH_B).start()

    copies = []
    first = 0
    for k, size in enumerate(sizes):
        for r in range(0, size, STEP_ROWS):
            block = first // STEP_ROWS

            @pl.loop(0, STEP_ROWS // UNIT)
            def _(u, first=first):
                rows = pl.ds(pl.multiple_of(first + u * UNIT, UNIT), UNIT)
                rounded = acc[rows, :].astype(BF16)
                act[rows, :] = rounded
                acc[rows, :] = rounded.astype(F32)

            rows, to = pl.ds(first, STEP_ROWS), pl.ds(r, STEP_ROWS)
            copies.append(pltpu.make_async_copy(acc.at[rows, :], out_refs[k].at[to, :], out_sem.at[block, 0]))
            copies.append(pltpu.make_async_copy(act.at[rows, :], final_ref.at[seq, rows, :], out_sem.at[block, 1]))
            for copy in copies[-2:]:
                copy.start()
            first += STEP_ROWS
    for copy in copies:
        copy.wait()


def run_layer(slot, table, over, hidden, ga, gm, cos, sin, wh, wo, wg, wu, wd, ck, cv, sib, full, fullf, pieces, final, sizes):
    n_ff = wg.shape[1] // BLK
    any_spec = pl.BlockSpec(memory_space=pl.ANY)
    smem = pl.BlockSpec(memory_space=pltpu.SMEM)
    vmem = pl.BlockSpec(memory_space=pltpu.VMEM)
    d = hidden.shape[2]
    args = list(pieces) + ([final] if final is not None else [])
    flops = 2 * HEAD * d * (KV_WIDE * 2 + WIDE * 2 + 3 * wg.shape[1]) + 1_100_000_000
    return pl.pallas_call(
        functools.partial(layer_kernel, 4, n_ff, sizes, slot),
        out_shape=[pltpu.HBM((n, d), F32) for n in sizes] + [jax.ShapeDtypeStruct(hidden.shape, BF16)],
        in_specs=[smem, smem] + [vmem] * 5 + [any_spec] * (10 + len(args)),
        out_specs=[any_spec] * (len(sizes) + 1),
        input_output_aliases={17 + len(pieces): len(sizes)} if final is not None else {},
        scratch_shapes=[
            pltpu.VMEM((HEAD, d), BF16),
            pltpu.VMEM((HEAD, d), BF16),
            pltpu.VMEM((HEAD, d), F32),
            pltpu.VMEM((HEAD, KV_WIDE), F32),
            pltpu.VMEM((HEAD, KV_WIDE), BF16),
            pltpu.VMEM((2 * DEPTH, d, BLK), BF16),
            pltpu.VMEM((DEPTH_B, BLK, d), BF16),
            pltpu.SemaphoreType.DMA((2 + PER_HALF,)),
            pltpu.SemaphoreType.DMA((3,)),
            pltpu.SemaphoreType.DMA((DEPTH_B, 3)),
            pltpu.SemaphoreType.DMA((HEAD // STEP_ROWS, 2)),
        ],
        compiler_params=pltpu.CompilerParams(vmem_limit_bytes=VMEM_BESIDE),
        cost_estimate=pl.CostEstimate(flops=flops, bytes_accessed=160_000_000, transcendentals=0),
    )(table, over, ga, gm, cos, sin, wh, hidden, wo, wg, wu, wd, ck, cv, sib, full, fullf, *args)


def window_kernel(sc_ref, h_ref, ga_ref, cos_ref, sin_ref, wh_ref, ck_ref, cv_ref, ok_ref, ov_ref):
    step = pl.program_id(0)
    lo = lax.axis_index('cp') * HALF
    a_rows, inside = [], []
    for j in range(2):
        first = lo - sc_ref[2 * step + j]
        want = first + lax.broadcasted_iota(jnp.int32, (HALF, HEAD), 0)
        have = lax.broadcasted_iota(jnp.int32, (HALF, HEAD), 1)
        pick = jnp.where(want == have, 1.0, 0.0).astype(BF16)
        a_rows.append(dot(pick, h_ref[j]))
        idx = first + lax.broadcasted_iota(jnp.int32, (HALF, HEAD), 0)
        inside.append((idx >= 0) & (idx < HEAD))
    a = rms_norm(jnp.concatenate(a_rows, axis=0), ga_ref[...])
    here = pl.ds(pl.multiple_of(lo, HALF), HALF)
    cos = jnp.concatenate([cos_ref[here, :]] * 2, axis=0)
    sin = jnp.concatenate([sin_ref[here, :]] * 2, axis=0)
    for g in range(4):
        kv = dot(a, wh_ref[g, :, 512:])
        k = rotate(kv[:, :HEAD], cos, sin).astype(BF16)
        v = kv[:, HEAD:].astype(BF16)
        cols = slice(g * HEAD, (g + 1) * HEAD)
        for j in range(2):
            rows = slice(j * HALF, (j + 1) * HALF)
            ok_ref[j, :, cols] = jnp.where(inside[j], k[rows], ck_ref[j, :, cols])
            ov_ref[j, :, cols] = jnp.where(inside[j], v[rows], cv_ref[j, :, cols])


def write_windows(scalars, hidden, ga, cos, sin, wh, cache_k, cache_v):
    n_seq, rows, width = cache_k.shape
    d = hidden.shape[2]
    one = pl.Buffered(1)
    cache_spec = pl.BlockSpec((2, rows, width), lambda i, sc: (i, 0, 0))
    return pl.pallas_call(
        window_kernel,
        out_shape=[jax.ShapeDtypeStruct(cache_k.shape, BF16)] * 2,
        grid_spec=pltpu.PrefetchScalarGridSpec(
            num_scalar_prefetch=1,
            grid=(n_seq // 2,),
            in_specs=[
                pl.BlockSpec((2, HEAD, d), lambda i, sc: (i, 0, 0)),
                pl.BlockSpec(memory_space=pltpu.VMEM),
                pl.BlockSpec(memory_space=pltpu.VMEM),
                pl.BlockSpec(memory_space=pltpu.VMEM),
                pl.BlockSpec(memory_space=pltpu.VMEM),
                cache_spec,
                cache_spec,
            ],
            out_specs=[cache_spec, cache_spec],
        ),
        compiler_params=pltpu.CompilerParams(vmem_limit_bytes=VMEM_BESIDE),
        cost_estimate=pl.CostEstimate(flops=2 * n_seq * rows * d * 2 * width, bytes_accessed=60_000_000, transcendentals=0),
        name="cache_window",
    )(scalars, hidden, ga, cos, sin, wh, cache_k, cache_v)


def place_kernel(where, blk, tab_ref, *rest):
    n_part = len(where)
    parts = rest[:n_part]
    out_ref, wide, narrow, in_sem, out_sem = rest[-5:]
    slots = wide.shape[0]
    jobs = [(k, b) for k in range(n_part) for b in range(parts[k].shape[0] // blk)]

    def load(n):
        k, b = jobs[n]
        return pltpu.make_async_copy(parts[k].at[pl.ds(b * blk, blk), :], wide.at[n % slots], in_sem.at[n % slots])

    def store(n):
        k, b = jobs[n]
        entry, first = where[k]
        return pltpu.make_async_copy(narrow.at[n % slots], out_ref.at[tab_ref[entry], pl.ds(first + b * blk, blk), :],
                                     out_sem.at[n % slots])

    for n in range(min(slots, len(jobs))):
        load(n).start()
    for n in range(len(jobs)):
        load(n).wait()
        if n >= slots:
            store(n - slots).wait()

        @pl.loop(0, blk // 16)
        def _(r, n=n):
            rows = pl.ds(pl.multiple_of(r * 16, 16), 16)
            narrow[n % slots, rows, :] = wide[n % slots, rows, :].astype(BF16)

        store(n).start()
        if n + slots < len(jobs):
            load(n + slots).start()
    for n in range(max(0, len(jobs) - slots), len(jobs)):
        store(n).wait()


def place_rows(table, parts, where, out, blk):
    d = parts[0].shape[1]
    any_spec = pl.BlockSpec(memory_space=pl.ANY)
    n_part = len(parts)
    slots = min(8, sum(p.shape[0] // blk for p in parts))
    return pl.pallas_call(
        functools.partial(place_kernel, where, blk),
        out_shape=jax.ShapeDtypeStruct(out.shape, BF16),
        in_specs=[pl.BlockSpec(memory_space=pltpu.SMEM)] + [any_spec] * (n_part + 1),
        out_specs=any_spec,
        scratch_shapes=[
            pltpu.VMEM((slots, blk, d), F32),
            pltpu.VMEM((slots, blk, d), BF16),
            pltpu.SemaphoreType.DMA((slots,)),
            pltpu.SemaphoreType.DMA((slots,)),
        ],
        input_output_aliases={n_part + 1: 0},
        compiler_params=pltpu.CompilerParams(vmem_limit_bytes=VMEM_ALL),
        cost_estimate=pl.CostEstimate(flops=10_000_000, bytes_accessed=sum(p.size for p in parts) * 6, transcendentals=0),
    )(table, *parts, out)


def solution(mesh):
    d2d = [(0, 1), (1, 0), (2, 3), (3, 2)]
    cross = [(0, 2), (1, 3), (2, 0), (3, 1)]

    def send(x, pairs, axis='cp'):
        x = lax.ppermute(x, axis, pairs)
        return x

    def body(hidden, start_pos, cache_k, cache_v, w_q, w_k, w_v, w_o, w_gate, w_up, w_down, norm_attn, norm_mlp):
        n_seq, _, d = hidden.shape
        i32 = jnp.int32
        table, over, piece_a, piece_b, piece_e, piece_o = plan_and_pack(start_pos, cache_k, cache_v)
        in_smem = lambda x: pltpu.with_memory_space_constraint(x, pltpu.SMEM)
        got_a = send(piece_a, [(0, 3)])
        got_b = send(piece_b, [(0, 2), (2, 0), (3, 1)])
        got_a, piece_e, piece_o = lax.optimization_barrier((got_a, piece_e, piece_o))
        got_e = send(piece_e, [(1, 2)])
        got_o = send(piece_o, [(1, 3)])

        def send_all(_):
            sid = jnp.arange(n_seq, dtype=i32)
            before = (start_pos[None, :] < start_pos[:, None]) | (
                (start_pos[None, :] == start_pos[:, None]) & (sid[None, :] < sid[:, None]))
            rank = jnp.sum(before.astype(i32), axis=1)
            order = jnp.sum((rank[None, :] == sid[:, None]).astype(i32) * sid[None, :], axis=1)
            got = lax.ppermute(pack_full(order, cache_k, cache_v), 'cp', [(0, 2), (1, 3)])
            return got, lax.ppermute(got, 'cp', [(2, 3), (3, 2)])

        full, full_f = lax.cond(over[0] > 0, send_all, lambda _: tuple(blank(2)), 0)

        w_q, w_k, w_v, full, full_f = lax.optimization_barrier((w_q, w_k, w_v, full, full_f))
        *kept, piece_s, piece_d = split_heads(in_smem(table), cache_k, cache_v, w_q, w_k, w_v, norm_attn, norm_mlp)
        sib = send(piece_s, [(0, 1), (1, 0)])
        got_d = send(piece_d, [(0, 3)])
        wh, cos, sin, ga, gm = [pltpu.with_memory_space_constraint(x, pltpu.VMEM) for x in kept]
        wo = w_o.reshape(-1, d)

        out = None
        tab = table
        parts, where = [], []
        for t in range(4):
            pieces = (got_a, got_b if t > 0 else got_a) + ((got_d, got_e, got_o) if t > 1 else (got_a,) * 3)
            *own, out = run_layer(t, in_smem(tab), in_smem(over), hidden, ga, gm, cos, sin, wh, wo, w_gate, w_up, w_down,
                                  cache_k, cache_v, sib, full, full_f, pieces, out, (192, 64) if t == 3 else (HEAD,))
            tab, own = lax.optimization_barrier((tab, own))
            if t < 3:
                crs = send(own[0], cross)
                near = send(own[0], d2d)
                dia = send(crs, d2d)
                parts += [near, crs, dia]
                where += [(ROW * t + k, 0) for k in (1, 2, 3)]
        most, rest = own
        crs_most, near_most = send(most, cross), send(most, d2d)
        start_late, _ = lax.optimization_barrier((start_pos, tab))
        new_k, new_v = write_windows(start_late, hidden, ga, cos, sin, wh, cache_k, cache_v)
        rest, new_k = lax.optimization_barrier((rest, new_k))
        crs_rest, near_rest = send(rest, cross), send(rest, d2d)
        dia_most, dia_rest = send(crs_most, d2d), send(crs_rest, d2d)
        last = ROW * 3
        out = place_rows(in_smem(tab), parts + [near_most], where + [(last + 1, 0)], out, 64)
        out = place_rows(in_smem(tab), [crs_most, near_rest], [(last + 2, 0), (last + 1, 192)], out, 64)
        out = place_rows(in_smem(tab), [dia_most], [(last + 3, 0)], out, 64)
        out = place_rows(in_smem(tab), [crs_rest], [(last + 2, 192)], out, 32)
        out = place_rows(in_smem(tab), [dia_rest], [(last + 3, 192)], out, 32)
        return out, new_k, new_v

    group_spec = P('dp', None, None)
    cache_spec = P('dp', 'cp', None)
    whole_spec = P()
    return jax.shard_map(
        body,
        mesh=mesh,
        in_specs=(group_spec, P('dp'), cache_spec, cache_spec) + (whole_spec,) * 9,
        out_specs=(group_spec, cache_spec, cache_spec),
        check_vma=False,
    )
```
